32 devices in a mesh: dp: 2 (over x), col: 4 (over z), row: 4 (over y, core).
Axes of the slice: x: 2, y: 2, z: 4, core: 2. Of those that a mesh axis runs over, the one named last changes fastest.
Arguments:
- x_act: bfloat16 [128, 8192], P(('dp', 'row'), 'col'), parts along dimension 0
- ln_gain: float32 [8192], P('col')
- w_in: bfloat16 [8192, 32768], P('row', 'col')
- w_out: bfloat16 [32768, 8192], P('row', 'col')
Outputs:
- output: bfloat16 [128, 8192], P(('dp', 'row'), 'col'), parts along dimension 0
There are 2 independent parts. The reference program is written for one: setup_inputs(seed, part) draws one part's arguments, and reference() takes and returns one part's arrays. A program takes and returns all parts, laid end to end along the dimension named above; an argument that names none is the same for every part.
All inputs are finite; a program needn't handle non-finite values.
Results may differ from the reference program's by a relative error of at most 0.00115.
Values are sent between devices in bfloat16 or wider.
A program may use at most 1 GiB of HBM per device.

```python
import jax
import jax.numpy as jnp
from jax import lax

TOKENS = 64
D_MODEL = 8192
D_FF = 32768

NORM_EPS = 1e-5


def setup_inputs(seed: int = 0, part: int = 0) -> dict:
    key = jax.random.key(seed)
    part_key, shared_key = jax.random.split(key)
    part_key = jax.random.fold_in(part_key, part)
    key_noise, key_row, key_shift, key_scale = jax.random.split(part_key, 4)
    key_gain, key_in, key_out = jax.random.split(shared_key, 3)
    walk_norm = D_MODEL ** -0.5
    feat_shift = 0.8 * walk_norm * jnp.cumsum(jax.random.normal(key_shift, (D_MODEL,), jnp.float32))
    feat_scale = jnp.exp(0.5 * walk_norm * jnp.cumsum(jax.random.normal(key_scale, (D_MODEL,), jnp.float32)))
    row_shift = 0.5 * jax.random.normal(key_row, (TOKENS, 1), jnp.float32)
    noise = jax.random.normal(key_noise, (TOKENS, D_MODEL), jnp.float32)
    x_act = (noise * feat_scale + feat_shift + row_shift).astype(jnp.bfloat16)
    ln_gain = jax.random.uniform(key_gain, (D_MODEL,), jnp.float32, 0.5, 1.5)
    w_in = (D_MODEL ** -0.5 * jax.random.normal(key_in, (D_MODEL, D_FF), jnp.float32)).astype(jnp.bfloat16)
    w_out = (1.5 * D_FF ** -0.5 * jax.random.normal(key_out, (D_FF, D_MODEL), jnp.float32)).astype(jnp.bfloat16)
    return {"x_act": x_act, "ln_gain": ln_gain, "w_in": w_in, "w_out": w_out}


def reference(x_act, ln_gain, w_in, w_out):
    x_f32 = x_act.astype(jnp.float32)
    row_mean = jnp.mean(x_f32, axis=1, keepdims=True)
    row_var = jnp.mean(x_f32 * x_f32, axis=1, keepdims=True) - row_mean * row_mean
    z_norm = ((x_f32 - row_mean) * lax.rsqrt(row_var + NORM_EPS) * ln_gain).astype(jnp.bfloat16)
    hidden = jax.nn.gelu(jnp.dot(z_norm, w_in, preferred_element_type=jnp.float32), approximate=True).astype(jnp.bfloat16)
    branch = jnp.dot(hidden, w_out, preferred_element_type=jnp.float32)
    return (x_f32 + branch).astype(jnp.bfloat16)
```

```python
import functools

import jax
import jax.numpy as jnp
from jax import lax
from jax.experimental import pallas as pl
from jax.experimental.pallas import tpu as pltpu
from jax.sharding import PartitionSpec as P

NORM_EPS = 1e-5
MESH = pl.DeviceIdType.MESH
BF16, F32 = jnp.bfloat16, jnp.float32
N_COL = 4
N_ROW = 4


def gelu_tanh(x):
    return x * (0.5 * (1.0 + jnp.tanh(0.7978845608028654 * (x + 0.044715 * (x * x * x)))))


def mlp_kernel(
    n_chunks, n_slots, blk,
    x_hbm, g_hbm, w_in_hbm, w_out_hbm, y_ref,
    x_own, gain, stats, x_all, z_ref, ring, part, from_near, from_far, hid, acc, near_sum, pair_sum, far_sum,
    x_load, w_load, x_send, x_recv, g_send, g_recv, s_send, s_recv, p_send, p_recv, f_recv,
    h_up, h_down, h_recv, n_send, n_recv, o_send, o_recv,
):
    dp, c, r = lax.axis_index("dp"), lax.axis_index("col"), lax.axis_index("row")
    rows = x_own.shape[0]
    n_blk = x_own.shape[1] // blk
    d_model = x_own.shape[1] * N_COL
    near = r + 1 - 2 * (r % 2)
    far = (r + 2) % N_ROW
    me = c * N_ROW + r
    is_root = c == r

    def remote(src, dst, send, recv, to_col, to_row):
        return pltpu.make_async_remote_copy(
            src_ref=src, dst_ref=dst, send_sem=send, recv_sem=recv,
            device_id=(dp, to_col, to_row), device_id_type=MESH,
        )

    def peer(i):
        other = (me + i) % (N_COL * N_ROW)
        return other // N_ROW, other % N_ROW

    x_cp = pltpu.make_async_copy(x_hbm, x_own, x_load.at[0])
    x_cp.start()
    g_cp = pltpu.make_async_copy(g_hbm, gain.at[c], x_load.at[1])
    g_cp.start()
    barrier = pltpu.get_barrier_semaphore()
    for i in range(1, N_COL * N_ROW):
        pc, pr = peer(i)
        pl.semaphore_signal(barrier, inc=1, device_id=(dp, pc, pr), device_id_type=MESH)

    def load_in(j, slot):
        for k in range(n_blk):
            pltpu.make_async_copy(
                w_in_hbm.at[pl.ds(k * blk, blk), pl.ds(pl.multiple_of(j * blk, blk), blk)],
                ring.at[slot, k], w_load.at[slot],
            ).start()

    def load_out(j, slot):
        for k in range(n_blk):
            pltpu.make_async_copy(
                w_out_hbm.at[pl.ds(pl.multiple_of(j * blk, blk), blk), pl.ds(k * blk, blk)],
                ring.at[slot, k], w_load.at[slot],
            ).start()

    def wait_slot(slot):
        pltpu.make_async_copy(ring.at[slot], ring.at[slot], w_load.at[slot]).wait()

    def fill_in(j, _):
        load_in(j, j)
        return 0

    def fill_out(j, _):
        load_out(j, n_chunks + j)
        return 0

    lax.fori_loop(0, n_chunks, fill_in, 0)
    lax.fori_loop(0, n_slots - n_chunks, fill_out, 0)

    x_cp.wait()
    g_cp.wait()
    x_f32 = x_own[...].astype(F32)
    lane = lax.broadcasted_iota(jnp.int32, (rows, 128), 1)
    sub = lax.broadcasted_iota(jnp.int32, (rows, 128), 0)
    total = jnp.sum(x_f32, axis=1, keepdims=True)
    square = jnp.sum(x_f32 * x_f32, axis=1, keepdims=True)
    packed = jnp.where(lane == sub, total, 0.0) + jnp.where(lane == sub + rows, square, 0.0)
    stats[me] = jnp.sum(packed, axis=0, keepdims=True)

    pl.semaphore_wait(barrier, N_COL * N_ROW - 1)

    def stat_copy(i):
        pc, pr = peer(i)
        return remote(stats.at[me], stats.at[me], s_send.at[i], s_recv.at[me], pc, pr)

    def x_copy(i):
        return remote(x_own, x_all.at[pl.ds(r * rows, rows)], x_send.at[i], x_recv.at[r], (c + i) % N_COL, c)

    def g_copy(i):
        return remote(gain.at[c], gain.at[c], g_send.at[i], g_recv.at[0], (c + i) % N_COL, c)

    for i in range(1, N_COL * N_ROW):
        stat_copy(i).start()
    for i in (3, 2, 1):
        x_copy(i).start()

    @pl.when(is_root)
    def _():
        for i in (3, 2, 1):
            g_copy(i).start()
        x_all[pl.ds(pl.multiple_of(r * rows, rows), rows), :] = x_own[...]

    @pl.when(jnp.logical_not(is_root))
    def _():
        x_copy(0).start()

    for i in range(1, N_COL * N_ROW):
        other = (me + i) % (N_COL * N_ROW)
        pltpu.make_async_copy(stats.at[other], stats.at[other], s_recv.at[other]).wait()

    @pl.when(jnp.logical_not(is_root))
    def _():
        pltpu.make_async_copy(gain.at[r], gain.at[r], g_recv.at[0]).wait()

    for q in range(N_ROW):
        at = pl.ds(q * rows, rows)

        @pl.when(jnp.logical_not(jnp.logical_and(is_root, r == q)))
        def _():
            pltpu.make_async_copy(x_all.at[at], x_all.at[at], x_recv.at[q]).wait()

        whole = stats[q] + stats[N_ROW + q] + stats[2 * N_ROW + q] + stats[3 * N_ROW + q]
        whole = jnp.broadcast_to(whole, (rows, 128))
        mean = jnp.sum(jnp.where(lane == sub, whole, 0.0), axis=1, keepdims=True) / d_model
        mean_sq = jnp.sum(jnp.where(lane == sub + rows, whole, 0.0), axis=1, keepdims=True) / d_model
        inv = lax.rsqrt(mean_sq - mean * mean + NORM_EPS)
        z_ref[at, :] = ((x_all[at, :].astype(F32) - mean) * inv * gain[r]).astype(BF16)

    role_near = near == c
    role_far = far == c
    role_relay = jnp.logical_not(jnp.logical_or(is_root, jnp.logical_or(role_near, role_far)))

    def near_copy(j):
        return remote(part.at[j], from_near.at[j], p_send.at[j], p_recv.at[j], c, near)

    def far_copy(j):
        return remote(part.at[j], from_far.at[j], p_send.at[j], f_recv.at[j], c, far)

    def pass_on(j):
        near_copy(j).wait_recv()
        part[j] = part[j] + from_near[j]
        far_copy(j).start()

    def up(j, _):
        wait_slot(j)
        total = jnp.dot(z_ref[:, pl.ds(0, blk)], ring[j, 0], preferred_element_type=F32)
        for k in range(1, n_blk):
            total += jnp.dot(z_ref[:, pl.ds(k * blk, blk)], ring[j, k], preferred_element_type=F32)
        part[j] = total

        @pl.when(j < 2 * n_chunks - n_slots)
        def _():
            load_out(j + n_slots - n_chunks, j)

        @pl.when(jnp.logical_or(role_near, role_relay))
        def _():
            near_copy(j).start()

        @pl.when(jnp.logical_and(role_far, j >= 1))
        def _():
            pass_on(j - 1)

        return 0

    lax.fori_loop(0, n_chunks, up, 0)

    @pl.when(role_far)
    def _():
        pass_on(n_chunks - 1)

    def up_copy(j):
        return remote(hid.at[j], hid.at[j], h_up.at[j], h_recv.at[j], (c + 1) % N_COL, r)

    def down_copy(j):
        return remote(hid.at[j], hid.at[j], h_down.at[j], h_recv.at[j], (c + N_COL - 1) % N_COL, r)

    sends_up = jnp.logical_and(c >= r, c < N_COL - 1)
    sends_down = jnp.logical_and(c <= r, c > 0)
    acc[...] = jnp.zeros_like(acc)

    def down(j, _):
        @pl.when(is_root)
        def _():
            near_copy(j).wait_recv()
            far_copy(j).wait_recv()
            hid[j] = gelu_tanh(part[j] + from_near[j] + from_far[j]).astype(BF16)

        @pl.when(jnp.logical_not(is_root))
        def _():
            up_copy(j).wait_recv()

        @pl.when(sends_up)
        def _():
            up_copy(j).start()

        @pl.when(sends_down)
        def _():
            down_copy(j).start()

        slot = (n_chunks + j) % n_slots
        wait_slot(slot)
        for k in range(n_blk):
            at = pl.ds(k * blk, blk)
            acc[:, at] += jnp.dot(hid[j], ring[slot, k], preferred_element_type=F32)
        return 0

    lax.fori_loop(0, n_chunks, down, 0)

    def near_part(i, k):
        other = near if i == 0 else (near + 2) % N_ROW
        at = pl.ds(k * blk, blk)
        return remote(
            acc.at[pl.ds(pl.multiple_of(other * rows, rows), rows), at], near_sum.at[i, :, at],
            n_send.at[i, k], n_recv.at[i, k], c, near,
        )

    def far_part(k):
        at = pl.ds(k * blk, blk)
        return remote(pair_sum.at[:, at], far_sum.at[:, at], o_send.at[k], o_recv.at[k], c, far)

    for i in (1, 0):
        for k in range(n_blk):
            near_part(i, k).start()
    for k in range(n_blk):
        at = pl.ds(k * blk, blk)
        near_part(1, k).wait_recv()
        pair_sum[:, at] = acc[pl.ds(pl.multiple_of(far * rows, rows), rows), at] + near_sum[1, :, at]
        far_part(k).start()
    for k in range(n_blk):
        at = pl.ds(k * blk, blk)
        near_part(0, k).wait_recv()
        far_part(k).wait_recv()
        own = acc[pl.ds(pl.multiple_of(r * rows, rows), rows), at] + near_sum[0, :, at] + far_sum[:, at]
        y_ref[:, at] = (x_own[:, at].astype(F32) + own).astype(BF16)

    for i in range(1, N_COL * N_ROW):
        stat_copy(i).wait_send()
    for i in (3, 2, 1):
        x_copy(i).wait_send()

    @pl.when(is_root)
    def _():
        for i in (3, 2, 1):
            g_copy(i).wait_send()

    @pl.when(jnp.logical_not(is_root))
    def _():
        x_copy(0).wait_send()

    def finish(j, _):
        @pl.when(jnp.logical_not(is_root))
        def _():
            near_copy(j).wait_send()

        @pl.when(sends_up)
        def _():
            up_copy(j).wait_send()

        @pl.when(sends_down)
        def _():
            down_copy(j).wait_send()

        return 0

    lax.fori_loop(0, n_chunks, finish, 0)
    for i in (1, 0):
        for k in range(n_blk):
            near_part(i, k).wait_send()
    for k in range(n_blk):
        far_part(k).wait_send()


def solution(mesh):
    def local_block(x_blk, gain_blk, w_in_blk, w_out_blk):
        rows, depth = x_blk.shape
        blk = depth // 4
        n_chunks = w_in_blk.shape[1] // blk
        n_slots = n_chunks + n_chunks // 2
        tokens = rows * N_ROW
        dma = pltpu.SemaphoreType.DMA
        n_all = N_COL * N_ROW
        return pl.pallas_call(
            functools.partial(mlp_kernel, n_chunks, n_slots, blk),
            out_shape=jax.ShapeDtypeStruct((rows, depth), BF16),
            in_specs=[pl.BlockSpec(memory_space=pl.ANY)] * 4,
            out_specs=pl.BlockSpec(memory_space=pltpu.VMEM),
            scratch_shapes=[
                pltpu.VMEM((rows, depth), BF16),
                pltpu.VMEM((N_COL, 1, depth), F32),
                pltpu.VMEM((n_all, 1, 128), F32),
                pltpu.VMEM((tokens, depth), BF16),
                pltpu.VMEM((tokens, depth), BF16),
                pltpu.VMEM((n_slots, depth // blk, blk, blk), BF16),
                pltpu.VMEM((n_chunks, tokens, blk), F32),
                pltpu.VMEM((n_chunks, tokens, blk), F32),
                pltpu.VMEM((n_chunks, tokens, blk), F32),
                pltpu.VMEM((n_chunks, tokens, blk), BF16),
                pltpu.VMEM((tokens, depth), F32),
                pltpu.VMEM((2, rows, depth), F32),
                pltpu.VMEM((rows, depth), F32),
                pltpu.VMEM((rows, depth), F32),
                dma((2,)), dma((n_slots,)),
                dma((N_COL,)), dma((N_ROW,)), dma((N_COL,)), dma((1,)), dma((n_all,)), dma((n_all,)),
                dma((n_chunks,)), dma((n_chunks,)), dma((n_chunks,)),
                dma((n_chunks,)), dma((n_chunks,)), dma((n_chunks,)),
                dma((2, depth // blk)), dma((2, depth // blk)), dma((depth // blk,)), dma((depth // blk,)),
            ],
            compiler_params=pltpu.CompilerParams(
                collective_id=0, has_side_effects=True, vmem_limit_bytes=67_000_000
            ),
        )(x_blk, gain_blk.reshape(1, depth), w_in_blk, w_out_blk)

    return jax.shard_map(
        local_block,
        mesh=mesh,
        in_specs=(P(("dp", "row"), "col"), P("col"), P("row", "col"), P("row", "col")),
        out_specs=P(("dp", "row"), "col"),
        check_vma=False,
    )
```

```python
import functools

import jax
import jax.numpy as jnp
from jax import lax
from jax.experimental import pallas as pl
from jax.experimental.pallas import tpu as pltpu
from jax.sharding import PartitionSpec as P

NORM_EPS = 1e-5
MESH = pl.DeviceIdType.MESH
BF16, F32 = jnp.bfloat16, jnp.float32
N_COL = 4
N_ROW = 4


def gelu_tanh(x):
    return x * (0.5 * (1.0 + jnp.tanh(0.7978845608028654 * (x + 0.044715 * (x * x * x)))))


def mlp_kernel(
    n_chunks, n_slots, blk,
    x_hbm, g_hbm, w_in_hbm, w_out_hbm, y_ref,
    x_own, gain, stats, x_all, z_ref, ring, part, from_near, from_far, hid, hid_sent, acc, near_sum, pair_sum, far_sum,
    x_load, w_load, x_send, x_recv, g_send, g_recv, s_send, s_recv, p_send, p_recv, f_recv,
    h_inner, h_outer, h_recv, w_send, n_send, n_recv, o_send, o_recv,
):
    dp, c, r = lax.axis_index("dp"), lax.axis_index("col"), lax.axis_index("row")
    rows = x_own.shape[0]
    n_blk = x_own.shape[1] // blk
    d_model = x_own.shape[1] * N_COL
    near = r + 1 - 2 * (r % 2)
    far = (r + 2) % N_ROW
    me = c * N_ROW + r
    is_root = c == r

    def remote(src, dst, send, recv, to_col, to_row):
        return pltpu.make_async_remote_copy(
            src_ref=src, dst_ref=dst, send_sem=send, recv_sem=recv,
            device_id=(dp, to_col, to_row), device_id_type=MESH,
        )

    def peer(i):
        other = (me + i) % (N_COL * N_ROW)
        return other // N_ROW, other % N_ROW

    x_cp = pltpu.make_async_copy(x_hbm, x_own, x_load.at[0])
    x_cp.start()
    g_cp = pltpu.make_async_copy(g_hbm, gain.at[c], x_load.at[1])
    g_cp.start()
    barrier = pltpu.get_barrier_semaphore()
    for i in range(1, N_COL * N_ROW):
        pc, pr = peer(i)
        pl.semaphore_signal(barrier, inc=1, device_id=(dp, pc, pr), device_id_type=MESH)

    def load_in(j, slot):
        pltpu.make_async_copy(
            w_in_hbm.at[:, pl.ds(pl.multiple_of(j * blk, blk), blk)], ring.at[slot], w_load.at[slot]
        ).start()

    def load_out(j, slot):
        for k in range(n_blk):
            pltpu.make_async_copy(
                w_out_hbm.at[pl.ds(pl.multiple_of(j * blk, blk), blk), pl.ds(k * blk, blk)],
                ring.at[slot, pl.ds(k * blk, blk)], w_load.at[slot],
            ).start()

    def wait_slot(slot):
        pltpu.make_async_copy(ring.at[slot], ring.at[slot], w_load.at[slot]).wait()

    def fill_in(j, _):
        load_in(j, j)
        return 0

    def fill_out(j, _):
        load_out(j, n_chunks + j)
        return 0

    lax.fori_loop(0, n_chunks, fill_in, 0)

    x_cp.wait()
    g_cp.wait()
    x_f32 = x_own[...].astype(F32)
    lane = lax.broadcasted_iota(jnp.int32, (rows, 128), 1)
    sub = lax.broadcasted_iota(jnp.int32, (rows, 128), 0)
    total = jnp.sum(x_f32, axis=1, keepdims=True)
    square = jnp.sum(x_f32 * x_f32, axis=1, keepdims=True)
    packed = jnp.where(lane == sub, total, 0.0) + jnp.where(lane == sub + rows, square, 0.0)
    stats[me] = jnp.sum(packed, axis=0, keepdims=True)

    pl.semaphore_wait(barrier, N_COL * N_ROW - 1)

    def stat_copy(i):
        pc, pr = peer(i)
        return remote(stats.at[me], stats.at[me], s_send.at[i], s_recv.at[me], pc, pr)

    def x_copy(i):
        return remote(x_own, x_all.at[pl.ds(r * rows, rows)], x_send.at[i], x_recv.at[r], (c + i) % N_COL, c)

    def g_copy(i):
        return remote(gain.at[c], gain.at[c], g_send.at[i], g_recv.at[0], (c + i) % N_COL, c)

    for i in range(1, N_COL * N_ROW):
        stat_copy(i).start()
    for i in (3, 2, 1):
        x_copy(i).start()

    @pl.when(is_root)
    def _():
        for i in (3, 2, 1):
            g_copy(i).start()
        x_all[pl.ds(pl.multiple_of(r * rows, rows), rows), :] = x_own[...]

    @pl.when(jnp.logical_not(is_root))
    def _():
        x_copy(0).start()

    lax.fori_loop(0, n_slots - n_chunks, fill_out, 0)

    for i in range(1, N_COL * N_ROW):
        other = (me + i) % (N_COL * N_ROW)
        pltpu.make_async_copy(stats.at[other], stats.at[other], s_recv.at[other]).wait()

    @pl.when(jnp.logical_not(is_root))
    def _():
        pltpu.make_async_copy(gain.at[r], gain.at[r], g_recv.at[0]).wait()

    for q in range(N_ROW):
        at = pl.ds(q * rows, rows)

        @pl.when(jnp.logical_not(jnp.logical_and(is_root, r == q)))
        def _():
            pltpu.make_async_copy(x_all.at[at], x_all.at[at], x_recv.at[q]).wait()

        whole = stats[q] + stats[N_ROW + q] + stats[2 * N_ROW + q] + stats[3 * N_ROW + q]
        whole = jnp.broadcast_to(whole, (rows, 128))
        mean = jnp.sum(jnp.where(lane == sub, whole, 0.0), axis=1, keepdims=True) / d_model
        mean_sq = jnp.sum(jnp.where(lane == sub + rows, whole, 0.0), axis=1, keepdims=True) / d_model
        inv = lax.rsqrt(mean_sq - mean * mean + NORM_EPS)
        z_ref[at, :] = ((x_all[at, :].astype(F32) - mean) * inv * gain[r]).astype(BF16)

    role_near = near == c
    role_far = far == c
    role_last = r == N_ROW - 1 - c

    def kind_phase(j):
        return (j + 4) % 5

    def at_root(j):
        return jnp.logical_or(kind_phase(j) == 0, kind_phase(j) == 2)

    def by_root(j):
        return jnp.logical_or(kind_phase(j) == 1, kind_phase(j) == 3)

    def direct(j):
        return kind_phase(j) == 4

    def near_copy(j):
        return remote(part.at[j], from_near.at[j], p_send.at[j], p_recv.at[j], c, near)

    def far_copy(j):
        return remote(part.at[j], from_far.at[j], p_send.at[j], f_recv.at[j], c, far)

    def passes(j):
        return jnp.logical_or(
            jnp.logical_and(at_root(j), role_far), jnp.logical_and(jnp.logical_not(at_root(j)), role_near)
        )

    def ends(j):
        return jnp.logical_or(
            jnp.logical_and(at_root(j), is_root), jnp.logical_and(jnp.logical_not(at_root(j)), role_last)
        )

    def gives(j):
        return jnp.logical_not(jnp.logical_or(passes(j), ends(j)))

    def pass_on(j):
        @pl.when(passes(j))
        def _():
            near_copy(j).wait_recv()
            part[j] = part[j] + from_near[j]
            far_copy(j).start()

    def up(j, _):
        wait_slot(j)
        total = jnp.dot(z_ref[:, pl.ds(0, blk)], ring[j, pl.ds(0, blk)], preferred_element_type=F32)
        for k in range(1, n_blk):
            at = pl.ds(k * blk, blk)
            total += jnp.dot(z_ref[:, at], ring[j, at], preferred_element_type=F32)
        part[j] = total

        @pl.when(j < 2 * n_chunks - n_slots)
        def _():
            load_out(j + n_slots - n_chunks, j)

        @pl.when(gives(j))
        def _():
            near_copy(j).start()

        @pl.when(j >= 1)
        def _():
            pass_on(j - 1)

        return 0

    lax.fori_loop(0, n_chunks, up, 0)
    pass_on(n_chunks - 1)

    inner = 1 + c % 2
    outer = (3 * c + 2) % 5
    inside = jnp.logical_or(c == 1, c == 2)
    forwards = jnp.logical_or(jnp.logical_and(c == 2, r < 2), jnp.logical_and(c == 1, r >= 2))

    def inner_copy(j):
        return remote(hid.at[j], hid.at[j], h_inner.at[j], h_recv.at[j], inner, r)

    def outer_copy(j):
        return remote(hid.at[j], hid.at[j], h_outer.at[j], h_recv.at[j], outer, r)

    def forward_copy(j):
        return remote(hid.at[j], hid.at[j], h_inner.at[j], h_recv.at[j], 3 * (c - 1), r)

    def last_copy(j, to):
        return remote(hid_sent.at[j], hid.at[j], w_send.at[to, j], h_recv.at[j], to, c)

    acc[...] = jnp.zeros_like(acc)
    early_lag = jnp.where(inside | is_root, 6, 11)
    late_lag = jnp.where(is_root, 6, early_lag + 6)

    def finish_sum(j):
        @pl.when(ends(j))
        def _():
            near_copy(j).wait_recv()
            far_copy(j).wait_recv()
            chunk = gelu_tanh(part[j] + from_near[j] + from_far[j]).astype(BF16)

            @pl.when(is_root)
            def _():
                hid[j] = chunk
                inner_copy(j).start()
                outer_copy(j).start()

            @pl.when(jnp.logical_not(is_root))
            def _():
                hid_sent[j] = chunk

                @pl.when(by_root(j))
                def _():
                    last_copy(j, c).start()

                @pl.when(direct(j))
                def _():
                    for to in range(N_COL):
                        last_copy(j, to).start()

    def use(j):
        @pl.when(jnp.logical_not(jnp.logical_and(is_root, at_root(j))))
        def _():
            inner_copy(j).wait_recv()

        @pl.when(jnp.logical_and(is_root, by_root(j)))
        def _():
            inner_copy(j).start()
            outer_copy(j).start()

        @pl.when(jnp.logical_and(forwards, jnp.logical_not(direct(j))))
        def _():
            forward_copy(j).start()

        slot = (n_chunks + j) % n_slots
        wait_slot(slot)
        for k in range(n_blk):
            at = pl.ds(k * blk, blk)
            acc[:, at] += jnp.dot(hid[j], ring[slot, at], preferred_element_type=F32)

    def down(t, _):
        @pl.when(t < n_chunks)
        def _():
            finish_sum(t)

        early = t - early_lag
        late = t - late_lag

        @pl.when(jnp.logical_and(early >= 0, early < n_chunks))
        def _():
            @pl.when(at_root(early))
            def _():
                use(early)

        @pl.when(jnp.logical_and(late >= 0, late < n_chunks))
        def _():
            @pl.when(jnp.logical_not(at_root(late)))
            def _():
                use(late)

        return 0

    lax.fori_loop(0, n_chunks + 17, down, 0)

    def near_part(i, k):
        other = near if i == 0 else (near + 2) % N_ROW
        at = pl.ds(k * blk, blk)
        return remote(
            acc.at[pl.ds(pl.multiple_of(other * rows, rows), rows), at], near_sum.at[i, :, at],
            n_send.at[i, k], n_recv.at[i, k], c, near,
        )

    def far_part(k):
        at = pl.ds(k * blk, blk)
        return remote(pair_sum.at[:, at], far_sum.at[:, at], o_send.at[k], o_recv.at[k], c, far)

    for i in (1, 0):
        for k in range(n_blk):
            near_part(i, k).start()
    for k in range(n_blk):
        at = pl.ds(k * blk, blk)
        near_part(1, k).wait_recv()
        pair_sum[:, at] = acc[pl.ds(pl.multiple_of(far * rows, rows), rows), at] + near_sum[1, :, at]
        far_part(k).start()
    for k in range(n_blk):
        at = pl.ds(k * blk, blk)
        near_part(0, k).wait_recv()
        far_part(k).wait_recv()
        own = acc[pl.ds(pl.multiple_of(r * rows, rows), rows), at] + near_sum[0, :, at] + far_sum[:, at]
        y_ref[:, at] = (x_own[:, at].astype(F32) + own).astype(BF16)

    for i in range(1, N_COL * N_ROW):
        stat_copy(i).wait_send()
    for i in (3, 2, 1):
        x_copy(i).wait_send()

    @pl.when(is_root)
    def _():
        for i in (3, 2, 1):
            g_copy(i).wait_send()

    @pl.when(jnp.logical_not(is_root))
    def _():
        x_copy(0).wait_send()

    def finish(j, _):
        @pl.when(jnp.logical_not(ends(j)))
        def _():
            near_copy(j).wait_send()

        @pl.when(jnp.logical_and(is_root, jnp.logical_not(direct(j))))
        def _():
            inner_copy(j).wait_send()
            outer_copy(j).wait_send()

        @pl.when(jnp.logical_and(forwards, jnp.logical_not(direct(j))))
        def _():
            forward_copy(j).wait_send()

        @pl.when(jnp.logical_and(role_last, by_root(j)))
        def _():
            last_copy(j, c).wait_send()

        @pl.when(jnp.logical_and(role_last, direct(j)))
        def _():
            for to in range(N_COL):
                last_copy(j, to).wait_send()

        return 0

    lax.fori_loop(0, n_chunks, finish, 0)
    for i in (1, 0):
        for k in range(n_blk):
            near_part(i, k).wait_send()
    for k in range(n_blk):
        far_part(k).wait_send()


def solution(mesh):
    def local_block(x_blk, gain_blk, w_in_blk, w_out_blk):
        rows, depth = x_blk.shape
        blk = depth // 8
        n_chunks = w_in_blk.shape[1] // blk
        n_slots = n_chunks + n_chunks // 2
        tokens = rows * N_ROW
        dma = pltpu.SemaphoreType.DMA
        n_all = N_COL * N_ROW
        return pl.pallas_call(
            functools.partial(mlp_kernel, n_chunks, n_slots, blk),
            out_shape=jax.ShapeDtypeStruct((rows, depth), BF16),
            in_specs=[pl.BlockSpec(memory_space=pl.ANY)] * 4,
            out_specs=pl.BlockSpec(memory_space=pltpu.VMEM),
            scratch_shapes=[
                pltpu.VMEM((rows, depth), BF16),
                pltpu.VMEM((N_COL, 1, depth), F32),
                pltpu.VMEM((n_all, 1, 128), F32),
                pltpu.VMEM((tokens, depth), BF16),
                pltpu.VMEM((tokens, depth), BF16),
                pltpu.VMEM((n_slots, depth, blk), BF16),
                pltpu.VMEM((n_chunks, tokens, blk), F32),
                pltpu.VMEM((n_chunks, tokens, blk), F32),
                pltpu.VMEM((n_chunks, tokens, blk), F32),
                pltpu.VMEM((n_chunks, tokens, blk), BF16),
                pltpu.VMEM((n_chunks, tokens, blk), BF16),
                pltpu.VMEM((tokens, depth), F32),
                pltpu.VMEM((2, rows, depth), F32),
                pltpu.VMEM((rows, depth), F32),
                pltpu.VMEM((rows, depth), F32),
                dma((2,)), dma((n_slots,)),
                dma((N_COL,)), dma((N_ROW,)), dma((N_COL,)), dma((1,)), dma((n_all,)), dma((n_all,)),
                dma((n_chunks,)), dma((n_chunks,)), dma((n_chunks,)),
                dma((n_chunks,)), dma((n_chunks,)), dma((n_chunks,)), dma((N_COL, n_chunks)),
                dma((2, depth // blk)), dma((2, depth // blk)), dma((depth // blk,)), dma((depth // blk,)),
            ],
            compiler_params=pltpu.CompilerParams(
                collective_id=0, has_side_effects=True, vmem_limit_bytes=67_000_000
            ),
        )(x_blk, gain_blk.reshape(1, depth), w_in_blk, w_out_blk)

    return jax.shard_map(
        local_block,
        mesh=mesh,
        in_specs=(P(("dp", "row"), "col"), P("col"), P("row", "col"), P("row", "col")),
        out_specs=P(("dp", "row"), "col"),
        check_vma=False,
    )
```

```python
import functools

import jax
import jax.numpy as jnp
from jax import lax
from jax.experimental import pallas as pl
from jax.experimental.pallas import tpu as pltpu
from jax.sharding import PartitionSpec as P

NORM_EPS = 1e-5
MESH = pl.DeviceIdType.MESH
BF16, F32 = jnp.bfloat16, jnp.float32
N_COL = 4
N_ROW = 4


def gelu_tanh(x):
    return x * (0.5 * (1.0 + jnp.tanh(0.7978845608028654 * (x + 0.044715 * (x * x * x)))))


def mlp_kernel(
    n_chunks, n_slots, blk,
    x_hbm, g_hbm, w_in_hbm, w_out_hbm, y_ref,
    x_own, gain, stats, x_all, z_ref, ring, part, from_near, from_far, hid, hid_sent, acc, near_sum, pair_sum, far_sum,
    x_load, w_load, x_send, x_recv, g_send, g_recv, s_send, s_recv, p_send, p_recv, f_recv,
    h_inner, h_outer, h_recv, w_send, n_send, n_recv, o_send, o_recv,
):
    dp, c, r = lax.axis_index("dp"), lax.axis_index("col"), lax.axis_index("row")
    rows = x_own.shape[0]
    n_blk = x_own.shape[1] // blk
    d_model = x_own.shape[1] * N_COL
    near = r + 1 - 2 * (r % 2)
    far = (r + 2) % N_ROW
    me = c * N_ROW + r
    is_root = c == r

    def remote(src, dst, send, recv, to_col, to_row):
        return pltpu.make_async_remote_copy(
            src_ref=src, dst_ref=dst, send_sem=send, recv_sem=recv,
            device_id=(dp, to_col, to_row), device_id_type=MESH,
        )

    def peer(i):
        other = (me + i) % (N_COL * N_ROW)
        return other // N_ROW, other % N_ROW

    x_cp = pltpu.make_async_copy(x_hbm, x_own, x_load.at[0])
    x_cp.start()
    g_cp = pltpu.make_async_copy(g_hbm, gain.at[c], x_load.at[1])
    g_cp.start()
    barrier = pltpu.get_barrier_semaphore()
    for i in range(1, N_COL * N_ROW):
        pc, pr = peer(i)
        pl.semaphore_signal(barrier, inc=1, device_id=(dp, pc, pr), device_id_type=MESH)

    def load_in(j, slot):
        pltpu.make_async_copy(
            w_in_hbm.at[:, pl.ds(pl.multiple_of(j * blk, blk), blk)], ring.at[slot], w_load.at[slot]
        ).start()

    def load_out(j, slot):
        for k in range(n_blk):
            pltpu.make_async_copy(
                w_out_hbm.at[pl.ds(pl.multiple_of(j * blk, blk), blk), pl.ds(k * blk, blk)],
                ring.at[slot, pl.ds(k * blk, blk)], w_load.at[slot],
            ).start()

    def wait_slot(slot):
        pltpu.make_async_copy(ring.at[slot], ring.at[slot], w_load.at[slot]).wait()

    def fill_in(j, _):
        load_in(j, j)
        return 0

    def fill_out(j, _):
        load_out(j, n_chunks + j)
        return 0

    lax.fori_loop(0, n_chunks, fill_in, 0)

    x_cp.wait()
    g_cp.wait()
    x_f32 = x_own[...].astype(F32)
    lane = lax.broadcasted_iota(jnp.int32, (rows, 128), 1)
    sub = lax.broadcasted_iota(jnp.int32, (rows, 128), 0)
    total = jnp.sum(x_f32, axis=1, keepdims=True)
    square = jnp.sum(x_f32 * x_f32, axis=1, keepdims=True)
    packed = jnp.where(lane == sub, total, 0.0) + jnp.where(lane == sub + rows, square, 0.0)
    stats[me] = jnp.sum(packed, axis=0, keepdims=True)

    pl.semaphore_wait(barrier, N_COL * N_ROW - 1)

    def stat_copy(i):
        pc, pr = peer(i)
        return remote(stats.at[me], stats.at[me], s_send.at[i], s_recv.at[me], pc, pr)

    def x_copy(i):
        return remote(x_own, x_all.at[pl.ds(r * rows, rows)], x_send.at[i], x_recv.at[r], (c + i) % N_COL, c)

    def g_copy(i):
        return remote(gain.at[c], gain.at[c], g_send.at[i], g_recv.at[0], (c + i) % N_COL, c)

    for i in range(1, N_COL * N_ROW):
        stat_copy(i).start()
    for i in (3, 2, 1):
        x_copy(i).start()

    @pl.when(is_root)
    def _():
        for i in (3, 2, 1):
            g_copy(i).start()
        x_all[pl.ds(pl.multiple_of(r * rows, rows), rows), :] = x_own[...]

    @pl.when(jnp.logical_not(is_root))
    def _():
        x_copy(0).start()

    lax.fori_loop(0, n_slots - n_chunks, fill_out, 0)

    for i in range(1, N_COL * N_ROW):
        other = (me + i) % (N_COL * N_ROW)
        pltpu.make_async_copy(stats.at[other], stats.at[other], s_recv.at[other]).wait()

    @pl.when(jnp.logical_not(is_root))
    def _():
        pltpu.make_async_copy(gain.at[r], gain.at[r], g_recv.at[0]).wait()

    for q in range(N_ROW):
        at = pl.ds(q * rows, rows)

        @pl.when(jnp.logical_not(jnp.logical_and(is_root, r == q)))
        def _():
            pltpu.make_async_copy(x_all.at[at], x_all.at[at], x_recv.at[q]).wait()

        whole = stats[q] + stats[N_ROW + q] + stats[2 * N_ROW + q] + stats[3 * N_ROW + q]
        whole = jnp.broadcast_to(whole, (rows, 128))
        mean = jnp.sum(jnp.where(lane == sub, whole, 0.0), axis=1, keepdims=True) / d_model
        mean_sq = jnp.sum(jnp.where(lane == sub + rows, whole, 0.0), axis=1, keepdims=True) / d_model
        inv = lax.rsqrt(mean_sq - mean * mean + NORM_EPS)
        z_ref[at, :] = ((x_all[at, :].astype(F32) - mean) * inv * gain[r]).astype(BF16)

    role_near = near == c
    role_far = far == c
    role_last = r == N_ROW - 1 - c

    def kind_phase(j):
        return (j + 4) % 5

    def at_root(j):
        return jnp.logical_or(kind_phase(j) == 0, kind_phase(j) == 2)

    def by_root(j):
        return jnp.logical_or(kind_phase(j) == 1, kind_phase(j) == 3)

    def direct(j):
        return kind_phase(j) == 4

    def near_copy(j):
        return remote(part.at[j], from_near.at[j], p_send.at[j], p_recv.at[j], c, near)

    def far_copy(j):
        return remote(part.at[j], from_far.at[j], p_send.at[j], f_recv.at[j], c, far)

    def passes(j):
        return jnp.logical_or(
            jnp.logical_and(at_root(j), role_far), jnp.logical_and(jnp.logical_not(at_root(j)), role_near)
        )

    def ends(j):
        return jnp.logical_or(
            jnp.logical_and(at_root(j), is_root), jnp.logical_and(jnp.logical_not(at_root(j)), role_last)
        )

    def gives(j):
        return jnp.logical_not(jnp.logical_or(passes(j), ends(j)))

    def pass_on(j):
        @pl.when(passes(j))
        def _():
            near_copy(j).wait_recv()
            part[j] = part[j] + from_near[j]
            far_copy(j).start()

    def up(j, _):
        wait_slot(j)
        total = jnp.dot(z_ref[:, pl.ds(0, blk)], ring[j, pl.ds(0, blk)], preferred_element_type=F32)
        for k in range(1, n_blk):
            at = pl.ds(k * blk, blk)
            total += jnp.dot(z_ref[:, at], ring[j, at], preferred_element_type=F32)
        part[j] = total

        @pl.when(j < 2 * n_chunks - n_slots)
        def _():
            load_out(j + n_slots - n_chunks, j)

        @pl.when(gives(j))
        def _():
            near_copy(j).start()

        @pl.when(j >= 1)
        def _():
            pass_on(j - 1)

        return 0

    lax.fori_loop(0, n_chunks, up, 0)
    pass_on(n_chunks - 1)

    inner = 1 + c % 2
    outer = (3 * c + 2) % 5
    inside = jnp.logical_or(c == 1, c == 2)
    forwards = jnp.logical_or(jnp.logical_and(c == 2, r < 2), jnp.logical_and(c == 1, r >= 2))

    def inner_copy(j):
        return remote(hid.at[j], hid.at[j], h_inner.at[j], h_recv.at[j], inner, r)

    def outer_copy(j):
        return remote(hid.at[j], hid.at[j], h_outer.at[j], h_recv.at[j], outer, r)

    def forward_copy(j):
        return remote(hid.at[j], hid.at[j], h_inner.at[j], h_recv.at[j], 3 * (c - 1), r)

    def last_copy(j, to):
        return remote(hid_sent.at[j], hid.at[j], w_send.at[to, j], h_recv.at[j], to, c)

    acc[...] = jnp.zeros_like(acc)
    early_lag = jnp.where(inside | is_root, 3, 6)
    late_lag = jnp.where(is_root, 3, early_lag + 3)

    def finish_sum(j):
        @pl.when(ends(j))
        def _():
            near_copy(j).wait_recv()
            far_copy(j).wait_recv()
            chunk = gelu_tanh(part[j] + from_near[j] + from_far[j]).astype(BF16)

            @pl.when(is_root)
            def _():
                hid[j] = chunk
                inner_copy(j).start()
                outer_copy(j).start()

            @pl.when(jnp.logical_not(is_root))
            def _():
                hid_sent[j] = chunk

                @pl.when(by_root(j))
                def _():
                    last_copy(j, c).start()

                @pl.when(direct(j))
                def _():
                    for to in range(N_COL):
                        last_copy(j, to).start()

    def use(j):
        @pl.when(jnp.logical_not(jnp.logical_and(is_root, at_root(j))))
        def _():
            inner_copy(j).wait_recv()

        @pl.when(jnp.logical_and(is_root, by_root(j)))
        def _():
            inner_copy(j).start()
            outer_copy(j).start()

        @pl.when(jnp.logical_and(forwards, jnp.logical_not(direct(j))))
        def _():
            forward_copy(j).start()

        slot = (n_chunks + j) % n_slots
        wait_slot(slot)
        for k in range(n_blk):
            at = pl.ds(k * blk, blk)
            acc[:, at] += jnp.dot(hid[j], ring[slot, at], preferred_element_type=F32)

    def down(t, _):
        @pl.when(t < n_chunks)
        def _():
            finish_sum(t)

        early = t - early_lag
        late = t - late_lag

        @pl.when(jnp.logical_and(early >= 0, early < n_chunks))
        def _():
            @pl.when(at_root(early))
            def _():
                use(early)

        @pl.when(jnp.logical_and(late >= 0, late < n_chunks))
        def _():
            @pl.when(jnp.logical_not(at_root(late)))
            def _():
                use(late)

        return 0

    lax.fori_loop(0, n_chunks + 9, down, 0)

    def near_part(i, k):
        other = near if i == 0 else (near + 2) % N_ROW
        at = pl.ds(k * blk, blk)
        return remote(
            acc.at[pl.ds(pl.multiple_of(other * rows, rows), rows), at], near_sum.at[i, :, at],
            n_send.at[i, k], n_recv.at[i, k], c, near,
        )

    def far_part(k):
        at = pl.ds(k * blk, blk)
        return remote(pair_sum.at[:, at], far_sum.at[:, at], o_send.at[k], o_recv.at[k], c, far)

    for i in (1, 0):
        for k in range(n_blk):
            near_part(i, k).start()
    for k in range(n_blk):
        at = pl.ds(k * blk, blk)
        near_part(1, k).wait_recv()
        pair_sum[:, at] = acc[pl.ds(pl.multiple_of(far * rows, rows), rows), at] + near_sum[1, :, at]
        far_part(k).start()
    for k in range(n_blk):
        at = pl.ds(k * blk, blk)
        near_part(0, k).wait_recv()
        far_part(k).wait_recv()
        own = acc[pl.ds(pl.multiple_of(r * rows, rows), rows), at] + near_sum[0, :, at] + far_sum[:, at]
        y_ref[:, at] = (x_own[:, at].astype(F32) + own).astype(BF16)

    for i in range(1, N_COL * N_ROW):
        stat_copy(i).wait_send()
    for i in (3, 2, 1):
        x_copy(i).wait_send()

    @pl.when(is_root)
    def _():
        for i in (3, 2, 1):
            g_copy(i).wait_send()

    @pl.when(jnp.logical_not(is_root))
    def _():
        x_copy(0).wait_send()

    def finish(j, _):
        @pl.when(jnp.logical_not(ends(j)))
        def _():
            near_copy(j).wait_send()

        @pl.when(jnp.logical_and(is_root, jnp.logical_not(direct(j))))
        def _():
            inner_copy(j).wait_send()
            outer_copy(j).wait_send()

        @pl.when(jnp.logical_and(forwards, jnp.logical_not(direct(j))))
        def _():
            forward_copy(j).wait_send()

        @pl.when(jnp.logical_and(role_last, by_root(j)))
        def _():
            last_copy(j, c).wait_send()

        @pl.when(jnp.logical_and(role_last, direct(j)))
        def _():
            for to in range(N_COL):
                last_copy(j, to).wait_send()

        return 0

    lax.fori_loop(0, n_chunks, finish, 0)
    for i in (1, 0):
        for k in range(n_blk):
            near_part(i, k).wait_send()
    for k in range(n_blk):
        far_part(k).wait_send()


def solution(mesh):
    def local_block(x_blk, gain_blk, w_in_blk, w_out_blk):
        rows, depth = x_blk.shape
        blk = depth // 4
        n_chunks = w_in_blk.shape[1] // blk
        n_slots = n_chunks + n_chunks // 2
        tokens = rows * N_ROW
        dma = pltpu.SemaphoreType.DMA
        n_all = N_COL * N_ROW
        return pl.pallas_call(
            functools.partial(mlp_kernel, n_chunks, n_slots, blk),
            out_shape=jax.ShapeDtypeStruct((rows, depth), BF16),
            in_specs=[pl.BlockSpec(memory_space=pl.ANY)] * 4,
            out_specs=pl.BlockSpec(memory_space=pltpu.VMEM),
            scratch_shapes=[
                pltpu.VMEM((rows, depth), BF16),
                pltpu.VMEM((N_COL, 1, depth), F32),
                pltpu.VMEM((n_all, 1, 128), F32),
                pltpu.VMEM((tokens, depth), BF16),
                pltpu.VMEM((tokens, depth), BF16),
                pltpu.VMEM((n_slots, depth, blk), BF16),
                pltpu.VMEM((n_chunks, tokens, blk), F32),
                pltpu.VMEM((n_chunks, tokens, blk), F32),
                pltpu.VMEM((n_chunks, tokens, blk), F32),
                pltpu.VMEM((n_chunks, tokens, blk), BF16),
                pltpu.VMEM((n_chunks, tokens, blk), BF16),
                pltpu.VMEM((tokens, depth), F32),
                pltpu.VMEM((2, rows, depth), F32),
                pltpu.VMEM((rows, depth), F32),
                pltpu.VMEM((rows, depth), F32),
                dma((2,)), dma((n_slots,)),
                dma((N_COL,)), dma((N_ROW,)), dma((N_COL,)), dma((1,)), dma((n_all,)), dma((n_all,)),
                dma((n_chunks,)), dma((n_chunks,)), dma((n_chunks,)),
                dma((n_chunks,)), dma((n_chunks,)), dma((n_chunks,)), dma((N_COL, n_chunks)),
                dma((2, depth // blk)), dma((2, depth // blk)), dma((depth // blk,)), dma((depth // blk,)),
            ],
            compiler_params=pltpu.CompilerParams(
                collective_id=0, has_side_effects=True, vmem_limit_bytes=67_000_000
            ),
        )(x_blk, gain_blk.reshape(1, depth), w_in_blk, w_out_blk)

    return jax.shard_map(
        local_block,
        mesh=mesh,
        in_specs=(P(("dp", "row"), "col"), P("col"), P("row", "col"), P("row", "col")),
        out_specs=P(("dp", "row"), "col"),
        check_vma=False,
    )
```

```python
import functools

import jax
import jax.numpy as jnp
from jax import lax
from jax.experimental import pallas as pl
from jax.experimental.pallas import tpu as pltpu
from jax.sharding import PartitionSpec as P

NORM_EPS = 1e-5
MESH = pl.DeviceIdType.MESH
BF16, F32 = jnp.bfloat16, jnp.float32
N_COL = 4
N_ROW = 4


def gelu_tanh(x):
    return x * (0.5 * (1.0 + jnp.tanh(0.7978845608028654 * (x + 0.044715 * (x * x * x)))))


def mlp_kernel(
    n_chunks, n_slots, blk,
    x_hbm, g_hbm, w_in_hbm, w_out_hbm, y_ref,
    x_own, gain, stats, x_all, z_ref, ring, part, from_near, from_far, hid, hid_sent, acc, near_sum, pair_sum, far_sum,
    x_load, w_load, x_send, x_recv, g_send, g_recv, s_send, s_recv, p_send, p_recv, f_recv,
    h_inner, h_outer, h_recv, w_send, n_send, n_recv, o_send, o_recv,
):
    dp, c, r = lax.axis_index("dp"), lax.axis_index("col"), lax.axis_index("row")
    rows = x_own.shape[0]
    n_blk = x_own.shape[1] // blk
    d_model = x_own.shape[1] * N_COL
    near = r + 1 - 2 * (r % 2)
    far = (r + 2) % N_ROW
    me = c * N_ROW + r
    is_root = c == r

    def remote(src, dst, send, recv, to_col, to_row):
        return pltpu.make_async_remote_copy(
            src_ref=src, dst_ref=dst, send_sem=send, recv_sem=recv,
            device_id=(dp, to_col, to_row), device_id_type=MESH,
        )

    def peer(i):
        other = (me + i) % (N_COL * N_ROW)
        return other // N_ROW, other % N_ROW

    x_cp = pltpu.make_async_copy(x_hbm, x_own, x_load.at[0])
    x_cp.start()
    g_cp = pltpu.make_async_copy(g_hbm, gain.at[c], x_load.at[1])
    g_cp.start()
    barrier = pltpu.get_barrier_semaphore()
    for i in range(1, N_COL * N_ROW):
        pc, pr = peer(i)
        pl.semaphore_signal(barrier, inc=1, device_id=(dp, pc, pr), device_id_type=MESH)

    def load_in(j, slot):
        pltpu.make_async_copy(
            w_in_hbm.at[:, pl.ds(pl.multiple_of(j * blk, blk), blk)], ring.at[slot], w_load.at[slot]
        ).start()

    def load_out(j, slot):
        for k in range(n_blk):
            pltpu.make_async_copy(
                w_out_hbm.at[pl.ds(pl.multiple_of(j * blk, blk), blk), pl.ds(k * blk, blk)],
                ring.at[slot, pl.ds(k * blk, blk)], w_load.at[slot],
            ).start()

    def wait_slot(slot):
        pltpu.make_async_copy(ring.at[slot], ring.at[slot], w_load.at[slot]).wait()

    def fill_in(j, _):
        load_in(j, j)
        return 0

    def fill_out(j, _):
        load_out(j, n_chunks + j)
        return 0

    lax.fori_loop(0, n_chunks, fill_in, 0)

    x_cp.wait()
    g_cp.wait()
    x_f32 = x_own[...].astype(F32)
    lane = lax.broadcasted_iota(jnp.int32, (rows, 128), 1)
    sub = lax.broadcasted_iota(jnp.int32, (rows, 128), 0)
    total = jnp.sum(x_f32, axis=1, keepdims=True)
    square = jnp.sum(x_f32 * x_f32, axis=1, keepdims=True)
    packed = jnp.where(lane == sub, total, 0.0) + jnp.where(lane == sub + rows, square, 0.0)
    stats[me] = jnp.sum(packed, axis=0, keepdims=True)

    pl.semaphore_wait(barrier, N_COL * N_ROW - 1)

    def stat_copy(i):
        pc, pr = peer(i)
        return remote(stats.at[me], stats.at[me], s_send.at[i], s_recv.at[me], pc, pr)

    def x_copy(i):
        return remote(x_own, x_all.at[pl.ds(r * rows, rows)], x_send.at[i], x_recv.at[r], (c + i) % N_COL, c)

    def g_copy(i):
        return remote(gain.at[c], gain.at[c], g_send.at[i], g_recv.at[0], (c + i) % N_COL, c)

    for i in range(1, N_COL * N_ROW):
        stat_copy(i).start()
    for i in (3, 2, 1):
        x_copy(i).start()

    @pl.when(is_root)
    def _():
        for i in (3, 2, 1):
            g_copy(i).start()
        x_all[pl.ds(pl.multiple_of(r * rows, rows), rows), :] = x_own[...]

    @pl.when(jnp.logical_not(is_root))
    def _():
        x_copy(0).start()

    lax.fori_loop(0, n_slots - n_chunks, fill_out, 0)

    for i in range(1, N_COL * N_ROW):
        other = (me + i) % (N_COL * N_ROW)
        pltpu.make_async_copy(stats.at[other], stats.at[other], s_recv.at[other]).wait()

    @pl.when(jnp.logical_not(is_root))
    def _():
        pltpu.make_async_copy(gain.at[r], gain.at[r], g_recv.at[0]).wait()

    for q in range(N_ROW):
        at = pl.ds(q * rows, rows)

        @pl.when(jnp.logical_not(jnp.logical_and(is_root, r == q)))
        def _():
            pltpu.make_async_copy(x_all.at[at], x_all.at[at], x_recv.at[q]).wait()

        whole = stats[q] + stats[N_ROW + q] + stats[2 * N_ROW + q] + stats[3 * N_ROW + q]
        whole = jnp.broadcast_to(whole, (rows, 128))
        mean = jnp.sum(jnp.where(lane == sub, whole, 0.0), axis=1, keepdims=True) / d_model
        mean_sq = jnp.sum(jnp.where(lane == sub + rows, whole, 0.0), axis=1, keepdims=True) / d_model
        inv = lax.rsqrt(mean_sq - mean * mean + NORM_EPS)
        z_ref[at, :] = ((x_all[at, :].astype(F32) - mean) * inv * gain[r]).astype(BF16)

    role_near = near == c
    role_far = far == c
    role_last = r == N_ROW - 1 - c

    def kind_phase(j):
        return (j + 4) % 5

    def at_root(j):
        return jnp.logical_or(kind_phase(j) == 0, kind_phase(j) == 2)

    def by_root(j):
        return jnp.logical_or(kind_phase(j) == 1, kind_phase(j) == 3)

    def direct(j):
        return kind_phase(j) == 4

    def near_copy(j):
        return remote(part.at[j], from_near.at[j], p_send.at[j], p_recv.at[j], c, near)

    def far_copy(j):
        return remote(part.at[j], from_far.at[j], p_send.at[j], f_recv.at[j], c, far)

    def passes(j):
        return jnp.logical_or(
            jnp.logical_and(at_root(j), role_far), jnp.logical_and(jnp.logical_not(at_root(j)), role_near)
        )

    def ends(j):
        return jnp.logical_or(
            jnp.logical_and(at_root(j), is_root), jnp.logical_and(jnp.logical_not(at_root(j)), role_last)
        )

    def gives(j):
        return jnp.logical_not(jnp.logical_or(passes(j), ends(j)))

    def pass_on(j):
        @pl.when(passes(j))
        def _():
            near_copy(j).wait_recv()
            part[j] = part[j] + from_near[j]
            far_copy(j).start()

    def up(j):
        wait_slot(j)
        total = jnp.dot(z_ref[:, pl.ds(0, blk)], ring[j, pl.ds(0, blk)], preferred_element_type=F32)
        for k in range(1, n_blk):
            at = pl.ds(k * blk, blk)
            total += jnp.dot(z_ref[:, at], ring[j, at], preferred_element_type=F32)
        part[j] = total

        @pl.when(j < 2 * n_chunks - n_slots)
        def _():
            load_out(j + n_slots - n_chunks, j)

        @pl.when(gives(j))
        def _():
            near_copy(j).start()


    inner = 1 + c % 2
    outer = (3 * c + 2) % 5
    inside = jnp.logical_or(c == 1, c == 2)
    forwards = jnp.logical_or(jnp.logical_and(c == 2, r < 2), jnp.logical_and(c == 1, r >= 2))

    def inner_copy(j):
        return remote(hid.at[j], hid.at[j], h_inner.at[j], h_recv.at[j], inner, r)

    def outer_copy(j):
        return remote(hid.at[j], hid.at[j], h_outer.at[j], h_recv.at[j], outer, r)

    def forward_copy(j):
        return remote(hid.at[j], hid.at[j], h_inner.at[j], h_recv.at[j], 3 * (c - 1), r)

    def last_copy(j, to):
        return remote(hid_sent.at[j], hid.at[j], w_send.at[to, j], h_recv.at[j], to, c)

    acc[...] = jnp.zeros_like(acc)
    sum_lag = (5 * n_chunks) // 8
    behind = 5
    early_lag = jnp.where(is_root, sum_lag + 2, jnp.where(role_last & jnp.logical_not(inside), n_chunks + behind, n_chunks))
    late_lag = jnp.where(is_root, sum_lag + behind, early_lag + behind)

    def finish_sum(j):
        @pl.when(ends(j))
        def _():
            near_copy(j).wait_recv()
            far_copy(j).wait_recv()
            chunk = gelu_tanh(part[j] + from_near[j] + from_far[j]).astype(BF16)

            @pl.when(is_root)
            def _():
                hid[j] = chunk
                inner_copy(j).start()
                outer_copy(j).start()

            @pl.when(jnp.logical_not(is_root))
            def _():
                hid_sent[j] = chunk

                @pl.when(by_root(j))
                def _():
                    last_copy(j, c).start()

                @pl.when(direct(j))
                def _():
                    for to in range(N_COL):
                        last_copy(j, to).start()

    def use(j):
        @pl.when(jnp.logical_not(jnp.logical_and(is_root, at_root(j))))
        def _():
            inner_copy(j).wait_recv()

        @pl.when(jnp.logical_and(is_root, by_root(j)))
        def _():
            inner_copy(j).start()
            outer_copy(j).start()

        @pl.when(jnp.logical_and(forwards, jnp.logical_not(direct(j))))
        def _():
            forward_copy(j).start()

        slot = (n_chunks + j) % n_slots
        wait_slot(slot)
        for k in range(n_blk):
            at = pl.ds(k * blk, blk)
            acc[:, at] += jnp.dot(hid[j], ring[slot, at], preferred_element_type=F32)

    def step(t, _):
        @pl.when(t < n_chunks)
        def _():
            up(t)

        @pl.when(jnp.logical_and(t >= 1, t <= n_chunks))
        def _():
            pass_on(t - 1)

        @pl.when(jnp.logical_and(t >= sum_lag, t < n_chunks + sum_lag))
        def _():
            finish_sum(t - sum_lag)

        early = t - early_lag
        late = t - late_lag

        @pl.when(jnp.logical_and(early >= 0, early < n_chunks))
        def _():
            @pl.when(at_root(early))
            def _():
                use(early)

        @pl.when(jnp.logical_and(late >= 0, late < n_chunks))
        def _():
            @pl.when(jnp.logical_not(at_root(late)))
            def _():
                use(late)

        return 0

    lax.fori_loop(0, 2 * n_chunks + 2 * behind, step, 0)

    def near_part(i, k):
        other = near if i == 0 else (near + 2) % N_ROW
        at = pl.ds(k * blk, blk)
        return remote(
            acc.at[pl.ds(pl.multiple_of(other * rows, rows), rows), at], near_sum.at[i, :, at],
            n_send.at[i, k], n_recv.at[i, k], c, near,
        )

    def far_part(k):
        at = pl.ds(k * blk, blk)
        return remote(pair_sum.at[:, at], far_sum.at[:, at], o_send.at[k], o_recv.at[k], c, far)

    for i in (1, 0):
        for k in range(n_blk):
            near_part(i, k).start()
    for k in range(n_blk):
        at = pl.ds(k * blk, blk)
        near_part(1, k).wait_recv()
        pair_sum[:, at] = acc[pl.ds(pl.multiple_of(far * rows, rows), rows), at] + near_sum[1, :, at]
        far_part(k).start()
    for i in range(1, N_COL * N_ROW):
        stat_copy(i).wait_send()
    for i in (3, 2, 1):
        x_copy(i).wait_send()

    @pl.when(is_root)
    def _():
        for i in (3, 2, 1):
            g_copy(i).wait_send()

    @pl.when(jnp.logical_not(is_root))
    def _():
        x_copy(0).wait_send()

    def finish(j, _):
        @pl.when(jnp.logical_not(ends(j)))
        def _():
            near_copy(j).wait_send()

        @pl.when(jnp.logical_and(is_root, jnp.logical_not(direct(j))))
        def _():
            inner_copy(j).wait_send()
            outer_copy(j).wait_send()

        @pl.when(jnp.logical_and(forwards, jnp.logical_not(direct(j))))
        def _():
            forward_copy(j).wait_send()

        @pl.when(jnp.logical_and(role_last, by_root(j)))
        def _():
            last_copy(j, c).wait_send()

        @pl.when(jnp.logical_and(role_last, direct(j)))
        def _():
            for to in range(N_COL):
                last_copy(j, to).wait_send()

        return 0

    lax.fori_loop(0, n_chunks, finish, 0)

    for k in range(n_blk):
        at = pl.ds(k * blk, blk)
        near_part(0, k).wait_recv()
        far_part(k).wait_recv()
        own = acc[pl.ds(pl.multiple_of(r * rows, rows), rows), at] + near_sum[0, :, at] + far_sum[:, at]
        y_ref[:, at] = (x_own[:, at].astype(F32) + own).astype(BF16)

    for i in (1, 0):
        for k in range(n_blk):
            near_part(i, k).wait_send()
    for k in range(n_blk):
        far_part(k).wait_send()


def solution(mesh):
    def local_block(x_blk, gain_blk, w_in_blk, w_out_blk):
        rows, depth = x_blk.shape
        blk = depth // 4
        n_chunks = w_in_blk.shape[1] // blk
        n_slots = n_chunks + n_chunks // 2
        tokens = rows * N_ROW
        dma = pltpu.SemaphoreType.DMA
        n_all = N_COL * N_ROW
        return pl.pallas_call(
            functools.partial(mlp_kernel, n_chunks, n_slots, blk),
            out_shape=jax.ShapeDtypeStruct((rows, depth), BF16),
            in_specs=[pl.BlockSpec(memory_space=pl.ANY)] * 4,
            out_specs=pl.BlockSpec(memory_space=pltpu.VMEM),
            scratch_shapes=[
                pltpu.VMEM((rows, depth), BF16),
                pltpu.VMEM((N_COL, 1, depth), F32),
                pltpu.VMEM((n_all, 1, 128), F32),
                pltpu.VMEM((tokens, depth), BF16),
                pltpu.VMEM((tokens, depth), BF16),
                pltpu.VMEM((n_slots, depth, blk), BF16),
                pltpu.VMEM((n_chunks, tokens, blk), F32),
                pltpu.VMEM((n_chunks, tokens, blk), F32),
                pltpu.VMEM((n_chunks, tokens, blk), F32),
                pltpu.VMEM((n_chunks, tokens, blk), BF16),
                pltpu.VMEM((n_chunks, tokens, blk), BF16),
                pltpu.VMEM((tokens, depth), F32),
                pltpu.VMEM((2, rows, depth), F32),
                pltpu.VMEM((rows, depth), F32),
                pltpu.VMEM((rows, depth), F32),
                dma((2,)), dma((n_slots,)),
                dma((N_COL,)), dma((N_ROW,)), dma((N_COL,)), dma((1,)), dma((n_all,)), dma((n_all,)),
                dma((n_chunks,)), dma((n_chunks,)), dma((n_chunks,)),
                dma((n_chunks,)), dma((n_chunks,)), dma((n_chunks,)), dma((N_COL, n_chunks)),
                dma((2, depth // blk)), dma((2, depth // blk)), dma((depth // blk,)), dma((depth // blk,)),
            ],
            compiler_params=pltpu.CompilerParams(
                collective_id=0, has_side_effects=True, vmem_limit_bytes=67_000_000
            ),
        )(x_blk, gain_blk.reshape(1, depth), w_in_blk, w_out_blk)

    return jax.shard_map(
        local_block,
        mesh=mesh,
        in_specs=(P(("dp", "row"), "col"), P("col"), P("row", "col"), P("row", "col")),
        out_specs=P(("dp", "row"), "col"),
        check_vma=False,
    )
```

```python
import functools

import jax
import jax.numpy as jnp
from jax import lax
from jax.experimental import pallas as pl
from jax.experimental.pallas import tpu as pltpu
from jax.sharding import PartitionSpec as P

NORM_EPS = 1e-5
MESH = pl.DeviceIdType.MESH
BF16, F32 = jnp.bfloat16, jnp.float32
N_COL = 4
N_ROW = 4
KINDS = (0, 1, 0, 1, 0, 2, 0, 1, 0, 2, 0, 1, 0, 2, 2, 2)


def gelu_tanh(x):
    return x * (0.5 * (1.0 + jnp.tanh(0.7978845608028654 * (x + 0.044715 * (x * x * x)))))


def mlp_kernel(
    n_chunks, n_slots, blk,
    x_hbm, g_hbm, w_in_hbm, w_out_hbm, y_hbm,
    x_own, gain, stats, x_all, z_ref, ring, part, from_near, from_far, hid, hid_sent, acc, near_sum, pair_sum, far_sum, y_ref,
    x_load, w_load, x_send, x_recv, g_send, g_recv, s_send, s_recv, p_send, p_recv, f_recv,
    h_inner, h_outer, h_recv, w_send, n_send, n_recv, o_send, o_recv, y_store,
):
    dp, c, r = lax.axis_index("dp"), lax.axis_index("col"), lax.axis_index("row")
    rows = x_own.shape[0]
    n_blk = x_own.shape[1] // blk
    d_model = x_own.shape[1] * N_COL
    near = r + 1 - 2 * (r % 2)
    far = (r + 2) % N_ROW
    me = c * N_ROW + r
    is_root = c == r

    def remote(src, dst, send, recv, to_col, to_row):
        return pltpu.make_async_remote_copy(
            src_ref=src, dst_ref=dst, send_sem=send, recv_sem=recv,
            device_id=(dp, to_col, to_row), device_id_type=MESH,
        )

    def peer(i):
        other = (me + i) % (N_COL * N_ROW)
        return other // N_ROW, other % N_ROW

    x_cp = pltpu.make_async_copy(x_hbm, x_own, x_load.at[0])
    x_cp.start()
    g_cp = pltpu.make_async_copy(g_hbm, gain.at[c], x_load.at[1])
    g_cp.start()
    barrier = pltpu.get_barrier_semaphore()
    for i in range(1, N_COL * N_ROW):
        pc, pr = peer(i)
        pl.semaphore_signal(barrier, inc=1, device_id=(dp, pc, pr), device_id_type=MESH)

    def load_in(j, slot):
        pltpu.make_async_copy(
            w_in_hbm.at[:, pl.ds(pl.multiple_of(j * blk, blk), blk)], ring.at[slot], w_load.at[slot]
        ).start()

    def load_out(j, slot):
        for k in range(n_blk):
            pltpu.make_async_copy(
                w_out_hbm.at[pl.ds(pl.multiple_of(j * blk, blk), blk), pl.ds(k * blk, blk)],
                ring.at[slot, pl.ds(k * blk, blk)], w_load.at[slot],
            ).start()

    def wait_slot(slot):
        pltpu.make_async_copy(ring.at[slot], ring.at[slot], w_load.at[slot]).wait()

    def fill_in(j, _):
        load_in(j, j)
        return 0

    def fill_out(j, _):
        load_out(j, n_chunks + j)
        return 0

    lax.fori_loop(0, n_chunks, fill_in, 0)

    x_cp.wait()
    g_cp.wait()
    x_f32 = x_own[...].astype(F32)
    lane = lax.broadcasted_iota(jnp.int32, (rows, 128), 1)
    sub = lax.broadcasted_iota(jnp.int32, (rows, 128), 0)
    total = jnp.sum(x_f32, axis=1, keepdims=True)
    square = jnp.sum(x_f32 * x_f32, axis=1, keepdims=True)
    packed = jnp.where(lane == sub, total, 0.0) + jnp.where(lane == sub + rows, square, 0.0)
    stats[me] = jnp.sum(packed, axis=0, keepdims=True)

    pl.semaphore_wait(barrier, N_COL * N_ROW - 1)

    def stat_copy(i):
        pc, pr = peer(i)
        return remote(stats.at[me], stats.at[me], s_send.at[i], s_recv.at[me], pc, pr)

    def far_first(i):
        if i == 0:
            return c
        if i == 3:
            return jnp.where(c < 2, 3, 0)
        if i == 2:
            return jnp.where(c < 2, 2, 1)
        return jnp.where(c < 2, 1 - c, 5 - c)

    def x_copy(i):
        return remote(x_own, x_all.at[pl.ds(r * rows, rows)], x_send.at[i], x_recv.at[r], far_first(i), c)

    def g_copy(i):
        return remote(gain.at[c], gain.at[c], g_send.at[i], g_recv.at[0], far_first(i), c)

    for i in range(1, N_COL * N_ROW):
        stat_copy(i).start()
    for i in (3, 2, 1):
        x_copy(i).start()

    @pl.when(is_root)
    def _():
        for i in (3, 2, 1):
            g_copy(i).start()
        x_all[pl.ds(pl.multiple_of(r * rows, rows), rows), :] = x_own[...]

    @pl.when(jnp.logical_not(is_root))
    def _():
        x_copy(0).start()

    lax.fori_loop(0, n_slots - n_chunks, fill_out, 0)

    for i in range(1, N_COL * N_ROW):
        other = (me + i) % (N_COL * N_ROW)
        pltpu.make_async_copy(stats.at[other], stats.at[other], s_recv.at[other]).wait()

    @pl.when(jnp.logical_not(is_root))
    def _():
        pltpu.make_async_copy(gain.at[r], gain.at[r], g_recv.at[0]).wait()

    for q in range(N_ROW):
        at = pl.ds(q * rows, rows)

        @pl.when(jnp.logical_not(jnp.logical_and(is_root, r == q)))
        def _():
            pltpu.make_async_copy(x_all.at[at], x_all.at[at], x_recv.at[q]).wait()

        whole = stats[q] + stats[N_ROW + q] + stats[2 * N_ROW + q] + stats[3 * N_ROW + q]
        whole = jnp.broadcast_to(whole, (rows, 128))
        mean = jnp.sum(jnp.where(lane == sub, whole, 0.0), axis=1, keepdims=True) / d_model
        mean_sq = jnp.sum(jnp.where(lane == sub + rows, whole, 0.0), axis=1, keepdims=True) / d_model
        inv = lax.rsqrt(mean_sq - mean * mean + NORM_EPS)
        z_ref[at, :] = ((x_all[at, :].astype(F32) - mean) * inv * gain[r]).astype(BF16)

    role_near = near == c
    role_far = far == c
    role_last = r == N_ROW - 1 - c

    def one_of(j, kind):
        found = [j == i for i in range(n_chunks) if KINDS[i % len(KINDS)] == kind]
        return functools.reduce(jnp.logical_or, found)

    def at_root(j):
        return one_of(j, 0)

    def by_root(j):
        return one_of(j, 1)

    def direct(j):
        return one_of(j, 2)

    def near_copy(j):
        return remote(part.at[j], from_near.at[j], p_send.at[j], p_recv.at[j], c, near)

    def far_copy(j):
        return remote(part.at[j], from_far.at[j], p_send.at[j], f_recv.at[j], c, far)

    def passes(j):
        return jnp.logical_or(
            jnp.logical_and(at_root(j), role_far), jnp.logical_and(jnp.logical_not(at_root(j)), role_near)
        )

    def ends(j):
        return jnp.logical_or(
            jnp.logical_and(at_root(j), is_root), jnp.logical_and(jnp.logical_not(at_root(j)), role_last)
        )

    def gives(j):
        return jnp.logical_not(jnp.logical_or(passes(j), ends(j)))

    def pass_on(j):
        @pl.when(passes(j))
        def _():
            near_copy(j).wait_recv()
            part[j] = part[j] + from_near[j]
            far_copy(j).start()

    def product(j):
        total = jnp.dot(z_ref[:, pl.ds(0, blk)], ring[j, pl.ds(0, blk)], preferred_element_type=F32)
        for k in range(1, n_blk):
            at = pl.ds(k * blk, blk)
            total += jnp.dot(z_ref[:, at], ring[j, at], preferred_element_type=F32)
        return total

    def up(i, _):
        pair = (2 * i, 2 * i + 1)
        for j in pair:
            wait_slot(j)
        totals = [product(j) for j in pair]
        for j, total in zip(pair, totals):
            part[j] = total
        for j in pair:
            @pl.when(gives(j))
            def _():
                near_copy(j).start()

        @pl.when(i < (2 * n_chunks - n_slots) // 2)
        def _():
            for j in pair:
                load_out(j + n_slots - n_chunks, j)

        @pl.when(i >= 1)
        def _():
            for j in pair:
                pass_on(j - 2)

        return 0

    lax.fori_loop(0, n_chunks // 2, up, 0)
    for j in (n_chunks - 2, n_chunks - 1):
        pass_on(j)

    inner = 1 + c % 2
    outer = (3 * c + 2) % 5
    inside = jnp.logical_or(c == 1, c == 2)
    forwards = jnp.logical_or(jnp.logical_and(c == 2, r < 2), jnp.logical_and(c == 1, r >= 2))

    def inner_copy(j):
        return remote(hid.at[j], hid.at[j], h_inner.at[j], h_recv.at[j], inner, r)

    def outer_copy(j):
        return remote(hid.at[j], hid.at[j], h_outer.at[j], h_recv.at[j], outer, r)

    def forward_copy(j):
        return remote(hid.at[j], hid.at[j], h_inner.at[j], h_recv.at[j], 3 * (c - 1), r)

    def last_copy(j, to):
        return remote(hid_sent.at[j], hid.at[j], w_send.at[to, j], h_recv.at[j], to, c)

    acc[...] = jnp.zeros_like(acc)
    behind = 3
    lag = jnp.where(is_root, 1, jnp.where(role_last, jnp.where(inside, n_chunks // 2, n_chunks), 0))
    root_lag = jnp.where(is_root, behind, lag + behind)
    direct_lag = jnp.where(is_root, n_chunks // 2, lag + behind)

    def finish_sum(j):
        @pl.when(ends(j))
        def _():
            near_copy(j).wait_recv()
            far_copy(j).wait_recv()
            chunk = gelu_tanh(part[j] + from_near[j] + from_far[j]).astype(BF16)

            @pl.when(is_root)
            def _():
                hid[j] = chunk
                inner_copy(j).start()
                outer_copy(j).start()

            @pl.when(jnp.logical_not(is_root))
            def _():
                hid_sent[j] = chunk

                @pl.when(by_root(j))
                def _():
                    last_copy(j, c).start()

                @pl.when(direct(j))
                def _():
                    for to in range(N_COL):
                        last_copy(j, to).start()

    def use(j):
        @pl.when(jnp.logical_not(jnp.logical_and(is_root, at_root(j))))
        def _():
            inner_copy(j).wait_recv()

        @pl.when(jnp.logical_and(is_root, by_root(j)))
        def _():
            inner_copy(j).start()
            outer_copy(j).start()

        @pl.when(jnp.logical_and(forwards, jnp.logical_not(direct(j))))
        def _():
            forward_copy(j).start()

        slot = (n_chunks + j) % n_slots
        wait_slot(slot)
        for k in range(n_blk):
            at = pl.ds(k * blk, blk)
            acc[:, at] += jnp.dot(hid[j], ring[slot, at], preferred_element_type=F32)

    def take(j, wanted):
        @pl.when(jnp.logical_and(j >= 0, j < n_chunks))
        def _():
            @pl.when(wanted(j))
            def _():
                use(j)

    def step(t, _):
        @pl.when(t < n_chunks)
        def _():
            finish_sum(t)

        take(t - lag, at_root)
        take(t - direct_lag, direct)
        take(t - root_lag, by_root)
        return 0

    lax.fori_loop(0, 2 * n_chunks + behind, step, 0)

    def near_part(i, k):
        other = near if i == 0 else (near + 2) % N_ROW
        at = pl.ds(k * blk, blk)
        return remote(
            acc.at[pl.ds(pl.multiple_of(other * rows, rows), rows), at], near_sum.at[i, :, at],
            n_send.at[i, k], n_recv.at[i, k], c, near,
        )

    def far_part(k):
        at = pl.ds(k * blk, blk)
        return remote(pair_sum.at[:, at], far_sum.at[:, at], o_send.at[k], o_recv.at[k], c, far)

    def store(k):
        at = pl.ds(k * blk, blk)
        return pltpu.make_async_copy(y_ref.at[:, at], y_hbm.at[:, at], y_store.at[k])

    for i in (1, 0):
        for k in range(n_blk):
            near_part(i, k).start()
    for k in range(n_blk):
        at = pl.ds(k * blk, blk)
        near_part(1, k).wait_recv()
        pair_sum[:, at] = acc[pl.ds(pl.multiple_of(far * rows, rows), rows), at] + near_sum[1, :, at]
        far_part(k).start()
    for i in range(1, N_COL * N_ROW):
        stat_copy(i).wait_send()
    for i in (3, 2, 1):
        x_copy(i).wait_send()

    @pl.when(is_root)
    def _():
        for i in (3, 2, 1):
            g_copy(i).wait_send()

    @pl.when(jnp.logical_not(is_root))
    def _():
        x_copy(0).wait_send()

    def finish(j, _):
        @pl.when(jnp.logical_not(ends(j)))
        def _():
            near_copy(j).wait_send()

        @pl.when(jnp.logical_and(is_root, jnp.logical_not(direct(j))))
        def _():
            inner_copy(j).wait_send()
            outer_copy(j).wait_send()

        @pl.when(jnp.logical_and(forwards, jnp.logical_not(direct(j))))
        def _():
            forward_copy(j).wait_send()

        @pl.when(jnp.logical_and(role_last, by_root(j)))
        def _():
            last_copy(j, c).wait_send()

        @pl.when(jnp.logical_and(role_last, direct(j)))
        def _():
            for to in range(N_COL):
                last_copy(j, to).wait_send()

        return 0

    lax.fori_loop(0, n_chunks, finish, 0)

    for k in range(n_blk):
        at = pl.ds(k * blk, blk)
        near_part(0, k).wait_recv()
        far_part(k).wait_recv()
        own = acc[pl.ds(pl.multiple_of(r * rows, rows), rows), at] + near_sum[0, :, at] + far_sum[:, at]
        y_ref[:, at] = (x_own[:, at].astype(F32) + own).astype(BF16)
        store(k).start()

    for i in (1, 0):
        for k in range(n_blk):
            near_part(i, k).wait_send()
    for k in range(n_blk):
        far_part(k).wait_send()
        store(k).wait()


def solution(mesh):
    def local_block(x_blk, gain_blk, w_in_blk, w_out_blk):
        rows, depth = x_blk.shape
        blk = depth // 4
        n_chunks = w_in_blk.shape[1] // blk
        n_slots = n_chunks + n_chunks // 2
        tokens = rows * N_ROW
        dma = pltpu.SemaphoreType.DMA
        n_all = N_COL * N_ROW
        return pl.pallas_call(
            functools.partial(mlp_kernel, n_chunks, n_slots, blk),
            out_shape=jax.ShapeDtypeStruct((rows, depth), BF16),
            in_specs=[pl.BlockSpec(memory_space=pl.ANY)] * 4,
            out_specs=pl.BlockSpec(memory_space=pl.ANY),
            scratch_shapes=[
                pltpu.VMEM((rows, depth), BF16),
                pltpu.VMEM((N_COL, 1, depth), F32),
                pltpu.VMEM((n_all, 1, 128), F32),
                pltpu.VMEM((tokens, depth), BF16),
                pltpu.VMEM((tokens, depth), BF16),
                pltpu.VMEM((n_slots, depth, blk), BF16),
                pltpu.VMEM((n_chunks, tokens, blk), F32),
                pltpu.VMEM((n_chunks, tokens, blk), F32),
                pltpu.VMEM((n_chunks, tokens, blk), F32),
                pltpu.VMEM((n_chunks, tokens, blk), BF16),
                pltpu.VMEM((n_chunks, tokens, blk), BF16),
                pltpu.VMEM((tokens, depth), F32),
                pltpu.VMEM((2, rows, depth), F32),
                pltpu.VMEM((rows, depth), F32),
                pltpu.VMEM((rows, depth), F32),
                pltpu.VMEM((rows, depth), BF16),
                dma((2,)), dma((n_slots,)),
                dma((N_COL,)), dma((N_ROW,)), dma((N_COL,)), dma((1,)), dma((n_all,)), dma((n_all,)),
                dma((n_chunks,)), dma((n_chunks,)), dma((n_chunks,)),
                dma((n_chunks,)), dma((n_chunks,)), dma((n_chunks,)), dma((N_COL, n_chunks)),
                dma((2, depth // blk)), dma((2, depth // blk)), dma((depth // blk,)), dma((depth // blk,)), dma((depth // blk,)),
            ],
            compiler_params=pltpu.CompilerParams(
                collective_id=0, has_side_effects=True, vmem_limit_bytes=67_000_000
            ),
        )(x_blk, gain_blk.reshape(1, depth), w_in_blk, w_out_blk)

    return jax.shard_map(
        local_block,
        mesh=mesh,
        in_specs=(P(("dp", "row"), "col"), P("col"), P("row", "col"), P("row", "col")),
        out_specs=P(("dp", "row"), "col"),
        check_vma=False,
    )
```

```python
import functools

import jax
import jax.numpy as jnp
from jax import lax
from jax.experimental import pallas as pl
from jax.experimental.pallas import tpu as pltpu
from jax.sharding import PartitionSpec as P

NORM_EPS = 1e-5
MESH = pl.DeviceIdType.MESH
BF16, F32 = jnp.bfloat16, jnp.float32
N_COL = 4
N_ROW = 4
KINDS = (0, 1, 0, 1, 0, 2, 0, 1, 0, 2, 0, 1, 0, 2, 2, 2)


def gelu_tanh(x):
    return x * (0.5 * (1.0 + jnp.tanh(0.7978845608028654 * (x + 0.044715 * (x * x * x)))))


def mlp_kernel(
    n_chunks, n_slots, blk,
    x_hbm, g_hbm, w_in_hbm, w_out_hbm, y_hbm,
    x_own, gain, stats, x_all, z_ref, ring, part, from_near, from_far, hid, hid_sent, acc, near_sum, pair_sum, far_sum, y_ref,
    x_load, w_load, x_send, x_recv, g_send, g_recv, s_send, s_recv, p_send, p_recv, f_recv,
    h_send, h_recv, w_send, n_send, n_recv, o_send, o_recv, y_store,
):
    dp, c, r = lax.axis_index("dp"), lax.axis_index("col"), lax.axis_index("row")
    rows = x_own.shape[0]
    n_blk = x_own.shape[1] // blk
    d_model = x_own.shape[1] * N_COL
    near = r + 1 - 2 * (r % 2)
    far = (r + 2) % N_ROW
    me = c * N_ROW + r
    is_root = c == r

    def remote(src, dst, send, recv, to_col, to_row):
        return pltpu.make_async_remote_copy(
            src_ref=src, dst_ref=dst, send_sem=send, recv_sem=recv,
            device_id=(dp, to_col, to_row), device_id_type=MESH,
        )

    def peer(i):
        other = (me + i) % (N_COL * N_ROW)
        return other // N_ROW, other % N_ROW

    x_cp = pltpu.make_async_copy(x_hbm, x_own, x_load.at[0])
    x_cp.start()
    g_cp = pltpu.make_async_copy(g_hbm, gain.at[c], x_load.at[1])
    g_cp.start()
    barrier = pltpu.get_barrier_semaphore()
    for i in range(1, N_COL * N_ROW):
        pc, pr = peer(i)
        pl.semaphore_signal(barrier, inc=1, device_id=(dp, pc, pr), device_id_type=MESH)

    def load_in(j, slot):
        pltpu.make_async_copy(
            w_in_hbm.at[:, pl.ds(pl.multiple_of(j * blk, blk), blk)], ring.at[slot], w_load.at[j // 4]
        ).start()

    def load_out(j, slot):
        for k in range(n_blk):
            pltpu.make_async_copy(
                w_out_hbm.at[pl.ds(pl.multiple_of(j * blk, blk), blk), pl.ds(k * blk, blk)],
                ring.at[slot, pl.ds(k * blk, blk)], w_load.at[n_chunks // 4 + j // n_half],
            ).start()

    n_half = n_chunks // 2

    def done(ref, sem):
        pltpu.make_async_copy(ref, ref, sem).wait()

    def fill_in(j, _):
        load_in(j, j)
        return 0

    def fill_out(j, _):
        load_out(j, n_chunks + j)
        return 0

    lax.fori_loop(0, n_chunks, fill_in, 0)

    x_cp.wait()
    g_cp.wait()
    x_f32 = x_own[...].astype(F32)
    lane = lax.broadcasted_iota(jnp.int32, (rows, 128), 1)
    sub = lax.broadcasted_iota(jnp.int32, (rows, 128), 0)
    total = jnp.sum(x_f32, axis=1, keepdims=True)
    square = jnp.sum(x_f32 * x_f32, axis=1, keepdims=True)
    packed = jnp.where(lane == sub, total, 0.0) + jnp.where(lane == sub + rows, square, 0.0)
    stats[me] = jnp.sum(packed, axis=0, keepdims=True)

    pl.semaphore_wait(barrier, N_COL * N_ROW - 1)

    def stat_copy(i):
        pc, pr = peer(i)
        return remote(stats.at[me], stats.at[me], s_send.at[0], s_recv.at[0], pc, pr)

    def far_first(i):
        if i == 0:
            return c
        if i == 3:
            return jnp.where(c < 2, 3, 0)
        if i == 2:
            return jnp.where(c < 2, 2, 1)
        return jnp.where(c < 2, 1 - c, 5 - c)

    def x_copy(i):
        return remote(x_own, x_all.at[pl.ds(r * rows, rows)], x_send.at[0], x_recv.at[0], far_first(i), c)

    def g_copy(i):
        return remote(gain.at[c], gain.at[c], g_send.at[0], g_recv.at[0], far_first(i), c)

    @pl.when(is_root)
    def _():
        for i in (3, 2, 1):
            g_copy(i).start()

    for i in range(1, N_COL * N_ROW):
        stat_copy(i).start()
    for i in (3, 2, 1):
        x_copy(i).start()

    @pl.when(is_root)
    def _():
        x_all[pl.ds(pl.multiple_of(r * rows, rows), rows), :] = x_own[...]

    @pl.when(jnp.logical_not(is_root))
    def _():
        x_copy(0).start()

    lax.fori_loop(0, n_slots - n_chunks, fill_out, 0)

    done(stats.at[pl.ds(0, N_COL * N_ROW - 1)], s_recv.at[0])

    @pl.when(is_root)
    def _():
        done(x_all.at[pl.ds(0, (N_ROW - 1) * rows)], x_recv.at[0])

    @pl.when(jnp.logical_not(is_root))
    def _():
        done(gain.at[0], g_recv.at[0])
        done(x_all, x_recv.at[0])

    for q in range(N_ROW):
        at = pl.ds(q * rows, rows)
        whole = stats[q] + stats[N_ROW + q] + stats[2 * N_ROW + q] + stats[3 * N_ROW + q]
        whole = jnp.broadcast_to(whole, (rows, 128))
        mean = jnp.sum(jnp.where(lane == sub, whole, 0.0), axis=1, keepdims=True) / d_model
        mean_sq = jnp.sum(jnp.where(lane == sub + rows, whole, 0.0), axis=1, keepdims=True) / d_model
        inv = lax.rsqrt(mean_sq - mean * mean + NORM_EPS)
        z_ref[at, :] = ((x_all[at, :].astype(F32) - mean) * inv * gain[r]).astype(BF16)

    role_near = near == c
    role_far = far == c
    role_last = r == N_ROW - 1 - c

    def one_of(j, kind):
        found = [j == i for i in range(n_chunks) if KINDS[i % len(KINDS)] == kind]
        return functools.reduce(jnp.logical_or, found)

    def at_root(j):
        return one_of(j, 0)

    def by_root(j):
        return one_of(j, 1)

    def direct(j):
        return one_of(j, 2)

    def near_copy(j):
        return remote(part.at[j], from_near.at[j], p_send.at[0], p_recv.at[j], c, near)

    def far_copy(j):
        return remote(part.at[j], from_far.at[j], p_send.at[0], f_recv.at[j], c, far)

    def passes(j):
        return jnp.logical_or(
            jnp.logical_and(at_root(j), role_far), jnp.logical_and(jnp.logical_not(at_root(j)), role_near)
        )

    def ends(j):
        return jnp.logical_or(
            jnp.logical_and(at_root(j), is_root), jnp.logical_and(jnp.logical_not(at_root(j)), role_last)
        )

    def gives(j):
        return jnp.logical_not(jnp.logical_or(passes(j), ends(j)))

    def pass_on(j):
        @pl.when(passes(j))
        def _():
            near_copy(j).wait_recv()
            part[j] = part[j] + from_near[j]
            far_copy(j).start()

    def product(j):
        total = jnp.dot(z_ref[:, pl.ds(0, blk)], ring[j, pl.ds(0, blk)], preferred_element_type=F32)
        for k in range(1, n_blk):
            at = pl.ds(k * blk, blk)
            total += jnp.dot(z_ref[:, at], ring[j, at], preferred_element_type=F32)
        return total

    def up(i, _):
        pair = (2 * i, 2 * i + 1)

        @pl.when(i % 2 == 0)
        def _():
            done(ring.at[pl.ds(0, 4)], w_load.at[i // 2])

        totals = [product(j) for j in pair]
        for j, total in zip(pair, totals):
            part[j] = total
        for j in pair:
            @pl.when(gives(j))
            def _():
                near_copy(j).start()

        @pl.when(i < (2 * n_chunks - n_slots) // 2)
        def _():
            for j in pair:
                load_out(j + n_slots - n_chunks, j)

        @pl.when(i >= 1)
        def _():
            for j in pair:
                pass_on(j - 2)

        return 0

    lax.fori_loop(0, n_chunks // 2, up, 0)
    for j in (n_chunks - 2, n_chunks - 1):
        pass_on(j)

    inner = 1 + c % 2
    outer = (3 * c + 2) % 5
    inside = jnp.logical_or(c == 1, c == 2)
    forwards = jnp.logical_or(jnp.logical_and(c == 2, r < 2), jnp.logical_and(c == 1, r >= 2))

    def inner_copy(j):
        return remote(hid.at[j], hid.at[j], h_send.at[0], h_recv.at[j], inner, r)

    def outer_copy(j):
        return remote(hid.at[j], hid.at[j], h_send.at[0], h_recv.at[j], outer, r)

    def forward_copy(j):
        return remote(hid.at[j], hid.at[j], h_send.at[0], h_recv.at[j], 3 * (c - 1), r)

    def last_copy(j, to):
        return remote(hid_sent.at[j], hid.at[j], w_send.at[0], h_recv.at[j], to, c)

    acc[...] = jnp.zeros_like(acc)
    behind = 3
    lag = jnp.where(is_root, 1, jnp.where(role_last, jnp.where(inside, n_chunks // 2, n_chunks), 0))
    root_lag = jnp.where(is_root, behind, lag + behind)
    direct_lag = jnp.where(is_root, 4, lag - 4)
    second_half = jnp.where(is_root, lag, direct_lag) + n_half
    done(ring.at[pl.ds(n_chunks, n_half)], w_load.at[n_chunks // 4])

    def finish_sum(j):
        @pl.when(ends(j))
        def _():
            near_copy(j).wait_recv()
            far_copy(j).wait_recv()
            chunk = gelu_tanh(part[j] + from_near[j] + from_far[j]).astype(BF16)

            @pl.when(is_root)
            def _():
                hid[j] = chunk
                inner_copy(j).start()
                outer_copy(j).start()

            @pl.when(jnp.logical_not(is_root))
            def _():
                hid_sent[j] = chunk

                @pl.when(by_root(j))
                def _():
                    last_copy(j, c).start()

                @pl.when(direct(j))
                def _():
                    for to in range(N_COL):
                        last_copy(j, to).start()

    def use(j):
        @pl.when(jnp.logical_not(jnp.logical_and(is_root, at_root(j))))
        def _():
            inner_copy(j).wait_recv()

        @pl.when(jnp.logical_and(is_root, by_root(j)))
        def _():
            inner_copy(j).start()
            outer_copy(j).start()

        @pl.when(jnp.logical_and(forwards, jnp.logical_not(direct(j))))
        def _():
            forward_copy(j).start()

        slot = (n_chunks + j) % n_slots
        for k in range(n_blk):
            at = pl.ds(k * blk, blk)
            acc[:, at] += jnp.dot(hid[j], ring[slot, at], preferred_element_type=F32)

    def take(j, wanted):
        @pl.when(jnp.logical_and(j >= 0, j < n_chunks))
        def _():
            @pl.when(wanted(j))
            def _():
                use(j)

    def step(t, _):
        @pl.when(t < n_chunks)
        def _():
            finish_sum(t)

        @pl.when(t == second_half)
        def _():
            done(ring.at[pl.ds(0, n_half)], w_load.at[n_chunks // 4 + 1])

        take(t - lag, at_root)
        take(t - direct_lag, direct)
        take(t - root_lag, by_root)
        return 0

    lax.fori_loop(0, 2 * n_chunks + behind, step, 0)

    def near_part(i, k):
        other = near if i == 0 else (near + 2) % N_ROW
        at = pl.ds(k * blk, blk)
        return remote(
            acc.at[pl.ds(pl.multiple_of(other * rows, rows), rows), at], near_sum.at[i, :, at],
            n_send.at[0], n_recv.at[i, k], c, near,
        )

    def far_part(k):
        at = pl.ds(k * blk, blk)
        return remote(pair_sum.at[:, at], far_sum.at[:, at], o_send.at[0], o_recv.at[k], c, far)

    def store(k):
        at = pl.ds(k * blk, blk)
        return pltpu.make_async_copy(y_ref.at[:, at], y_hbm.at[:, at], y_store.at[0])

    for i in (1, 0):
        for k in range(n_blk):
            near_part(i, k).start()
    for k in range(n_blk):
        at = pl.ds(k * blk, blk)
        near_part(1, k).wait_recv()
        pair_sum[:, at] = acc[pl.ds(pl.multiple_of(far * rows, rows), rows), at] + near_sum[1, :, at]
        far_part(k).start()
    count = [sum(KINDS[i % len(KINDS)] == kind for i in range(n_chunks)) for kind in range(3)]
    done(stats.at[pl.ds(0, N_COL * N_ROW - 1)], s_send.at[0])

    @pl.when(is_root)
    def _():
        done(gain.at[pl.ds(0, N_COL - 1)], g_send.at[0])
        done(x_all.at[pl.ds(0, (N_ROW - 1) * rows)], x_send.at[0])
        done(part.at[pl.ds(0, count[1] + count[2])], p_send.at[0])
        done(part.at[pl.ds(0, count[0] + count[1])], h_send.at[0])

    @pl.when(jnp.logical_not(is_root))
    def _():
        done(x_all, x_send.at[0])

    @pl.when(role_last)
    def _():
        done(part.at[pl.ds(0, count[0])], p_send.at[0])
        done(part.at[pl.ds(0, (count[1] + N_COL * count[2]) // 2)], w_send.at[0])

    @pl.when(jnp.logical_or(role_near, role_far))
    def _():
        done(part, p_send.at[0])

    @pl.when(forwards)
    def _():
        done(hid.at[pl.ds(0, count[0] + count[1])], h_send.at[0])

    for k in range(n_blk):
        at = pl.ds(k * blk, blk)
        near_part(0, k).wait_recv()
        far_part(k).wait_recv()
        own = acc[pl.ds(pl.multiple_of(r * rows, rows), rows), at] + near_sum[0, :, at] + far_sum[:, at]
        y_ref[:, at] = (x_own[:, at].astype(F32) + own).astype(BF16)
        store(k).start()

    done(near_sum, n_send.at[0])
    done(pair_sum, o_send.at[0])
    done(y_ref, y_store.at[0])


def solution(mesh):
    def local_block(x_blk, gain_blk, w_in_blk, w_out_blk):
        rows, depth = x_blk.shape
        blk = depth // 4
        n_chunks = w_in_blk.shape[1] // blk
        n_slots = n_chunks + n_chunks // 2
        tokens = rows * N_ROW
        dma = pltpu.SemaphoreType.DMA
        n_all = N_COL * N_ROW
        return pl.pallas_call(
            functools.partial(mlp_kernel, n_chunks, n_slots, blk),
            out_shape=jax.ShapeDtypeStruct((rows, depth), BF16),
            in_specs=[pl.BlockSpec(memory_space=pl.ANY)] * 4,
            out_specs=pl.BlockSpec(memory_space=pl.ANY),
            scratch_shapes=[
                pltpu.VMEM((rows, depth), BF16),
                pltpu.VMEM((N_COL, 1, depth), F32),
                pltpu.VMEM((n_all, 1, 128), F32),
                pltpu.VMEM((tokens, depth), BF16),
                pltpu.VMEM((tokens, depth), BF16),
                pltpu.VMEM((n_slots, depth, blk), BF16),
                pltpu.VMEM((n_chunks, tokens, blk), F32),
                pltpu.VMEM((n_chunks, tokens, blk), F32),
                pltpu.VMEM((n_chunks, tokens, blk), F32),
                pltpu.VMEM((n_chunks, tokens, blk), BF16),
                pltpu.VMEM((n_chunks, tokens, blk), BF16),
                pltpu.VMEM((tokens, depth), F32),
                pltpu.VMEM((2, rows, depth), F32),
                pltpu.VMEM((rows, depth), F32),
                pltpu.VMEM((rows, depth), F32),
                pltpu.VMEM((rows, depth), BF16),
                dma((2,)), dma((n_chunks // 4 + 2,)),
                dma((1,)), dma((1,)), dma((1,)), dma((1,)), dma((1,)), dma((1,)),
                dma((1,)), dma((n_chunks,)), dma((n_chunks,)),
                dma((1,)), dma((n_chunks,)), dma((1,)),
                dma((1,)), dma((2, depth // blk)), dma((1,)), dma((depth // blk,)), dma((1,)),
            ],
            compiler_params=pltpu.CompilerParams(
                collective_id=0, has_side_effects=True, vmem_limit_bytes=67_000_000
            ),
        )(x_blk, gain_blk.reshape(1, depth), w_in_blk, w_out_blk)

    return jax.shard_map(
        local_block,
        mesh=mesh,
        in_specs=(P(("dp", "row"), "col"), P("col"), P("row", "col"), P("row", "col")),
        out_specs=P(("dp", "row"), "col"),
        check_vma=False,
    )
```

```python
import functools

import jax
import jax.numpy as jnp
from jax import lax
from jax.experimental import pallas as pl
from jax.experimental.pallas import tpu as pltpu
from jax.sharding import PartitionSpec as P

NORM_EPS = 1e-5
MESH = pl.DeviceIdType.MESH
BF16, F32 = jnp.bfloat16, jnp.float32
N_COL = 4
N_ROW = 4
KINDS = (0, 1, 0, 1, 0, 1, 0, 1, 0, 0, 0, 2, 2, 2, 2, 2)


def gelu_tanh(x):
    return x * (0.5 * (1.0 + jnp.tanh(0.7978845608028654 * (x + 0.044715 * (x * x * x)))))


def mlp_kernel(
    n_chunks, n_slots, blk,
    x_hbm, g_hbm, w_in_hbm, w_out_hbm, y_hbm,
    x_own, gain, stats, x_all, z_ref, ring, part, from_near, from_far, hid, hid_sent, acc, near_sum, pair_sum, far_sum, y_ref,
    x_load, w_load, x_send, x_recv, g_send, g_recv, s_send, s_recv, p_send, p_recv, f_recv,
    h_send, h_recv, w_send, n_send, n_recv, o_send, o_recv, y_store,
):
    dp, c, r = lax.axis_index("dp"), lax.axis_index("col"), lax.axis_index("row")
    rows = x_own.shape[0]
    n_blk = x_own.shape[1] // blk
    d_model = x_own.shape[1] * N_COL
    near = r + 1 - 2 * (r % 2)
    far = (r + 2) % N_ROW
    me = c * N_ROW + r
    is_root = c == r

    def remote(src, dst, send, recv, to_col, to_row):
        return pltpu.make_async_remote_copy(
            src_ref=src, dst_ref=dst, send_sem=send, recv_sem=recv,
            device_id=(dp, to_col, to_row), device_id_type=MESH,
        )

    def peer(i):
        other = (me + i) % (N_COL * N_ROW)
        return other // N_ROW, other % N_ROW

    x_cp = pltpu.make_async_copy(x_hbm, x_own, x_load.at[0])
    x_cp.start()
    g_cp = pltpu.make_async_copy(g_hbm, gain.at[c], x_load.at[1])
    g_cp.start()
    barrier = pltpu.get_barrier_semaphore()
    for i in range(1, N_COL * N_ROW):
        pc, pr = peer(i)
        pl.semaphore_signal(barrier, inc=1, device_id=(dp, pc, pr), device_id_type=MESH)

    def load_in(j, slot):
        pltpu.make_async_copy(
            w_in_hbm.at[:, pl.ds(pl.multiple_of(j * blk, blk), blk)], ring.at[slot], w_load.at[j // 4]
        ).start()

    def load_out(j, slot):
        for k in range(n_blk):
            pltpu.make_async_copy(
                w_out_hbm.at[pl.ds(pl.multiple_of(j * blk, blk), blk), pl.ds(k * blk, blk)],
                ring.at[slot, pl.ds(k * blk, blk)], w_load.at[n_chunks // 4 + j // n_half],
            ).start()

    n_half = n_chunks // 2

    def done(ref, sem):
        pltpu.make_async_copy(ref, ref, sem).wait()

    def fill_in(j, _):
        load_in(j, j)
        return 0

    def fill_out(j, _):
        load_out(j, n_chunks + j)
        return 0

    lax.fori_loop(0, n_chunks, fill_in, 0)

    x_cp.wait()
    g_cp.wait()
    x_f32 = x_own[...].astype(F32)
    lane = lax.broadcasted_iota(jnp.int32, (rows, 128), 1)
    sub = lax.broadcasted_iota(jnp.int32, (rows, 128), 0)
    total = jnp.sum(x_f32, axis=1, keepdims=True)
    square = jnp.sum(x_f32 * x_f32, axis=1, keepdims=True)
    packed = jnp.where(lane == sub, total, 0.0) + jnp.where(lane == sub + rows, square, 0.0)
    stats[me] = jnp.sum(packed, axis=0, keepdims=True)

    pl.semaphore_wait(barrier, N_COL * N_ROW - 1)

    def stat_copy(i):
        pc, pr = peer(i)
        return remote(stats.at[me], stats.at[me], s_send.at[0], s_recv.at[0], pc, pr)

    def far_first(i):
        if i == 0:
            return c
        if i == 3:
            return jnp.where(c < 2, 3, 0)
        if i == 2:
            return jnp.where(c < 2, 2, 1)
        return jnp.where(c < 2, 1 - c, 5 - c)

    def x_copy(i):
        return remote(x_own, x_all.at[pl.ds(r * rows, rows)], x_send.at[0], x_recv.at[0], far_first(i), c)

    def g_copy(i):
        return remote(gain.at[c], gain.at[c], g_send.at[0], g_recv.at[0], far_first(i), c)

    @pl.when(is_root)
    def _():
        for i in (3, 2, 1):
            g_copy(i).start()

    for i in range(1, N_COL * N_ROW):
        stat_copy(i).start()
    for i in (3, 2, 1):
        x_copy(i).start()

    @pl.when(is_root)
    def _():
        x_all[pl.ds(pl.multiple_of(r * rows, rows), rows), :] = x_own[...]

    @pl.when(jnp.logical_not(is_root))
    def _():
        x_copy(0).start()

    lax.fori_loop(0, n_slots - n_chunks, fill_out, 0)

    done(stats.at[pl.ds(0, N_COL * N_ROW - 1)], s_recv.at[0])

    @pl.when(is_root)
    def _():
        done(x_all.at[pl.ds(0, (N_ROW - 1) * rows)], x_recv.at[0])

    @pl.when(jnp.logical_not(is_root))
    def _():
        done(gain.at[0], g_recv.at[0])
        done(x_all, x_recv.at[0])

    for q in range(N_ROW):
        at = pl.ds(q * rows, rows)
        whole = stats[q] + stats[N_ROW + q] + stats[2 * N_ROW + q] + stats[3 * N_ROW + q]
        whole = jnp.broadcast_to(whole, (rows, 128))
        mean = jnp.sum(jnp.where(lane == sub, whole, 0.0), axis=1, keepdims=True) / d_model
        mean_sq = jnp.sum(jnp.where(lane == sub + rows, whole, 0.0), axis=1, keepdims=True) / d_model
        inv = lax.rsqrt(mean_sq - mean * mean + NORM_EPS)
        z_ref[at, :] = ((x_all[at, :].astype(F32) - mean) * inv * gain[r]).astype(BF16)

    role_near = near == c
    role_far = far == c
    role_last = r == N_ROW - 1 - c

    def one_of(j, kind):
        found = [j == i for i in range(n_chunks) if KINDS[i % len(KINDS)] == kind]
        return functools.reduce(jnp.logical_or, found)

    def at_root(j):
        return one_of(j, 0)

    def by_root(j):
        return one_of(j, 1)

    def direct(j):
        return one_of(j, 2)

    def near_copy(j):
        return remote(part.at[j], from_near.at[j], p_send.at[0], p_recv.at[j], c, near)

    def far_copy(j):
        return remote(part.at[j], from_far.at[j], p_send.at[0], f_recv.at[j], c, far)

    def passes(j):
        return jnp.logical_or(
            jnp.logical_and(at_root(j), role_far), jnp.logical_and(jnp.logical_not(at_root(j)), role_near)
        )

    def ends(j):
        return jnp.logical_or(
            jnp.logical_and(at_root(j), is_root), jnp.logical_and(jnp.logical_not(at_root(j)), role_last)
        )

    def gives(j):
        return jnp.logical_not(jnp.logical_or(passes(j), ends(j)))

    def pass_on(j):
        @pl.when(passes(j))
        def _():
            near_copy(j).wait_recv()
            part[j] = part[j] + from_near[j]
            far_copy(j).start()

    def product(j):
        total = jnp.dot(z_ref[:, pl.ds(0, blk)], ring[j, pl.ds(0, blk)], preferred_element_type=F32)
        for k in range(1, n_blk):
            at = pl.ds(k * blk, blk)
            total += jnp.dot(z_ref[:, at], ring[j, at], preferred_element_type=F32)
        return total

    def up(i, _):
        pair = (2 * i, 2 * i + 1)

        @pl.when(i % 2 == 0)
        def _():
            done(ring.at[pl.ds(0, 4)], w_load.at[i // 2])

        totals = [product(j) for j in pair]
        for j, total in zip(pair, totals):
            part[j] = total
        for j in pair:
            @pl.when(gives(j))
            def _():
                near_copy(j).start()

        @pl.when(i < (2 * n_chunks - n_slots) // 2)
        def _():
            for j in pair:
                load_out(j + n_slots - n_chunks, j)

        @pl.when(i >= 1)
        def _():
            for j in pair:
                pass_on(j - 2)

        return 0

    lax.fori_loop(0, n_chunks // 2, up, 0)
    for j in (n_chunks - 2, n_chunks - 1):
        pass_on(j)

    inner = 1 + c % 2
    outer = (3 * c + 2) % 5
    inside = jnp.logical_or(c == 1, c == 2)
    forwards = jnp.logical_or(jnp.logical_and(c == 2, r < 2), jnp.logical_and(c == 1, r >= 2))

    def inner_copy(j):
        return remote(hid.at[j], hid.at[j], h_send.at[0], h_recv.at[j], inner, r)

    def outer_copy(j):
        return remote(hid.at[j], hid.at[j], h_send.at[0], h_recv.at[j], outer, r)

    def forward_copy(j):
        return remote(hid.at[j], hid.at[j], h_send.at[0], h_recv.at[j], 3 * (c - 1), r)

    def last_copy(j, to):
        return remote(hid_sent.at[j], hid.at[j], w_send.at[0], h_recv.at[j], to, c)

    acc[...] = jnp.zeros_like(acc)
    behind = 3
    lag = jnp.where(is_root, 1, jnp.where(role_last, jnp.where(inside, n_chunks // 2, n_chunks), 0))
    root_lag = jnp.where(is_root, behind, lag + behind)
    direct_lag = jnp.where(is_root, 4, lag - 4)
    second_half = jnp.where(is_root, lag, direct_lag) + n_half
    done(ring.at[pl.ds(n_chunks, n_half)], w_load.at[n_chunks // 4])

    def finish_sum(j):
        @pl.when(ends(j))
        def _():
            near_copy(j).wait_recv()
            far_copy(j).wait_recv()
            chunk = gelu_tanh(part[j] + from_near[j] + from_far[j]).astype(BF16)

            @pl.when(is_root)
            def _():
                hid[j] = chunk
                inner_copy(j).start()
                outer_copy(j).start()

            @pl.when(jnp.logical_not(is_root))
            def _():
                hid_sent[j] = chunk

                @pl.when(by_root(j))
                def _():
                    last_copy(j, c).start()

                @pl.when(direct(j))
                def _():
                    for to in range(N_COL):
                        last_copy(j, to).start()

    def use(j):
        @pl.when(jnp.logical_not(jnp.logical_and(is_root, at_root(j))))
        def _():
            inner_copy(j).wait_recv()

        @pl.when(jnp.logical_and(is_root, by_root(j)))
        def _():
            inner_copy(j).start()
            outer_copy(j).start()

        @pl.when(jnp.logical_and(forwards, jnp.logical_not(direct(j))))
        def _():
            forward_copy(j).start()

        slot = (n_chunks + j) % n_slots
        for k in range(n_blk):
            at = pl.ds(k * blk, blk)
            acc[:, at] += jnp.dot(hid[j], ring[slot, at], preferred_element_type=F32)

    def take(j, wanted):
        @pl.when(jnp.logical_and(j >= 0, j < n_chunks))
        def _():
            @pl.when(wanted(j))
            def _():
                use(j)

    def step(t, _):
        @pl.when(t < n_chunks)
        def _():
            finish_sum(t)

        @pl.when(t == second_half)
        def _():
            done(ring.at[pl.ds(0, n_half)], w_load.at[n_chunks // 4 + 1])

        take(t - lag, at_root)
        take(t - direct_lag, direct)
        take(t - root_lag, by_root)
        return 0

    lax.fori_loop(0, 2 * n_chunks + behind, step, 0)

    def near_part(i, k):
        other = near if i == 0 else (near + 2) % N_ROW
        at = pl.ds(k * blk, blk)
        return remote(
            acc.at[pl.ds(pl.multiple_of(other * rows, rows), rows), at], near_sum.at[i, :, at],
            n_send.at[0], n_recv.at[i, k], c, near,
        )

    def far_part(k):
        at = pl.ds(k * blk, blk)
        return remote(pair_sum.at[:, at], far_sum.at[:, at], o_send.at[0], o_recv.at[k], c, far)

    def store(k):
        at = pl.ds(k * blk, blk)
        return pltpu.make_async_copy(y_ref.at[:, at], y_hbm.at[:, at], y_store.at[0])

    for i in (1, 0):
        for k in range(n_blk):
            near_part(i, k).start()
    for k in range(n_blk):
        at = pl.ds(k * blk, blk)
        near_part(1, k).wait_recv()
        pair_sum[:, at] = acc[pl.ds(pl.multiple_of(far * rows, rows), rows), at] + near_sum[1, :, at]
        far_part(k).start()
    count = [sum(KINDS[i % len(KINDS)] == kind for i in range(n_chunks)) for kind in range(3)]
    done(stats.at[pl.ds(0, N_COL * N_ROW - 1)], s_send.at[0])

    @pl.when(is_root)
    def _():
        done(gain.at[pl.ds(0, N_COL - 1)], g_send.at[0])
        done(x_all.at[pl.ds(0, (N_ROW - 1) * rows)], x_send.at[0])
        done(part.at[pl.ds(0, count[1] + count[2])], p_send.at[0])
        done(part.at[pl.ds(0, count[0] + count[1])], h_send.at[0])

    @pl.when(jnp.logical_not(is_root))
    def _():
        done(x_all, x_send.at[0])

    @pl.when(role_last)
    def _():
        done(part.at[pl.ds(0, count[0])], p_send.at[0])
        done(part.at[pl.ds(0, (count[1] + N_COL * count[2]) // 2)], w_send.at[0])

    @pl.when(jnp.logical_or(role_near, role_far))
    def _():
        done(part, p_send.at[0])

    @pl.when(forwards)
    def _():
        done(hid.at[pl.ds(0, count[0] + count[1])], h_send.at[0])

    for k in range(n_blk):
        at = pl.ds(k * blk, blk)
        near_part(0, k).wait_recv()
        far_part(k).wait_recv()
        own = acc[pl.ds(pl.multiple_of(r * rows, rows), rows), at] + near_sum[0, :, at] + far_sum[:, at]
        y_ref[:, at] = (x_own[:, at].astype(F32) + own).astype(BF16)
        store(k).start()

    done(near_sum, n_send.at[0])
    done(pair_sum, o_send.at[0])
    done(y_ref, y_store.at[0])


def solution(mesh):
    def local_block(x_blk, gain_blk, w_in_blk, w_out_blk):
        rows, depth = x_blk.shape
        blk = depth // 4
        n_chunks = w_in_blk.shape[1] // blk
        n_slots = n_chunks + n_chunks // 2
        tokens = rows * N_ROW
        dma = pltpu.SemaphoreType.DMA
        n_all = N_COL * N_ROW
        return pl.pallas_call(
            functools.partial(mlp_kernel, n_chunks, n_slots, blk),
            out_shape=jax.ShapeDtypeStruct((rows, depth), BF16),
            in_specs=[pl.BlockSpec(memory_space=pl.ANY)] * 4,
            out_specs=pl.BlockSpec(memory_space=pl.ANY),
            scratch_shapes=[
                pltpu.VMEM((rows, depth), BF16),
                pltpu.VMEM((N_COL, 1, depth), F32),
                pltpu.VMEM((n_all, 1, 128), F32),
                pltpu.VMEM((tokens, depth), BF16),
                pltpu.VMEM((tokens, depth), BF16),
                pltpu.VMEM((n_slots, depth, blk), BF16),
                pltpu.VMEM((n_chunks, tokens, blk), F32),
                pltpu.VMEM((n_chunks, tokens, blk), F32),
                pltpu.VMEM((n_chunks, tokens, blk), F32),
                pltpu.VMEM((n_chunks, tokens, blk), BF16),
                pltpu.VMEM((n_chunks, tokens, blk), BF16),
                pltpu.VMEM((tokens, depth), F32),
                pltpu.VMEM((2, rows, depth), F32),
                pltpu.VMEM((rows, depth), F32),
                pltpu.VMEM((rows, depth), F32),
                pltpu.VMEM((rows, depth), BF16),
                dma((2,)), dma((n_chunks // 4 + 2,)),
                dma((1,)), dma((1,)), dma((1,)), dma((1,)), dma((1,)), dma((1,)),
                dma((1,)), dma((n_chunks,)), dma((n_chunks,)),
                dma((1,)), dma((n_chunks,)), dma((1,)),
                dma((1,)), dma((2, depth // blk)), dma((1,)), dma((depth // blk,)), dma((1,)),
            ],
            compiler_params=pltpu.CompilerParams(
                collective_id=0, has_side_effects=True, vmem_limit_bytes=67_000_000
            ),
        )(x_blk, gain_blk.reshape(1, depth), w_in_blk, w_out_blk)

    return jax.shard_map(
        local_block,
        mesh=mesh,
        in_specs=(P(("dp", "row"), "col"), P("col"), P("row", "col"), P("row", "col")),
        out_specs=P(("dp", "row"), "col"),
        check_vma=False,
    )
```

```python
import functools

import jax
import jax.numpy as jnp
from jax import lax
from jax.experimental import pallas as pl
from jax.experimental.pallas import tpu as pltpu
from jax.sharding import PartitionSpec as P

NORM_EPS = 1e-5
MESH = pl.DeviceIdType.MESH
BF16, F32 = jnp.bfloat16, jnp.float32
N_COL = 4
N_ROW = 4
KINDS = (0, 1, 0, 1, 0, 1, 0, 1, 0, 0, 0, 2, 2, 2, 2, 2)


def gelu_tanh(x):
    return x * (0.5 * (1.0 + jnp.tanh(0.7978845608028654 * (x + 0.044715 * (x * x * x)))))


def mlp_kernel(
    n_chunks, n_slots, blk,
    x_hbm, g_hbm, w_in_hbm, w_out_hbm, y_hbm,
    x_own, gain, stats, x_all, z_ref, ring, part, from_near, from_far, hid, hid_sent, acc, near_sum, pair_sum, far_sum, y_ref,
    x_load, w_load, x_send, x_recv, g_send, g_recv, s_send, s_recv, p_send, p_recv, f_recv,
    h_send, h_recv, w_send, n_send, n_recv, o_send, o_recv, y_store,
):
    dp, c, r = lax.axis_index("dp"), lax.axis_index("col"), lax.axis_index("row")
    rows = x_own.shape[0]
    n_blk = x_own.shape[1] // blk
    d_model = x_own.shape[1] * N_COL
    near = r + 1 - 2 * (r % 2)
    far = (r + 2) % N_ROW
    me = c * N_ROW + r
    is_root = c == r

    def remote(src, dst, send, recv, to_col, to_row):
        return pltpu.make_async_remote_copy(
            src_ref=src, dst_ref=dst, send_sem=send, recv_sem=recv,
            device_id=(dp, to_col, to_row), device_id_type=MESH,
        )

    def peer(i):
        other = (me + i) % (N_COL * N_ROW)
        return other // N_ROW, other % N_ROW

    x_cp = pltpu.make_async_copy(x_hbm, x_own, x_load.at[0])
    x_cp.start()
    g_cp = pltpu.make_async_copy(g_hbm, gain.at[c], x_load.at[1])
    g_cp.start()
    barrier = pltpu.get_barrier_semaphore()
    for i in range(1, N_COL * N_ROW):
        pc, pr = peer(i)
        pl.semaphore_signal(barrier, inc=1, device_id=(dp, pc, pr), device_id_type=MESH)

    def load_in(j, slot):
        pltpu.make_async_copy(
            w_in_hbm.at[:, pl.ds(pl.multiple_of(j * blk, blk), blk)], ring.at[slot], w_load.at[j // 4]
        ).start()

    def load_out(j, slot):
        for k in range(n_blk):
            pltpu.make_async_copy(
                w_out_hbm.at[pl.ds(pl.multiple_of(j * blk, blk), blk), pl.ds(k * blk, blk)],
                ring.at[slot, pl.ds(k * blk, blk)], w_load.at[n_chunks // 4 + j // n_half],
            ).start()

    n_half = n_chunks // 2

    def done(ref, sem):
        pltpu.make_async_copy(ref, ref, sem).wait()

    def fill_in(j, _):
        load_in(j, j)
        return 0

    def fill_out(j, _):
        load_out(j, n_chunks + j)
        return 0

    lax.fori_loop(0, n_chunks, fill_in, 0)

    x_cp.wait()
    g_cp.wait()
    x_f32 = x_own[...].astype(F32)
    lane = lax.broadcasted_iota(jnp.int32, (rows, 128), 1)
    sub = lax.broadcasted_iota(jnp.int32, (rows, 128), 0)
    total = jnp.sum(x_f32, axis=1, keepdims=True)
    square = jnp.sum(x_f32 * x_f32, axis=1, keepdims=True)
    packed = jnp.where(lane == sub, total, 0.0) + jnp.where(lane == sub + rows, square, 0.0)
    stats[me] = jnp.sum(packed, axis=0, keepdims=True)

    pl.semaphore_wait(barrier, N_COL * N_ROW - 1)

    def stat_copy(i):
        pc, pr = peer(i)
        return remote(stats.at[me], stats.at[me], s_send.at[0], s_recv.at[0], pc, pr)

    def far_first(i):
        if i == 0:
            return c
        if i == 3:
            return jnp.where(c < 2, 3, 0)
        if i == 2:
            return jnp.where(c < 2, 2, 1)
        return jnp.where(c < 2, 1 - c, 5 - c)

    def x_copy(i):
        return remote(x_own, x_all.at[pl.ds(r * rows, rows)], x_send.at[0], x_recv.at[0], far_first(i), c)

    def g_copy(i):
        return remote(gain.at[c], gain.at[c], g_send.at[0], g_recv.at[0], far_first(i), c)

    @pl.when(is_root)
    def _():
        for i in (3, 2, 1):
            g_copy(i).start()

    for i in range(1, N_COL * N_ROW):
        stat_copy(i).start()
    for i in (3, 2, 1):
        x_copy(i).start()

    @pl.when(is_root)
    def _():
        x_all[pl.ds(pl.multiple_of(r * rows, rows), rows), :] = x_own[...]

    @pl.when(jnp.logical_not(is_root))
    def _():
        x_copy(0).start()

    lax.fori_loop(0, n_slots - n_chunks, fill_out, 0)

    done(stats.at[pl.ds(0, N_COL * N_ROW - 1)], s_recv.at[0])

    @pl.when(is_root)
    def _():
        done(x_all.at[pl.ds(0, (N_ROW - 1) * rows)], x_recv.at[0])

    @pl.when(jnp.logical_not(is_root))
    def _():
        done(gain.at[0], g_recv.at[0])
        done(x_all, x_recv.at[0])

    for q in range(N_ROW):
        at = pl.ds(q * rows, rows)
        whole = stats[q] + stats[N_ROW + q] + stats[2 * N_ROW + q] + stats[3 * N_ROW + q]
        whole = jnp.broadcast_to(whole, (rows, 128))
        mean = jnp.sum(jnp.where(lane == sub, whole, 0.0), axis=1, keepdims=True) / d_model
        mean_sq = jnp.sum(jnp.where(lane == sub + rows, whole, 0.0), axis=1, keepdims=True) / d_model
        inv = lax.rsqrt(mean_sq - mean * mean + NORM_EPS)
        z_ref[at, :] = ((x_all[at, :].astype(F32) - mean) * inv * gain[r]).astype(BF16)

    role_near = near == c
    role_far = far == c
    role_last = r == N_ROW - 1 - c

    def one_of(j, kind):
        found = [j == i for i in range(n_chunks) if KINDS[i % len(KINDS)] == kind]
        return functools.reduce(jnp.logical_or, found)

    def at_root(j):
        return one_of(j, 0)

    def by_root(j):
        return one_of(j, 1)

    def direct(j):
        return one_of(j, 2)

    def near_copy(j):
        return remote(part.at[j], from_near.at[j], p_send.at[0], p_recv.at[j], c, near)

    def far_copy(j):
        return remote(part.at[j], from_far.at[j], p_send.at[0], f_recv.at[j], c, far)

    def passes(j):
        return jnp.logical_or(
            jnp.logical_and(at_root(j), role_far), jnp.logical_and(jnp.logical_not(at_root(j)), role_near)
        )

    def ends(j):
        return jnp.logical_or(
            jnp.logical_and(at_root(j), is_root), jnp.logical_and(jnp.logical_not(at_root(j)), role_last)
        )

    def gives(j):
        return jnp.logical_not(jnp.logical_or(passes(j), ends(j)))

    def pass_on(j):
        @pl.when(passes(j))
        def _():
            near_copy(j).wait_recv()
            part[j] = part[j] + from_near[j]
            far_copy(j).start()

    def product(j):
        total = jnp.dot(z_ref[:, pl.ds(0, blk)], ring[j, pl.ds(0, blk)], preferred_element_type=F32)
        for k in range(1, n_blk):
            at = pl.ds(k * blk, blk)
            total += jnp.dot(z_ref[:, at], ring[j, at], preferred_element_type=F32)
        return total

    def up(i, _):
        pair = (2 * i, 2 * i + 1)

        @pl.when(i % 2 == 0)
        def _():
            done(ring.at[pl.ds(0, 4)], w_load.at[i // 2])

        totals = [product(j) for j in pair]
        for j, total in zip(pair, totals):
            part[j] = total
        for j in pair:
            @pl.when(gives(j))
            def _():
                near_copy(j).start()

        @pl.when(i < (2 * n_chunks - n_slots) // 2)
        def _():
            for j in pair:
                load_out(j + n_slots - n_chunks, j)

        @pl.when(i >= 1)
        def _():
            for j in pair:
                pass_on(j - 2)

        return 0

    lax.fori_loop(0, n_chunks // 2, up, 0)
    for j in (n_chunks - 2, n_chunks - 1):
        pass_on(j)

    inner = 1 + c % 2
    outer = (3 * c + 2) % 5
    inside = jnp.logical_or(c == 1, c == 2)
    forwards = jnp.logical_or(jnp.logical_and(c == 2, r < 2), jnp.logical_and(c == 1, r >= 2))

    def inner_copy(j):
        return remote(hid.at[j], hid.at[j], h_send.at[0], h_recv.at[j], inner, r)

    def outer_copy(j):
        return remote(hid.at[j], hid.at[j], h_send.at[0], h_recv.at[j], outer, r)

    def forward_copy(j):
        return remote(hid.at[j], hid.at[j], h_send.at[0], h_recv.at[j], 3 * (c - 1), r)

    def last_copy(j, to):
        return remote(hid_sent.at[j], hid.at[j], w_send.at[0], h_recv.at[j], to, c)

    acc[...] = jnp.zeros_like(acc)
    behind = 3
    lag = jnp.where(is_root, 1, jnp.where(role_last, jnp.where(inside, 8, 9), 0))
    root_lag = jnp.where(is_root, behind, lag + behind)
    direct_lag = jnp.where(is_root, 4, lag - jnp.where(inside, 5, 7))
    second_half = jnp.where(is_root, lag, direct_lag) + n_half
    done(ring.at[pl.ds(n_chunks, n_half)], w_load.at[n_chunks // 4])

    def finish_sum(j):
        @pl.when(ends(j))
        def _():
            near_copy(j).wait_recv()
            far_copy(j).wait_recv()
            chunk = gelu_tanh(part[j] + from_near[j] + from_far[j]).astype(BF16)

            @pl.when(is_root)
            def _():
                hid[j] = chunk
                inner_copy(j).start()
                outer_copy(j).start()

            @pl.when(jnp.logical_not(is_root))
            def _():
                hid_sent[j] = chunk

                @pl.when(by_root(j))
                def _():
                    last_copy(j, c).start()

                @pl.when(direct(j))
                def _():
                    for to in range(N_COL):
                        last_copy(j, to).start()

    def use(j):
        @pl.when(jnp.logical_not(jnp.logical_and(is_root, at_root(j))))
        def _():
            inner_copy(j).wait_recv()

        @pl.when(jnp.logical_and(is_root, by_root(j)))
        def _():
            inner_copy(j).start()
            outer_copy(j).start()

        @pl.when(jnp.logical_and(forwards, jnp.logical_not(direct(j))))
        def _():
            forward_copy(j).start()

        slot = (n_chunks + j) % n_slots
        for k in range(n_blk):
            at = pl.ds(k * blk, blk)
            acc[:, at] += jnp.dot(hid[j], ring[slot, at], preferred_element_type=F32)

    def take(j, wanted):
        @pl.when(jnp.logical_and(j >= 0, j < n_chunks))
        def _():
            @pl.when(wanted(j))
            def _():
                use(j)

    def step(t, _):
        @pl.when(t < n_chunks)
        def _():
            finish_sum(t)

        @pl.when(t == second_half)
        def _():
            done(ring.at[pl.ds(0, n_half)], w_load.at[n_chunks // 4 + 1])

        take(t - lag, at_root)
        take(t - direct_lag, direct)
        take(t - root_lag, by_root)
        return 0

    lax.fori_loop(0, n_chunks + 9 + behind, step, 0)

    def near_part(i, k):
        other = near if i == 0 else (near + 2) % N_ROW
        at = pl.ds(k * blk, blk)
        return remote(
            acc.at[pl.ds(pl.multiple_of(other * rows, rows), rows), at], near_sum.at[i, :, at],
            n_send.at[0], n_recv.at[i, k], c, near,
        )

    def far_part(k):
        at = pl.ds(k * blk, blk)
        return remote(pair_sum.at[:, at], far_sum.at[:, at], o_send.at[0], o_recv.at[k], c, far)

    def store(k):
        at = pl.ds(k * blk, blk)
        return pltpu.make_async_copy(y_ref.at[:, at], y_hbm.at[:, at], y_store.at[0])

    for i in (1, 0):
        for k in range(n_blk):
            near_part(i, k).start()
    for k in range(n_blk):
        at = pl.ds(k * blk, blk)
        near_part(1, k).wait_recv()
        pair_sum[:, at] = acc[pl.ds(pl.multiple_of(far * rows, rows), rows), at] + near_sum[1, :, at]
        far_part(k).start()
    count = [sum(KINDS[i % len(KINDS)] == kind for i in range(n_chunks)) for kind in range(3)]
    done(stats.at[pl.ds(0, N_COL * N_ROW - 1)], s_send.at[0])

    @pl.when(is_root)
    def _():
        done(gain.at[pl.ds(0, N_COL - 1)], g_send.at[0])
        done(x_all.at[pl.ds(0, (N_ROW - 1) * rows)], x_send.at[0])
        done(part.at[pl.ds(0, count[1] + count[2])], p_send.at[0])
        done(part.at[pl.ds(0, count[0] + count[1])], h_send.at[0])

    @pl.when(jnp.logical_not(is_root))
    def _():
        done(x_all, x_send.at[0])

    @pl.when(role_last)
    def _():
        done(part.at[pl.ds(0, count[0])], p_send.at[0])
        done(part.at[pl.ds(0, (count[1] + N_COL * count[2]) // 2)], w_send.at[0])

    @pl.when(jnp.logical_or(role_near, role_far))
    def _():
        done(part, p_send.at[0])

    @pl.when(forwards)
    def _():
        done(hid.at[pl.ds(0, count[0] + count[1])], h_send.at[0])

    for k in range(n_blk):
        at = pl.ds(k * blk, blk)
        near_part(0, k).wait_recv()
        far_part(k).wait_recv()
        own = acc[pl.ds(pl.multiple_of(r * rows, rows), rows), at] + near_sum[0, :, at] + far_sum[:, at]
        y_ref[:, at] = (x_own[:, at].astype(F32) + own).astype(BF16)
        store(k).start()

    done(near_sum, n_send.at[0])
    done(pair_sum, o_send.at[0])
    done(y_ref, y_store.at[0])


def solution(mesh):
    def local_block(x_blk, gain_blk, w_in_blk, w_out_blk):
        rows, depth = x_blk.shape
        blk = depth // 4
        n_chunks = w_in_blk.shape[1] // blk
        n_slots = n_chunks + n_chunks // 2
        tokens = rows * N_ROW
        dma = pltpu.SemaphoreType.DMA
        n_all = N_COL * N_ROW
        return pl.pallas_call(
            functools.partial(mlp_kernel, n_chunks, n_slots, blk),
            out_shape=jax.ShapeDtypeStruct((rows, depth), BF16),
            in_specs=[pl.BlockSpec(memory_space=pl.ANY)] * 4,
            out_specs=pl.BlockSpec(memory_space=pl.ANY),
            scratch_shapes=[
                pltpu.VMEM((rows, depth), BF16),
                pltpu.VMEM((N_COL, 1, depth), F32),
                pltpu.VMEM((n_all, 1, 128), F32),
                pltpu.VMEM((tokens, depth), BF16),
                pltpu.VMEM((tokens, depth), BF16),
                pltpu.VMEM((n_slots, depth, blk), BF16),
                pltpu.VMEM((n_chunks, tokens, blk), F32),
                pltpu.VMEM((n_chunks, tokens, blk), F32),
                pltpu.VMEM((n_chunks, tokens, blk), F32),
                pltpu.VMEM((n_chunks, tokens, blk), BF16),
                pltpu.VMEM((n_chunks, tokens, blk), BF16),
                pltpu.VMEM((tokens, depth), F32),
                pltpu.VMEM((2, rows, depth), F32),
                pltpu.VMEM((rows, depth), F32),
                pltpu.VMEM((rows, depth), F32),
                pltpu.VMEM((rows, depth), BF16),
                dma((2,)), dma((n_chunks // 4 + 2,)),
                dma((1,)), dma((1,)), dma((1,)), dma((1,)), dma((1,)), dma((1,)),
                dma((1,)), dma((n_chunks,)), dma((n_chunks,)),
                dma((1,)), dma((n_chunks,)), dma((1,)),
                dma((1,)), dma((2, depth // blk)), dma((1,)), dma((depth // blk,)), dma((1,)),
            ],
            compiler_params=pltpu.CompilerParams(
                collective_id=0, has_side_effects=True, vmem_limit_bytes=67_000_000
            ),
        )(x_blk, gain_blk.reshape(1, depth), w_in_blk, w_out_blk)

    return jax.shard_map(
        local_block,
        mesh=mesh,
        in_specs=(P(("dp", "row"), "col"), P("col"), P("row", "col"), P("row", "col")),
        out_specs=P(("dp", "row"), "col"),
        check_vma=False,
    )
```

```python
import functools

import jax
import jax.numpy as jnp
from jax import lax
from jax.experimental import pallas as pl
from jax.experimental.pallas import tpu as pltpu
from jax.sharding import PartitionSpec as P

NORM_EPS = 1e-5
MESH = pl.DeviceIdType.MESH
BF16, F32 = jnp.bfloat16, jnp.float32
N_COL = 4
N_ROW = 4
KINDS = (0, 1, 0, 1, 0, 2, 0, 1, 0, 2, 0, 1, 0, 2, 2, 2)


def gelu_tanh(x):
    return x * (0.5 * (1.0 + jnp.tanh(0.7978845608028654 * (x + 0.044715 * (x * x * x)))))


def mlp_kernel(
    n_chunks, n_slots, blk,
    x_hbm, g_hbm, w_in_hbm, w_out_hbm, y_hbm,
    x_own, gain, stats, x_all, z_ref, ring, part, from_near, from_far, hid, hid_sent, acc, near_sum, pair_sum, far_sum, y_ref,
    x_load, w_load, x_send, x_recv, g_send, g_recv, s_send, s_recv, p_send, p_recv, f_recv,
    h_send, h_recv, w_send, n_send, n_recv, o_send, o_recv, y_store,
):
    dp, c, r = lax.axis_index("dp"), lax.axis_index("col"), lax.axis_index("row")
    rows = x_own.shape[0]
    n_blk = x_own.shape[1] // blk
    d_model = x_own.shape[1] * N_COL
    near = r + 1 - 2 * (r % 2)
    far = (r + 2) % N_ROW
    me = c * N_ROW + r
    is_root = c == r

    def remote(src, dst, send, recv, to_col, to_row):
        return pltpu.make_async_remote_copy(
            src_ref=src, dst_ref=dst, send_sem=send, recv_sem=recv,
            device_id=(dp, to_col, to_row), device_id_type=MESH,
        )

    def peer(i):
        other = (me + i) % (N_COL * N_ROW)
        return other // N_ROW, other % N_ROW

    x_cp = pltpu.make_async_copy(x_hbm, x_own, x_load.at[0])
    x_cp.start()
    g_cp = pltpu.make_async_copy(g_hbm, gain.at[c], x_load.at[1])
    g_cp.start()
    barrier = pltpu.get_barrier_semaphore()
    for i in range(1, N_COL * N_ROW):
        pc, pr = peer(i)
        pl.semaphore_signal(barrier, inc=1, device_id=(dp, pc, pr), device_id_type=MESH)

    tiles = blk // 128

    def load_in(j, slot):
        for k in range(tiles):
            pltpu.make_async_copy(
                w_in_hbm.at[:, pl.ds(pl.multiple_of(j * blk + k * 128, 128), 128)],
                ring.at[slot, k], w_load.at[j // 4],
            ).start()

    def load_out(j, slot):
        for k in range(n_blk):
            for m in range(tiles):
                pltpu.make_async_copy(
                    w_out_hbm.at[pl.ds(pl.multiple_of(j * blk, blk), blk), pl.ds(k * blk + m * 128, 128)],
                    ring.at[slot, m, pl.ds(k * blk, blk)], w_load.at[n_chunks // 4 + j // n_half],
                ).start()

    def weights(slot, k):
        at = pl.ds(k * blk, blk)
        return jnp.concatenate([ring[slot, m, at] for m in range(tiles)], axis=1)

    n_half = n_chunks // 2

    def done(ref, sem):
        pltpu.make_async_copy(ref, ref, sem).wait()

    def fill_in(j, _):
        load_in(j, j)
        return 0

    def fill_out(j, _):
        load_out(j, n_chunks + j)
        return 0

    lax.fori_loop(0, n_chunks, fill_in, 0)

    x_cp.wait()
    g_cp.wait()
    x_f32 = x_own[...].astype(F32)
    lane = lax.broadcasted_iota(jnp.int32, (rows, 128), 1)
    sub = lax.broadcasted_iota(jnp.int32, (rows, 128), 0)
    total = jnp.sum(x_f32, axis=1, keepdims=True)
    square = jnp.sum(x_f32 * x_f32, axis=1, keepdims=True)
    packed = jnp.where(lane == sub, total, 0.0) + jnp.where(lane == sub + rows, square, 0.0)
    stats[me] = jnp.sum(packed, axis=0, keepdims=True)

    pl.semaphore_wait(barrier, N_COL * N_ROW - 1)

    def stat_copy(i):
        pc, pr = peer(i)
        return remote(stats.at[me], stats.at[me], s_send.at[0], s_recv.at[0], pc, pr)

    def far_first(i):
        if i == 0:
            return c
        if i == 3:
            return jnp.where(c < 2, 3, 0)
        if i == 2:
            return jnp.where(c < 2, 2, 1)
        return jnp.where(c < 2, 1 - c, 5 - c)

    def x_copy(i):
        return remote(x_own, x_all.at[pl.ds(r * rows, rows)], x_send.at[0], x_recv.at[0], far_first(i), c)

    def g_copy(i):
        return remote(gain.at[c], gain.at[c], g_send.at[0], g_recv.at[0], far_first(i), c)

    @pl.when(is_root)
    def _():
        for i in (3, 2, 1):
            g_copy(i).start()

    for i in range(1, N_COL * N_ROW):
        stat_copy(i).start()
    for i in (3, 2, 1):
        x_copy(i).start()

    @pl.when(is_root)
    def _():
        x_all[pl.ds(pl.multiple_of(r * rows, rows), rows), :] = x_own[...]

    @pl.when(jnp.logical_not(is_root))
    def _():
        x_copy(0).start()

    lax.fori_loop(0, n_slots - n_chunks, fill_out, 0)

    done(stats.at[pl.ds(0, N_COL * N_ROW - 1)], s_recv.at[0])

    @pl.when(is_root)
    def _():
        done(x_all.at[pl.ds(0, (N_ROW - 1) * rows)], x_recv.at[0])

    @pl.when(jnp.logical_not(is_root))
    def _():
        done(gain.at[0], g_recv.at[0])
        done(x_all, x_recv.at[0])

    for q in range(N_ROW):
        at = pl.ds(q * rows, rows)
        whole = stats[q] + stats[N_ROW + q] + stats[2 * N_ROW + q] + stats[3 * N_ROW + q]
        whole = jnp.broadcast_to(whole, (rows, 128))
        mean = jnp.sum(jnp.where(lane == sub, whole, 0.0), axis=1, keepdims=True) / d_model
        mean_sq = jnp.sum(jnp.where(lane == sub + rows, whole, 0.0), axis=1, keepdims=True) / d_model
        inv = lax.rsqrt(mean_sq - mean * mean + NORM_EPS)
        z_ref[at, :] = ((x_all[at, :].astype(F32) - mean) * inv * gain[r]).astype(BF16)

    role_near = near == c
    role_far = far == c
    role_last = r == N_ROW - 1 - c

    def one_of(j, kind):
        found = [j == i for i in range(n_chunks) if KINDS[i % len(KINDS)] == kind]
        return functools.reduce(jnp.logical_or, found)

    def at_root(j):
        return one_of(j, 0)

    def by_root(j):
        return one_of(j, 1)

    def direct(j):
        return one_of(j, 2)

    def near_copy(j):
        return remote(part.at[j], from_near.at[j], p_send.at[0], p_recv.at[j], c, near)

    def far_copy(j):
        return remote(part.at[j], from_far.at[j], p_send.at[0], f_recv.at[j], c, far)

    def passes(j):
        return jnp.logical_or(
            jnp.logical_and(at_root(j), role_far), jnp.logical_and(jnp.logical_not(at_root(j)), role_near)
        )

    def ends(j):
        return jnp.logical_or(
            jnp.logical_and(at_root(j), is_root), jnp.logical_and(jnp.logical_not(at_root(j)), role_last)
        )

    def gives(j):
        return jnp.logical_not(jnp.logical_or(passes(j), ends(j)))

    def pass_on(j):
        @pl.when(passes(j))
        def _():
            near_copy(j).wait_recv()
            part[j] = part[j] + from_near[j]
            far_copy(j).start()

    def product(j):
        total = jnp.dot(z_ref[:, pl.ds(0, blk)], weights(j, 0), preferred_element_type=F32)
        for k in range(1, n_blk):
            total += jnp.dot(z_ref[:, pl.ds(k * blk, blk)], weights(j, k), preferred_element_type=F32)
        return total

    def up(i, _):
        pair = (2 * i, 2 * i + 1)

        @pl.when(i % 2 == 0)
        def _():
            done(ring.at[pl.ds(0, 4)], w_load.at[i // 2])

        totals = [product(j) for j in pair]
        for j, total in zip(pair, totals):
            part[j] = total
        for j in pair:
            @pl.when(gives(j))
            def _():
                near_copy(j).start()

        @pl.when(i < (2 * n_chunks - n_slots) // 2)
        def _():
            for j in pair:
                load_out(j + n_slots - n_chunks, j)

        @pl.when(i >= 1)
        def _():
            for j in pair:
                pass_on(j - 2)

        return 0

    lax.fori_loop(0, n_chunks // 2, up, 0)
    for j in (n_chunks - 2, n_chunks - 1):
        pass_on(j)

    inner = 1 + c % 2
    outer = (3 * c + 2) % 5
    inside = jnp.logical_or(c == 1, c == 2)
    forwards = jnp.logical_or(jnp.logical_and(c == 2, r < 2), jnp.logical_and(c == 1, r >= 2))

    def inner_copy(j):
        return remote(hid.at[j], hid.at[j], h_send.at[0], h_recv.at[j], inner, r)

    def outer_copy(j):
        return remote(hid.at[j], hid.at[j], h_send.at[0], h_recv.at[j], outer, r)

    def forward_copy(j):
        return remote(hid.at[j], hid.at[j], h_send.at[0], h_recv.at[j], 3 * (c - 1), r)

    def last_copy(j, to):
        return remote(hid_sent.at[j], hid.at[j], w_send.at[0], h_recv.at[j], to, c)

    acc[...] = jnp.zeros_like(acc)
    behind = 3
    lag = jnp.where(is_root, 1, jnp.where(role_last, jnp.where(inside, n_chunks // 2, n_chunks), 0))
    root_lag = jnp.where(is_root, behind, lag + behind)
    direct_lag = jnp.where(is_root, 4, lag - 4)
    second_half = jnp.where(is_root, lag, direct_lag) + n_half
    done(ring.at[pl.ds(n_chunks, n_half)], w_load.at[n_chunks // 4])

    def finish_sum(j):
        @pl.when(ends(j))
        def _():
            near_copy(j).wait_recv()
            far_copy(j).wait_recv()
            chunk = gelu_tanh(part[j] + from_near[j] + from_far[j]).astype(BF16)

            @pl.when(is_root)
            def _():
                hid[j] = chunk
                inner_copy(j).start()
                outer_copy(j).start()

            @pl.when(jnp.logical_not(is_root))
            def _():
                hid_sent[j] = chunk

                @pl.when(by_root(j))
                def _():
                    last_copy(j, c).start()

                @pl.when(direct(j))
                def _():
                    for to in range(N_COL):
                        last_copy(j, to).start()

    def use(j):
        @pl.when(jnp.logical_not(jnp.logical_and(is_root, at_root(j))))
        def _():
            inner_copy(j).wait_recv()

        @pl.when(jnp.logical_and(is_root, by_root(j)))
        def _():
            inner_copy(j).start()
            outer_copy(j).start()

        @pl.when(jnp.logical_and(forwards, jnp.logical_not(direct(j))))
        def _():
            forward_copy(j).start()

        slot = (n_chunks + j) % n_slots
        for k in range(n_blk):
            at = pl.ds(k * blk, blk)
            acc[:, at] += jnp.dot(hid[j], weights(slot, k), preferred_element_type=F32)

    def take(j, wanted):
        @pl.when(jnp.logical_and(j >= 0, j < n_chunks))
        def _():
            @pl.when(wanted(j))
            def _():
                use(j)

    def step(t, _):
        @pl.when(t < n_chunks)
        def _():
            finish_sum(t)

        @pl.when(t == second_half)
        def _():
            done(ring.at[pl.ds(0, n_half)], w_load.at[n_chunks // 4 + 1])

        take(t - lag, at_root)
        take(t - direct_lag, direct)
        take(t - root_lag, by_root)
        return 0

    lax.fori_loop(0, 2 * n_chunks + behind, step, 0)

    def near_part(i, k):
        other = near if i == 0 else (near + 2) % N_ROW
        at = pl.ds(k * blk, blk)
        return remote(
            acc.at[pl.ds(pl.multiple_of(other * rows, rows), rows), at], near_sum.at[i, :, at],
            n_send.at[0], n_recv.at[i, k], c, near,
        )

    def far_part(k):
        at = pl.ds(k * blk, blk)
        return remote(pair_sum.at[:, at], far_sum.at[:, at], o_send.at[0], o_recv.at[k], c, far)

    def store(k):
        at = pl.ds(k * blk, blk)
        return pltpu.make_async_copy(y_ref.at[:, at], y_hbm.at[:, at], y_store.at[0])

    for i in (1, 0):
        for k in range(n_blk):
            near_part(i, k).start()
    for k in range(n_blk):
        at = pl.ds(k * blk, blk)
        near_part(1, k).wait_recv()
        pair_sum[:, at] = acc[pl.ds(pl.multiple_of(far * rows, rows), rows), at] + near_sum[1, :, at]
        far_part(k).start()
    count = [sum(KINDS[i % len(KINDS)] == kind for i in range(n_chunks)) for kind in range(3)]
    done(stats.at[pl.ds(0, N_COL * N_ROW - 1)], s_send.at[0])

    @pl.when(is_root)
    def _():
        done(gain.at[pl.ds(0, N_COL - 1)], g_send.at[0])
        done(x_all.at[pl.ds(0, (N_ROW - 1) * rows)], x_send.at[0])
        done(part.at[pl.ds(0, count[1] + count[2])], p_send.at[0])
        done(part.at[pl.ds(0, count[0] + count[1])], h_send.at[0])

    @pl.when(jnp.logical_not(is_root))
    def _():
        done(x_all, x_send.at[0])

    @pl.when(role_last)
    def _():
        done(part.at[pl.ds(0, count[0])], p_send.at[0])
        done(part.at[pl.ds(0, (count[1] + N_COL * count[2]) // 2)], w_send.at[0])

    @pl.when(jnp.logical_or(role_near, role_far))
    def _():
        done(part, p_send.at[0])

    @pl.when(forwards)
    def _():
        done(hid.at[pl.ds(0, count[0] + count[1])], h_send.at[0])

    for k in range(n_blk):
        at = pl.ds(k * blk, blk)
        near_part(0, k).wait_recv()
        far_part(k).wait_recv()
        own = acc[pl.ds(pl.multiple_of(r * rows, rows), rows), at] + near_sum[0, :, at] + far_sum[:, at]
        y_ref[:, at] = (x_own[:, at].astype(F32) + own).astype(BF16)
        store(k).start()

    done(near_sum, n_send.at[0])
    done(pair_sum, o_send.at[0])
    done(y_ref, y_store.at[0])


def solution(mesh):
    def local_block(x_blk, gain_blk, w_in_blk, w_out_blk):
        rows, depth = x_blk.shape
        blk = depth // 4
        n_chunks = w_in_blk.shape[1] // blk
        n_slots = n_chunks + n_chunks // 2
        tokens = rows * N_ROW
        dma = pltpu.SemaphoreType.DMA
        n_all = N_COL * N_ROW
        return pl.pallas_call(
            functools.partial(mlp_kernel, n_chunks, n_slots, blk),
            out_shape=jax.ShapeDtypeStruct((rows, depth), BF16),
            in_specs=[pl.BlockSpec(memory_space=pl.ANY)] * 4,
            out_specs=pl.BlockSpec(memory_space=pl.ANY),
            scratch_shapes=[
                pltpu.VMEM((rows, depth), BF16),
                pltpu.VMEM((N_COL, 1, depth), F32),
                pltpu.VMEM((n_all, 1, 128), F32),
                pltpu.VMEM((tokens, depth), BF16),
                pltpu.VMEM((tokens, depth), BF16),
                pltpu.VMEM((n_slots, blk // 128, depth, 128), BF16),
                pltpu.VMEM((n_chunks, tokens, blk), F32),
                pltpu.VMEM((n_chunks, tokens, blk), F32),
                pltpu.VMEM((n_chunks, tokens, blk), F32),
                pltpu.VMEM((n_chunks, tokens, blk), BF16),
                pltpu.VMEM((n_chunks, tokens, blk), BF16),
                pltpu.VMEM((tokens, depth), F32),
                pltpu.VMEM((2, rows, depth), F32),
                pltpu.VMEM((rows, depth), F32),
                pltpu.VMEM((rows, depth), F32),
                pltpu.VMEM((rows, depth), BF16),
                dma((2,)), dma((n_chunks // 4 + 2,)),
                dma((1,)), dma((1,)), dma((1,)), dma((1,)), dma((1,)), dma((1,)),
                dma((1,)), dma((n_chunks,)), dma((n_chunks,)),
                dma((1,)), dma((n_chunks,)), dma((1,)),
                dma((1,)), dma((2, depth // blk)), dma((1,)), dma((depth // blk,)), dma((1,)),
            ],
            compiler_params=pltpu.CompilerParams(
                collective_id=0, has_side_effects=True, vmem_limit_bytes=67_000_000
            ),
        )(x_blk, gain_blk.reshape(1, depth), w_in_blk, w_out_blk)

    return jax.shard_map(
        local_block,
        mesh=mesh,
        in_specs=(P(("dp", "row"), "col"), P("col"), P("row", "col"), P("row", "col")),
        out_specs=P(("dp", "row"), "col"),
        check_vma=False,
    )
```

```python
import functools

import jax
import jax.numpy as jnp
from jax import lax
from jax.experimental import pallas as pl
from jax.experimental.pallas import tpu as pltpu
from jax.sharding import PartitionSpec as P

NORM_EPS = 1e-5
MESH = pl.DeviceIdType.MESH
BF16, F32 = jnp.bfloat16, jnp.float32
N_COL = 4
N_ROW = 4
KINDS = (0, 1, 0, 0, 1, 0, 2, 0, 0, 1, 0, 2, 0, 1, 0, 2)


def gelu_tanh(x):
    return x * (0.5 * (1.0 + jnp.tanh(0.7978845608028654 * (x + 0.044715 * (x * x * x)))))


def mlp_kernel(
    n_chunks, n_slots, blk,
    x_hbm, g_hbm, w_in_hbm, w_out_hbm, y_hbm,
    x_own, gain, stats, x_all, z_ref, ring, part, from_near, from_far, hid, hid_sent, acc, near_sum, pair_sum, far_sum, y_ref,
    x_load, w_load, x_send, x_recv, g_send, g_recv, s_send, s_recv, p_send, p_recv, f_recv,
    h_send, h_recv, w_send, n_send, n_recv, o_send, o_recv, y_store,
):
    dp, c, r = lax.axis_index("dp"), lax.axis_index("col"), lax.axis_index("row")
    rows = x_own.shape[0]
    n_blk = x_own.shape[1] // blk
    d_model = x_own.shape[1] * N_COL
    near = r + 1 - 2 * (r % 2)
    far = (r + 2) % N_ROW
    me = c * N_ROW + r
    is_root = c == r

    def remote(src, dst, send, recv, to_col, to_row):
        return pltpu.make_async_remote_copy(
            src_ref=src, dst_ref=dst, send_sem=send, recv_sem=recv,
            device_id=(dp, to_col, to_row), device_id_type=MESH,
        )

    def peer(i):
        other = (me + i) % (N_COL * N_ROW)
        return other // N_ROW, other % N_ROW

    x_cp = pltpu.make_async_copy(x_hbm, x_own, x_load.at[0])
    x_cp.start()
    g_cp = pltpu.make_async_copy(g_hbm, gain.at[c], x_load.at[1])
    g_cp.start()
    barrier = pltpu.get_barrier_semaphore()
    for i in range(1, N_COL * N_ROW):
        pc, pr = peer(i)
        pl.semaphore_signal(barrier, inc=1, device_id=(dp, pc, pr), device_id_type=MESH)

    def load_in(j, slot):
        pltpu.make_async_copy(
            w_in_hbm.at[:, pl.ds(pl.multiple_of(j * blk, blk), blk)], ring.at[slot], w_load.at[j // 4]
        ).start()

    def load_out(j, slot):
        for k in range(n_blk):
            pltpu.make_async_copy(
                w_out_hbm.at[pl.ds(pl.multiple_of(j * blk, blk), blk), pl.ds(k * blk, blk)],
                ring.at[slot, pl.ds(k * blk, blk)], w_load.at[n_chunks // 4 + j // n_half],
            ).start()

    n_half = n_chunks // 2

    def done(ref, sem):
        pltpu.make_async_copy(ref, ref, sem).wait()

    def fill_in(j, _):
        load_in(j, j)
        return 0

    def fill_out(j, _):
        load_out(j, n_chunks + j)
        return 0

    lax.fori_loop(0, n_chunks, fill_in, 0)

    x_cp.wait()
    g_cp.wait()
    x_f32 = x_own[...].astype(F32)
    lane = lax.broadcasted_iota(jnp.int32, (rows, 128), 1)
    sub = lax.broadcasted_iota(jnp.int32, (rows, 128), 0)
    total = jnp.sum(x_f32, axis=1, keepdims=True)
    square = jnp.sum(x_f32 * x_f32, axis=1, keepdims=True)
    packed = jnp.where(lane == sub, total, 0.0) + jnp.where(lane == sub + rows, square, 0.0)
    stats[me] = jnp.sum(packed, axis=0, keepdims=True)

    pl.semaphore_wait(barrier, N_COL * N_ROW - 1)

    def stat_copy(i):
        pc, pr = peer(i)
        return remote(stats.at[me], stats.at[me], s_send.at[0], s_recv.at[0], pc, pr)

    def far_first(i):
        if i == 0:
            return c
        if i == 3:
            return jnp.where(c < 2, 3, 0)
        if i == 2:
            return jnp.where(c < 2, 2, 1)
        return jnp.where(c < 2, 1 - c, 5 - c)

    def x_copy(i):
        return remote(x_own, x_all.at[pl.ds(r * rows, rows)], x_send.at[0], x_recv.at[0], far_first(i), c)

    def g_copy(i):
        return remote(gain.at[c], gain.at[c], g_send.at[0], g_recv.at[0], far_first(i), c)

    @pl.when(is_root)
    def _():
        for i in (3, 2, 1):
            g_copy(i).start()

    for i in range(1, N_COL * N_ROW):
        stat_copy(i).start()
    for i in (3, 2, 1):
        x_copy(i).start()

    @pl.when(is_root)
    def _():
        x_all[pl.ds(pl.multiple_of(r * rows, rows), rows), :] = x_own[...]

    @pl.when(jnp.logical_not(is_root))
    def _():
        x_copy(0).start()

    lax.fori_loop(0, n_slots - n_chunks, fill_out, 0)

    done(stats.at[pl.ds(0, N_COL * N_ROW - 1)], s_recv.at[0])

    @pl.when(is_root)
    def _():
        done(x_all.at[pl.ds(0, (N_ROW - 1) * rows)], x_recv.at[0])

    @pl.when(jnp.logical_not(is_root))
    def _():
        done(gain.at[0], g_recv.at[0])
        done(x_all, x_recv.at[0])

    for q in range(N_ROW):
        at = pl.ds(q * rows, rows)
        whole = stats[q] + stats[N_ROW + q] + stats[2 * N_ROW + q] + stats[3 * N_ROW + q]
        whole = jnp.broadcast_to(whole, (rows, 128))
        mean = jnp.sum(jnp.where(lane == sub, whole, 0.0), axis=1, keepdims=True) / d_model
        mean_sq = jnp.sum(jnp.where(lane == sub + rows, whole, 0.0), axis=1, keepdims=True) / d_model
        inv = lax.rsqrt(mean_sq - mean * mean + NORM_EPS)
        z_ref[at, :] = ((x_all[at, :].astype(F32) - mean) * inv * gain[r]).astype(BF16)

    role_near = near == c
    role_far = far == c
    role_last = r == N_ROW - 1 - c

    def one_of(j, kind):
        found = [j == i for i in range(n_chunks) if KINDS[i % len(KINDS)] == kind]
        return functools.reduce(jnp.logical_or, found)

    def at_root(j):
        return one_of(j, 0)

    def by_root(j):
        return one_of(j, 1)

    def direct(j):
        return one_of(j, 2)

    def near_copy(j):
        return remote(part.at[j], from_near.at[j], p_send.at[0], p_recv.at[j], c, near)

    def far_copy(j):
        return remote(part.at[j], from_far.at[j], p_send.at[0], f_recv.at[j], c, far)

    def passes(j):
        return jnp.logical_or(
            jnp.logical_and(at_root(j), role_far), jnp.logical_and(jnp.logical_not(at_root(j)), role_near)
        )

    def ends(j):
        return jnp.logical_or(
            jnp.logical_and(at_root(j), is_root), jnp.logical_and(jnp.logical_not(at_root(j)), role_last)
        )

    def gives(j):
        return jnp.logical_not(jnp.logical_or(passes(j), ends(j)))

    def pass_on(j):
        @pl.when(passes(j))
        def _():
            near_copy(j).wait_recv()
            part[j] = part[j] + from_near[j]
            far_copy(j).start()

    def product(j):
        total = jnp.dot(z_ref[:, pl.ds(0, blk)], ring[j, pl.ds(0, blk)], preferred_element_type=F32)
        for k in range(1, n_blk):
            at = pl.ds(k * blk, blk)
            total += jnp.dot(z_ref[:, at], ring[j, at], preferred_element_type=F32)
        return total

    def up(i, _):
        pair = (2 * i, 2 * i + 1)

        @pl.when(i % 2 == 0)
        def _():
            done(ring.at[pl.ds(0, 4)], w_load.at[i // 2])

        totals = [product(j) for j in pair]
        for j, total in zip(pair, totals):
            part[j] = total
        for j in pair:
            @pl.when(gives(j))
            def _():
                near_copy(j).start()

        @pl.when(i < (2 * n_chunks - n_slots) // 2)
        def _():
            for j in pair:
                load_out(j + n_slots - n_chunks, j)

        @pl.when(i >= 1)
        def _():
            for j in pair:
                pass_on(j - 2)

        return 0

    lax.fori_loop(0, n_chunks // 2, up, 0)
    for j in (n_chunks - 2, n_chunks - 1):
        pass_on(j)

    inner = 1 + c % 2
    outer = (3 * c + 2) % 5
    inside = jnp.logical_or(c == 1, c == 2)
    forwards = jnp.logical_or(jnp.logical_and(c == 2, r < 2), jnp.logical_and(c == 1, r >= 2))

    def inner_copy(j):
        return remote(hid.at[j], hid.at[j], h_send.at[0], h_recv.at[j], inner, r)

    def outer_copy(j):
        return remote(hid.at[j], hid.at[j], h_send.at[0], h_recv.at[j], outer, r)

    def forward_copy(j):
        return remote(hid.at[j], hid.at[j], h_send.at[0], h_recv.at[j], 3 * (c - 1), r)

    def last_copy(j, to):
        return remote(hid_sent.at[j], hid.at[j], w_send.at[0], h_recv.at[j], to, c)

    acc[...] = jnp.zeros_like(acc)
    behind = 3
    lag = jnp.where(is_root, 1, jnp.where(role_last, jnp.where(inside, n_chunks // 2, n_chunks), 0))
    root_lag = jnp.where(is_root, behind, lag + behind)
    direct_lag = jnp.where(is_root, 4, lag - 4)
    second_half = jnp.where(is_root, lag, direct_lag) + n_half
    done(ring.at[pl.ds(n_chunks, n_half)], w_load.at[n_chunks // 4])

    def finish_sum(j):
        @pl.when(ends(j))
        def _():
            near_copy(j).wait_recv()
            far_copy(j).wait_recv()
            chunk = gelu_tanh(part[j] + from_near[j] + from_far[j]).astype(BF16)

            @pl.when(is_root)
            def _():
                hid[j] = chunk
                inner_copy(j).start()
                outer_copy(j).start()

            @pl.when(jnp.logical_not(is_root))
            def _():
                hid_sent[j] = chunk

                @pl.when(by_root(j))
                def _():
                    last_copy(j, c).start()

                @pl.when(direct(j))
                def _():
                    for to in range(N_COL):
                        last_copy(j, to).start()

    def use(j):
        @pl.when(jnp.logical_not(jnp.logical_and(is_root, at_root(j))))
        def _():
            inner_copy(j).wait_recv()

        @pl.when(jnp.logical_and(is_root, by_root(j)))
        def _():
            inner_copy(j).start()
            outer_copy(j).start()

        @pl.when(jnp.logical_and(forwards, jnp.logical_not(direct(j))))
        def _():
            forward_copy(j).start()

        slot = (n_chunks + j) % n_slots
        for k in range(n_blk):
            at = pl.ds(k * blk, blk)
            acc[:, at] += jnp.dot(hid[j], ring[slot, at], preferred_element_type=F32)

    def take(j, wanted):
        @pl.when(jnp.logical_and(j >= 0, j < n_chunks))
        def _():
            @pl.when(wanted(j))
            def _():
                use(j)

    def step(t, _):
        @pl.when(t < n_chunks)
        def _():
            finish_sum(t)

        @pl.when(t == second_half)
        def _():
            done(ring.at[pl.ds(0, n_half)], w_load.at[n_chunks // 4 + 1])

        take(t - lag, at_root)
        take(t - direct_lag, direct)
        take(t - root_lag, by_root)
        return 0

    lax.fori_loop(0, 2 * n_chunks + behind, step, 0)

    def near_part(i, k):
        other = near if i == 0 else (near + 2) % N_ROW
        at = pl.ds(k * blk, blk)
        return remote(
            acc.at[pl.ds(pl.multiple_of(other * rows, rows), rows), at], near_sum.at[i, :, at],
            n_send.at[0], n_recv.at[i, k], c, near,
        )

    def far_part(k):
        at = pl.ds(k * blk, blk)
        return remote(pair_sum.at[:, at], far_sum.at[:, at], o_send.at[0], o_recv.at[k], c, far)

    def store(k):
        at = pl.ds(k * blk, blk)
        return pltpu.make_async_copy(y_ref.at[:, at], y_hbm.at[:, at], y_store.at[0])

    for i in (1, 0):
        for k in range(n_blk):
            near_part(i, k).start()
    for k in range(n_blk):
        at = pl.ds(k * blk, blk)
        near_part(1, k).wait_recv()
        pair_sum[:, at] = acc[pl.ds(pl.multiple_of(far * rows, rows), rows), at] + near_sum[1, :, at]
        far_part(k).start()
    count = [sum(KINDS[i % len(KINDS)] == kind for i in range(n_chunks)) for kind in range(3)]
    done(stats.at[pl.ds(0, N_COL * N_ROW - 1)], s_send.at[0])

    @pl.when(is_root)
    def _():
        done(gain.at[pl.ds(0, N_COL - 1)], g_send.at[0])
        done(x_all.at[pl.ds(0, (N_ROW - 1) * rows)], x_send.at[0])
        done(part.at[pl.ds(0, count[1] + count[2])], p_send.at[0])
        done(part.at[pl.ds(0, count[0] + count[1])], h_send.at[0])

    @pl.when(jnp.logical_not(is_root))
    def _():
        done(x_all, x_send.at[0])

    @pl.when(role_last)
    def _():
        done(part.at[pl.ds(0, count[0])], p_send.at[0])
        done(part.at[pl.ds(0, (count[1] + N_COL * count[2]) // 2)], w_send.at[0])

    @pl.when(jnp.logical_or(role_near, role_far))
    def _():
        done(part, p_send.at[0])

    @pl.when(forwards)
    def _():
        done(hid.at[pl.ds(0, count[0] + count[1])], h_send.at[0])

    for k in range(n_blk):
        at = pl.ds(k * blk, blk)
        near_part(0, k).wait_recv()
        far_part(k).wait_recv()
        own = acc[pl.ds(pl.multiple_of(r * rows, rows), rows), at] + near_sum[0, :, at] + far_sum[:, at]
        y_ref[:, at] = (x_own[:, at].astype(F32) + own).astype(BF16)
        store(k).start()

    done(near_sum, n_send.at[0])
    done(pair_sum, o_send.at[0])
    done(y_ref, y_store.at[0])


def solution(mesh):
    def local_block(x_blk, gain_blk, w_in_blk, w_out_blk):
        rows, depth = x_blk.shape
        blk = depth // 4
        n_chunks = w_in_blk.shape[1] // blk
        n_slots = n_chunks + n_chunks // 2
        tokens = rows * N_ROW
        dma = pltpu.SemaphoreType.DMA
        n_all = N_COL * N_ROW
        return pl.pallas_call(
            functools.partial(mlp_kernel, n_chunks, n_slots, blk),
            out_shape=jax.ShapeDtypeStruct((rows, depth), BF16),
            in_specs=[pl.BlockSpec(memory_space=pl.ANY)] * 4,
            out_specs=pl.BlockSpec(memory_space=pl.ANY),
            scratch_shapes=[
                pltpu.VMEM((rows, depth), BF16),
                pltpu.VMEM((N_COL, 1, depth), F32),
                pltpu.VMEM((n_all, 1, 128), F32),
                pltpu.VMEM((tokens, depth), BF16),
                pltpu.VMEM((tokens, depth), BF16),
                pltpu.VMEM((n_slots, depth, blk), BF16),
                pltpu.VMEM((n_chunks, tokens, blk), F32),
                pltpu.VMEM((n_chunks, tokens, blk), F32),
                pltpu.VMEM((n_chunks, tokens, blk), F32),
                pltpu.VMEM((n_chunks, tokens, blk), BF16),
                pltpu.VMEM((n_chunks, tokens, blk), BF16),
                pltpu.VMEM((tokens, depth), F32),
                pltpu.VMEM((2, rows, depth), F32),
                pltpu.VMEM((rows, depth), F32),
                pltpu.VMEM((rows, depth), F32),
                pltpu.VMEM((rows, depth), BF16),
                dma((2,)), dma((n_chunks // 4 + 2,)),
                dma((1,)), dma((1,)), dma((1,)), dma((1,)), dma((1,)), dma((1,)),
                dma((1,)), dma((n_chunks,)), dma((n_chunks,)),
                dma((1,)), dma((n_chunks,)), dma((1,)),
                dma((1,)), dma((2, depth // blk)), dma((1,)), dma((depth // blk,)), dma((1,)),
            ],
            compiler_params=pltpu.CompilerParams(
                collective_id=0, has_side_effects=True, vmem_limit_bytes=67_000_000
            ),
        )(x_blk, gain_blk.reshape(1, depth), w_in_blk, w_out_blk)

    return jax.shard_map(
        local_block,
        mesh=mesh,
        in_specs=(P(("dp", "row"), "col"), P("col"), P("row", "col"), P("row", "col")),
        out_specs=P(("dp", "row"), "col"),
        check_vma=False,
    )
```

```python
import functools

import jax
import jax.numpy as jnp
from jax import lax
from jax.experimental import pallas as pl
from jax.experimental.pallas import tpu as pltpu
from jax.sharding import PartitionSpec as P

NORM_EPS = 1e-5
MESH = pl.DeviceIdType.MESH
BF16, F32 = jnp.bfloat16, jnp.float32
N_COL = 4
N_ROW = 4
KINDS = (0, 1, 0, 1, 0, 1, 0, 1, 0, 0, 0, 2, 2, 2, 2, 2)


def gelu_tanh(x):
    return x * (0.5 * (1.0 + jnp.tanh(0.7978845608028654 * (x + 0.044715 * (x * x * x)))))


def mlp_kernel(
    n_chunks, n_slots, blk,
    x_hbm, g_hbm, w_in_hbm, w_out_hbm, y_hbm,
    x_own, gain, stats, x_all, z_ref, ring, part, from_near, from_far, hid, hid_sent, acc, near_sum, pair_sum, far_sum, y_ref,
    x_load, w_load, x_send, x_recv, g_send, g_recv, s_send, s_recv, p_send, p_recv, f_recv,
    h_send, h_recv, w_send, n_send, n_recv, o_send, o_recv, y_store,
):
    dp, c, r = lax.axis_index("dp"), lax.axis_index("col"), lax.axis_index("row")
    rows = x_own.shape[0]
    n_blk = x_own.shape[1] // blk
    d_model = x_own.shape[1] * N_COL
    near = r + 1 - 2 * (r % 2)
    far = (r + 2) % N_ROW
    me = c * N_ROW + r
    is_root = c == r

    def remote(src, dst, send, recv, to_col, to_row):
        return pltpu.make_async_remote_copy(
            src_ref=src, dst_ref=dst, send_sem=send, recv_sem=recv,
            device_id=(dp, to_col, to_row), device_id_type=MESH,
        )

    def peer(i):
        other = (me + i) % (N_COL * N_ROW)
        return other // N_ROW, other % N_ROW

    x_cp = pltpu.make_async_copy(x_hbm, x_own, x_load.at[0])
    x_cp.start()
    g_cp = pltpu.make_async_copy(g_hbm, gain.at[c], x_load.at[1])
    g_cp.start()
    barrier = pltpu.get_barrier_semaphore()
    for i in range(1, N_COL * N_ROW):
        pc, pr = peer(i)
        pl.semaphore_signal(barrier, inc=1, device_id=(dp, pc, pr), device_id_type=MESH)

    def load_in(j, slot):
        pltpu.make_async_copy(
            w_in_hbm.at[:, pl.ds(pl.multiple_of(j * blk, blk), blk)], ring.at[slot], w_load.at[j // 4]
        ).start()

    def load_out(j, slot):
        for k in range(n_blk):
            pltpu.make_async_copy(
                w_out_hbm.at[pl.ds(pl.multiple_of(j * blk, blk), blk), pl.ds(k * blk, blk)],
                ring.at[slot, pl.ds(k * blk, blk)], w_load.at[n_chunks // 4 + j // n_half],
            ).start()

    n_half = n_chunks // 2

    def done(ref, sem):
        pltpu.make_async_copy(ref, ref, sem).wait()

    def fill_in(j, _):
        load_in(j, j)
        return 0

    def fill_out(j, _):
        load_out(j, n_chunks + j)
        return 0

    lax.fori_loop(0, n_chunks, fill_in, 0)

    x_cp.wait()
    g_cp.wait()
    x_f32 = x_own[...].astype(F32)
    lane = lax.broadcasted_iota(jnp.int32, (rows, 128), 1)
    sub = lax.broadcasted_iota(jnp.int32, (rows, 128), 0)
    total = jnp.sum(x_f32, axis=1, keepdims=True)
    square = jnp.sum(x_f32 * x_f32, axis=1, keepdims=True)
    packed = jnp.where(lane == sub, total, 0.0) + jnp.where(lane == sub + rows, square, 0.0)
    stats[me] = jnp.sum(packed, axis=0, keepdims=True)

    pl.semaphore_wait(barrier, N_COL * N_ROW - 1)

    def stat_copy(i):
        pc, pr = peer(i)
        return remote(stats.at[me], stats.at[me], s_send.at[0], s_recv.at[0], pc, pr)

    def far_first(i):
        if i == 0:
            return c
        if i == 3:
            return jnp.where(c < 2, 3, 0)
        if i == 2:
            return jnp.where(c < 2, 2, 1)
        return jnp.where(c < 2, 1 - c, 5 - c)

    def x_copy(i):
        return remote(x_own, x_all.at[pl.ds(r * rows, rows)], x_send.at[0], x_recv.at[0], far_first(i), c)

    def g_copy(i):
        return remote(gain.at[c], gain.at[c], g_send.at[0], g_recv.at[0], far_first(i), c)

    @pl.when(is_root)
    def _():
        for i in (3, 2, 1):
            g_copy(i).start()

    for i in range(1, N_COL * N_ROW):
        stat_copy(i).start()
    for i in (3, 2, 1):
        x_copy(i).start()

    @pl.when(is_root)
    def _():
        x_all[pl.ds(pl.multiple_of(r * rows, rows), rows), :] = x_own[...]

    @pl.when(jnp.logical_not(is_root))
    def _():
        x_copy(0).start()

    lax.fori_loop(0, n_slots - n_chunks, fill_out, 0)

    done(stats.at[pl.ds(0, N_COL * N_ROW - 1)], s_recv.at[0])

    @pl.when(is_root)
    def _():
        done(x_all.at[pl.ds(0, (N_ROW - 1) * rows)], x_recv.at[0])

    @pl.when(jnp.logical_not(is_root))
    def _():
        done(gain.at[0], g_recv.at[0])
        done(x_all, x_recv.at[0])

    for q in range(N_ROW):
        at = pl.ds(q * rows, rows)
        whole = stats[q] + stats[N_ROW + q] + stats[2 * N_ROW + q] + stats[3 * N_ROW + q]
        whole = jnp.broadcast_to(whole, (rows, 128))
        mean = jnp.sum(jnp.where(lane == sub, whole, 0.0), axis=1, keepdims=True) / d_model
        mean_sq = jnp.sum(jnp.where(lane == sub + rows, whole, 0.0), axis=1, keepdims=True) / d_model
        inv = lax.rsqrt(mean_sq - mean * mean + NORM_EPS)
        z_ref[at, :] = ((x_all[at, :].astype(F32) - mean) * inv * gain[r]).astype(BF16)

    role_near = near == c
    role_far = far == c
    role_last = r == N_ROW - 1 - c

    def one_of(j, kind):
        found = [j == i for i in range(n_chunks) if KINDS[i % len(KINDS)] == kind]
        return functools.reduce(jnp.logical_or, found)

    def at_root(j):
        return one_of(j, 0)

    def by_root(j):
        return one_of(j, 1)

    def direct(j):
        return one_of(j, 2)

    def near_copy(j):
        return remote(part.at[j], from_near.at[j], p_send.at[0], p_recv.at[j], c, near)

    def far_copy(j):
        return remote(part.at[j], from_far.at[j], p_send.at[0], f_recv.at[j], c, far)

    def passes(j):
        return jnp.logical_or(
            jnp.logical_and(at_root(j), role_far), jnp.logical_and(jnp.logical_not(at_root(j)), role_near)
        )

    def ends(j):
        return jnp.logical_or(
            jnp.logical_and(at_root(j), is_root), jnp.logical_and(jnp.logical_not(at_root(j)), role_last)
        )

    def gives(j):
        return jnp.logical_not(jnp.logical_or(passes(j), ends(j)))

    def pass_on(j):
        @pl.when(passes(j))
        def _():
            near_copy(j).wait_recv()
            part[j] = part[j] + from_near[j]
            far_copy(j).start()

    def product(j):
        total = jnp.dot(z_ref[:, pl.ds(0, blk)], ring[j, pl.ds(0, blk)], preferred_element_type=F32)
        for k in range(1, n_blk):
            at = pl.ds(k * blk, blk)
            total += jnp.dot(z_ref[:, at], ring[j, at], preferred_element_type=F32)
        return total

    def up(i, _):
        pair = (2 * i, 2 * i + 1)

        @pl.when(i % 2 == 0)
        def _():
            done(ring.at[pl.ds(0, 4)], w_load.at[i // 2])

        totals = [product(j) for j in pair]
        for j, total in zip(pair, totals):
            part[j] = total
        for j in pair:
            @pl.when(gives(j))
            def _():
                near_copy(j).start()

        @pl.when(i < (2 * n_chunks - n_slots) // 2)
        def _():
            for j in pair:
                load_out(j + n_slots - n_chunks, j)

        @pl.when(i >= 1)
        def _():
            for j in pair:
                pass_on(j - 2)

        return 0

    lax.fori_loop(0, n_chunks // 2, up, 0)
    for j in (n_chunks - 2, n_chunks - 1):
        pass_on(j)

    inner = 1 + c % 2
    outer = (3 * c + 2) % 5
    inside = jnp.logical_or(c == 1, c == 2)
    forwards = jnp.logical_or(jnp.logical_and(c == 2, r < 2), jnp.logical_and(c == 1, r >= 2))

    def inner_copy(j):
        return remote(hid.at[j], hid.at[j], h_send.at[0], h_recv.at[j], inner, r)

    def outer_copy(j):
        return remote(hid.at[j], hid.at[j], h_send.at[0], h_recv.at[j], outer, r)

    def forward_copy(j):
        return remote(hid.at[j], hid.at[j], h_send.at[0], h_recv.at[j], 3 * (c - 1), r)

    def last_copy(j, to):
        return remote(hid_sent.at[j], hid.at[j], w_send.at[0], h_recv.at[j], to, c)

    acc[...] = jnp.zeros_like(acc)
    behind = 3
    lag = jnp.where(is_root, 1, jnp.where(role_last, jnp.where(inside, n_chunks // 2, n_chunks), 0))
    root_lag = jnp.where(is_root, behind, lag + behind)
    direct_lag = jnp.where(is_root, 4, lag - jnp.where(inside, 4, 8))
    second_half = jnp.where(is_root, lag, direct_lag + 2) + n_half
    done(ring.at[pl.ds(n_chunks, n_half)], w_load.at[n_chunks // 4])

    def finish_sum(j):
        @pl.when(ends(j))
        def _():
            near_copy(j).wait_recv()
            far_copy(j).wait_recv()
            chunk = gelu_tanh(part[j] + from_near[j] + from_far[j]).astype(BF16)

            @pl.when(is_root)
            def _():
                hid[j] = chunk
                inner_copy(j).start()
                outer_copy(j).start()

            @pl.when(jnp.logical_not(is_root))
            def _():
                hid_sent[j] = chunk

                @pl.when(by_root(j))
                def _():
                    last_copy(j, c).start()

                @pl.when(direct(j))
                def _():
                    for to in range(N_COL):
                        last_copy(j, to).start()

    def use(j):
        @pl.when(jnp.logical_not(jnp.logical_and(is_root, at_root(j))))
        def _():
            inner_copy(j).wait_recv()

        @pl.when(jnp.logical_and(is_root, by_root(j)))
        def _():
            inner_copy(j).start()
            outer_copy(j).start()

        @pl.when(jnp.logical_and(forwards, jnp.logical_not(direct(j))))
        def _():
            forward_copy(j).start()

        slot = (n_chunks + j) % n_slots
        for k in range(n_blk):
            at = pl.ds(k * blk, blk)
            acc[:, at] += jnp.dot(hid[j], ring[slot, at], preferred_element_type=F32)

    def take(j, wanted):
        @pl.when(jnp.logical_and(j >= 0, j < n_chunks))
        def _():
            @pl.when(wanted(j))
            def _():
                use(j)

    def step(t, _):
        @pl.when(t < n_chunks)
        def _():
            finish_sum(t)

        @pl.when(t == second_half)
        def _():
            done(ring.at[pl.ds(0, n_half)], w_load.at[n_chunks // 4 + 1])

        take(t - lag, at_root)
        take(t - direct_lag, direct)
        take(t - root_lag, by_root)
        return 0

    lax.fori_loop(0, 2 * n_chunks + behind, step, 0)

    def near_part(i, k):
        other = near if i == 0 else (near + 2) % N_ROW
        at = pl.ds(k * blk, blk)
        return remote(
            acc.at[pl.ds(pl.multiple_of(other * rows, rows), rows), at], near_sum.at[i, :, at],
            n_send.at[0], n_recv.at[i, k], c, near,
        )

    def far_part(k):
        at = pl.ds(k * blk, blk)
        return remote(pair_sum.at[:, at], far_sum.at[:, at], o_send.at[0], o_recv.at[k], c, far)

    def store(k):
        at = pl.ds(k * blk, blk)
        return pltpu.make_async_copy(y_ref.at[:, at], y_hbm.at[:, at], y_store.at[0])

    for i in (1, 0):
        for k in range(n_blk):
            near_part(i, k).start()
    for k in range(n_blk):
        at = pl.ds(k * blk, blk)
        near_part(1, k).wait_recv()
        pair_sum[:, at] = acc[pl.ds(pl.multiple_of(far * rows, rows), rows), at] + near_sum[1, :, at]
        far_part(k).start()
    count = [sum(KINDS[i % len(KINDS)] == kind for i in range(n_chunks)) for kind in range(3)]
    done(stats.at[pl.ds(0, N_COL * N_ROW - 1)], s_send.at[0])

    @pl.when(is_root)
    def _():
        done(gain.at[pl.ds(0, N_COL - 1)], g_send.at[0])
        done(x_all.at[pl.ds(0, (N_ROW - 1) * rows)], x_send.at[0])
        done(part.at[pl.ds(0, count[1] + count[2])], p_send.at[0])
        done(part.at[pl.ds(0, count[0] + count[1])], h_send.at[0])

    @pl.when(jnp.logical_not(is_root))
    def _():
        done(x_all, x_send.at[0])

    @pl.when(role_last)
    def _():
        done(part.at[pl.ds(0, count[0])], p_send.at[0])
        done(part.at[pl.ds(0, (count[1] + N_COL * count[2]) // 2)], w_send.at[0])

    @pl.when(jnp.logical_or(role_near, role_far))
    def _():
        done(part, p_send.at[0])

    @pl.when(forwards)
    def _():
        done(hid.at[pl.ds(0, count[0] + count[1])], h_send.at[0])

    for k in range(n_blk):
        at = pl.ds(k * blk, blk)
        near_part(0, k).wait_recv()
        far_part(k).wait_recv()
        own = acc[pl.ds(pl.multiple_of(r * rows, rows), rows), at] + near_sum[0, :, at] + far_sum[:, at]
        y_ref[:, at] = (x_own[:, at].astype(F32) + own).astype(BF16)
        store(k).start()

    done(near_sum, n_send.at[0])
    done(pair_sum, o_send.at[0])
    done(y_ref, y_store.at[0])


def solution(mesh):
    def local_block(x_blk, gain_blk, w_in_blk, w_out_blk):
        rows, depth = x_blk.shape
        blk = depth // 4
        n_chunks = w_in_blk.shape[1] // blk
        n_slots = n_chunks + n_chunks // 2
        tokens = rows * N_ROW
        dma = pltpu.SemaphoreType.DMA
        n_all = N_COL * N_ROW
        return pl.pallas_call(
            functools.partial(mlp_kernel, n_chunks, n_slots, blk),
            out_shape=jax.ShapeDtypeStruct((rows, depth), BF16),
            in_specs=[pl.BlockSpec(memory_space=pl.ANY)] * 4,
            out_specs=pl.BlockSpec(memory_space=pl.ANY),
            scratch_shapes=[
                pltpu.VMEM((rows, depth), BF16),
                pltpu.VMEM((N_COL, 1, depth), F32),
                pltpu.VMEM((n_all, 1, 128), F32),
                pltpu.VMEM((tokens, depth), BF16),
                pltpu.VMEM((tokens, depth), BF16),
                pltpu.VMEM((n_slots, depth, blk), BF16),
                pltpu.VMEM((n_chunks, tokens, blk), F32),
                pltpu.VMEM((n_chunks, tokens, blk), F32),
                pltpu.VMEM((n_chunks, tokens, blk), F32),
                pltpu.VMEM((n_chunks, tokens, blk), BF16),
                pltpu.VMEM((n_chunks, tokens, blk), BF16),
                pltpu.VMEM((tokens, depth), F32),
                pltpu.VMEM((2, rows, depth), F32),
                pltpu.VMEM((rows, depth), F32),
                pltpu.VMEM((rows, depth), F32),
                pltpu.VMEM((rows, depth), BF16),
                dma((2,)), dma((n_chunks // 4 + 2,)),
                dma((1,)), dma((1,)), dma((1,)), dma((1,)), dma((1,)), dma((1,)),
                dma((1,)), dma((n_chunks,)), dma((n_chunks,)),
                dma((1,)), dma((n_chunks,)), dma((1,)),
                dma((1,)), dma((2, depth // blk)), dma((1,)), dma((depth // blk,)), dma((1,)),
            ],
            compiler_params=pltpu.CompilerParams(
                collective_id=0, has_side_effects=True, vmem_limit_bytes=67_000_000
            ),
        )(x_blk, gain_blk.reshape(1, depth), w_in_blk, w_out_blk)

    return jax.shard_map(
        local_block,
        mesh=mesh,
        in_specs=(P(("dp", "row"), "col"), P("col"), P("row", "col"), P("row", "col")),
        out_specs=P(("dp", "row"), "col"),
        check_vma=False,
    )
```

```python
import functools

import jax
import jax.numpy as jnp
from jax import lax
from jax.experimental import pallas as pl
from jax.experimental.pallas import tpu as pltpu
from jax.sharding import PartitionSpec as P

NORM_EPS = 1e-5
MESH = pl.DeviceIdType.MESH
BF16, F32 = jnp.bfloat16, jnp.float32
N_COL = 4
N_ROW = 4
KINDS = (0, 1, 0, 1, 0, 1, 0, 1, 0, 0, 0, 2, 2, 2, 2, 2)


def gelu_tanh(x):
    return x * (0.5 * (1.0 + jnp.tanh(0.7978845608028654 * (x + 0.044715 * (x * x * x)))))


def mlp_kernel(
    n_chunks, n_slots, blk,
    x_hbm, g_hbm, w_in_hbm, w_out_hbm, y_hbm,
    x_own, gain, stats, x_all, z_ref, ring, part, from_near, from_far, hid, hid_sent, acc, near_sum, pair_sum, far_sum, y_ref,
    x_load, w_load, x_send, x_recv, g_send, g_recv, s_send, s_recv, p_send, p_recv, f_recv,
    h_send, h_recv, w_send, n_send, n_recv, o_send, o_recv, y_store,
):
    dp, c, r = lax.axis_index("dp"), lax.axis_index("col"), lax.axis_index("row")
    rows = x_own.shape[0]
    n_blk = x_own.shape[1] // blk
    d_model = x_own.shape[1] * N_COL
    near = r + 1 - 2 * (r % 2)
    far = (r + 2) % N_ROW
    me = c * N_ROW + r
    is_root = c == r

    def remote(src, dst, send, recv, to_col, to_row):
        return pltpu.make_async_remote_copy(
            src_ref=src, dst_ref=dst, send_sem=send, recv_sem=recv,
            device_id=(dp, to_col, to_row), device_id_type=MESH,
        )

    def peer(i):
        other = (me + i) % (N_COL * N_ROW)
        return other // N_ROW, other % N_ROW

    x_cp = pltpu.make_async_copy(x_hbm, x_own, x_load.at[0])
    x_cp.start()
    g_cp = pltpu.make_async_copy(g_hbm, gain.at[c], x_load.at[1])
    g_cp.start()
    barrier = pltpu.get_barrier_semaphore()
    for i in range(1, N_COL * N_ROW):
        pc, pr = peer(i)
        pl.semaphore_signal(barrier, inc=1, device_id=(dp, pc, pr), device_id_type=MESH)

    def load_in(j, slot):
        pltpu.make_async_copy(
            w_in_hbm.at[:, pl.ds(pl.multiple_of(j * blk, blk), blk)], ring.at[slot], w_load.at[j // 4]
        ).start()

    def load_out(j, slot):
        for k in range(n_blk):
            pltpu.make_async_copy(
                w_out_hbm.at[pl.ds(pl.multiple_of(j * blk, blk), blk), pl.ds(k * blk, blk)],
                ring.at[slot, pl.ds(k * blk, blk)], w_load.at[n_chunks // 4 + j // n_half],
            ).start()

    n_half = n_chunks // 2

    def done(ref, sem):
        pltpu.make_async_copy(ref, ref, sem).wait()

    def fill_in(j, _):
        load_in(j, j)
        return 0

    def fill_out(j, _):
        load_out(j, n_chunks + j)
        return 0

    lax.fori_loop(0, n_chunks, fill_in, 0)

    x_cp.wait()
    g_cp.wait()
    x_f32 = x_own[...].astype(F32)
    lane = lax.broadcasted_iota(jnp.int32, (rows, 128), 1)
    sub = lax.broadcasted_iota(jnp.int32, (rows, 128), 0)
    total = jnp.sum(x_f32, axis=1, keepdims=True)
    square = jnp.sum(x_f32 * x_f32, axis=1, keepdims=True)
    packed = jnp.where(lane == sub, total, 0.0) + jnp.where(lane == sub + rows, square, 0.0)
    stats[me] = jnp.sum(packed, axis=0, keepdims=True)

    pl.semaphore_wait(barrier, N_COL * N_ROW - 1)

    def stat_copy(i):
        pc, pr = peer(i)
        return remote(stats.at[me], stats.at[me], s_send.at[0], s_recv.at[0], pc, pr)

    def far_first(i):
        if i == 0:
            return c
        if i == 3:
            return jnp.where(c < 2, 3, 0)
        if i == 2:
            return jnp.where(c < 2, 2, 1)
        return jnp.where(c < 2, 1 - c, 5 - c)

    def x_copy(i):
        return remote(x_own, x_all.at[pl.ds(r * rows, rows)], x_send.at[0], x_recv.at[0], far_first(i), c)

    def g_copy(i):
        return remote(gain.at[c], gain.at[c], g_send.at[0], g_recv.at[0], far_first(i), c)

    @pl.when(is_root)
    def _():
        for i in (3, 2, 1):
            g_copy(i).start()

    for i in range(1, N_COL * N_ROW):
        stat_copy(i).start()
    for i in (3, 2, 1):
        x_copy(i).start()

    @pl.when(is_root)
    def _():
        x_all[pl.ds(pl.multiple_of(r * rows, rows), rows), :] = x_own[...]

    @pl.when(jnp.logical_not(is_root))
    def _():
        x_copy(0).start()

    lax.fori_loop(0, n_slots - n_chunks, fill_out, 0)

    done(stats.at[pl.ds(0, N_COL * N_ROW - 1)], s_recv.at[0])

    @pl.when(is_root)
    def _():
        done(x_all.at[pl.ds(0, (N_ROW - 1) * rows)], x_recv.at[0])

    @pl.when(jnp.logical_not(is_root))
    def _():
        done(gain.at[0], g_recv.at[0])
        done(x_all, x_recv.at[0])

    for q in range(N_ROW):
        at = pl.ds(q * rows, rows)
        whole = stats[q] + stats[N_ROW + q] + stats[2 * N_ROW + q] + stats[3 * N_ROW + q]
        whole = jnp.broadcast_to(whole, (rows, 128))
        mean = jnp.sum(jnp.where(lane == sub, whole, 0.0), axis=1, keepdims=True) / d_model
        mean_sq = jnp.sum(jnp.where(lane == sub + rows, whole, 0.0), axis=1, keepdims=True) / d_model
        inv = lax.rsqrt(mean_sq - mean * mean + NORM_EPS)
        z_ref[at, :] = ((x_all[at, :].astype(F32) - mean) * inv * gain[r]).astype(BF16)

    role_near = near == c
    role_far = far == c
    role_last = r == N_ROW - 1 - c

    def one_of(j, kind):
        found = [j == i for i in range(n_chunks) if KINDS[i % len(KINDS)] == kind]
        return functools.reduce(jnp.logical_or, found)

    def at_root(j):
        return one_of(j, 0)

    def by_root(j):
        return one_of(j, 1)

    def direct(j):
        return one_of(j, 2)

    def near_copy(j):
        return remote(part.at[j], from_near.at[j], p_send.at[0], p_recv.at[j], c, near)

    def far_copy(j):
        return remote(part.at[j], from_far.at[j], p_send.at[0], f_recv.at[j], c, far)

    def passes(j):
        return jnp.logical_or(
            jnp.logical_and(at_root(j), role_far), jnp.logical_and(jnp.logical_not(at_root(j)), role_near)
        )

    def ends(j):
        return jnp.logical_or(
            jnp.logical_and(at_root(j), is_root), jnp.logical_and(jnp.logical_not(at_root(j)), role_last)
        )

    def gives(j):
        return jnp.logical_not(jnp.logical_or(passes(j), ends(j)))

    def pass_on(j):
        @pl.when(passes(j))
        def _():
            near_copy(j).wait_recv()
            part[j] = part[j] + from_near[j]
            far_copy(j).start()

    def product(j):
        total = jnp.dot(z_ref[:, pl.ds(0, blk)], ring[j, pl.ds(0, blk)], preferred_element_type=F32)
        for k in range(1, n_blk):
            at = pl.ds(k * blk, blk)
            total += jnp.dot(z_ref[:, at], ring[j, at], preferred_element_type=F32)
        return total

    def up(i, _):
        pair = (2 * i, 2 * i + 1)

        @pl.when(i % 2 == 0)
        def _():
            done(ring.at[pl.ds(0, 4)], w_load.at[i // 2])

        totals = [product(j) for j in pair]
        for j, total in zip(pair, totals):
            part[j] = total
        for j in pair:
            @pl.when(gives(j))
            def _():
                near_copy(j).start()

        @pl.when(i < (2 * n_chunks - n_slots) // 2)
        def _():
            for j in pair:
                load_out(j + n_slots - n_chunks, j)

        @pl.when(i >= 1)
        def _():
            for j in pair:
                pass_on(j - 2)

        return 0

    lax.fori_loop(0, n_chunks // 2, up, 0)
    for j in (n_chunks - 2, n_chunks - 1):
        pass_on(j)

    inner = 1 + c % 2
    outer = (3 * c + 2) % 5
    inside = jnp.logical_or(c == 1, c == 2)
    forwards = jnp.logical_or(jnp.logical_and(c == 2, r < 2), jnp.logical_and(c == 1, r >= 2))

    def inner_copy(j):
        return remote(hid.at[j], hid.at[j], h_send.at[0], h_recv.at[j], inner, r)

    def outer_copy(j):
        return remote(hid.at[j], hid.at[j], h_send.at[0], h_recv.at[j], outer, r)

    def forward_copy(j):
        return remote(hid.at[j], hid.at[j], h_send.at[0], h_recv.at[j], 3 * (c - 1), r)

    def last_copy(j, to):
        return remote(hid_sent.at[j], hid.at[j], w_send.at[0], h_recv.at[j], to, c)

    acc[...] = jnp.zeros_like(acc)
    behind = 3
    lag = jnp.where(is_root, 1, jnp.where(role_last, jnp.where(inside, n_chunks // 2, n_chunks), 0))
    root_lag = jnp.where(is_root, behind, lag + behind)
    direct_lag = jnp.where(is_root, 4, lag - jnp.where(inside, 0, 8))
    second_half = jnp.where(is_root | inside, lag, direct_lag + 2) + n_half
    done(ring.at[pl.ds(n_chunks, n_half)], w_load.at[n_chunks // 4])

    def finish_sum(j):
        @pl.when(ends(j))
        def _():
            near_copy(j).wait_recv()
            far_copy(j).wait_recv()
            chunk = gelu_tanh(part[j] + from_near[j] + from_far[j]).astype(BF16)

            @pl.when(is_root)
            def _():
                hid[j] = chunk
                inner_copy(j).start()
                outer_copy(j).start()

            @pl.when(jnp.logical_not(is_root))
            def _():
                hid_sent[j] = chunk

                @pl.when(by_root(j))
                def _():
                    last_copy(j, c).start()

                @pl.when(direct(j))
                def _():
                    for to in range(N_COL):
                        last_copy(j, to).start()

    def use(j):
        @pl.when(jnp.logical_not(jnp.logical_and(is_root, at_root(j))))
        def _():
            inner_copy(j).wait_recv()

        @pl.when(jnp.logical_and(is_root, by_root(j)))
        def _():
            inner_copy(j).start()
            outer_copy(j).start()

        @pl.when(jnp.logical_and(forwards, jnp.logical_not(direct(j))))
        def _():
            forward_copy(j).start()

        slot = (n_chunks + j) % n_slots
        for k in range(n_blk):
            at = pl.ds(k * blk, blk)
            acc[:, at] += jnp.dot(hid[j], ring[slot, at], preferred_element_type=F32)

    def take(j, wanted):
        @pl.when(jnp.logical_and(j >= 0, j < n_chunks))
        def _():
            @pl.when(wanted(j))
            def _():
                use(j)

    def step(t, _):
        @pl.when(t < n_chunks)
        def _():
            finish_sum(t)

        @pl.when(t == second_half)
        def _():
            done(ring.at[pl.ds(0, n_half)], w_load.at[n_chunks // 4 + 1])

        take(t - lag, at_root)
        take(t - direct_lag, direct)
        take(t - root_lag, by_root)
        return 0

    lax.fori_loop(0, 2 * n_chunks + behind, step, 0)

    def near_part(i, k):
        other = near if i == 0 else (near + 2) % N_ROW
        at = pl.ds(k * blk, blk)
        return remote(
            acc.at[pl.ds(pl.multiple_of(other * rows, rows), rows), at], near_sum.at[i, :, at],
            n_send.at[0], n_recv.at[i, k], c, near,
        )

    def far_part(k):
        at = pl.ds(k * blk, blk)
        return remote(pair_sum.at[:, at], far_sum.at[:, at], o_send.at[0], o_recv.at[k], c, far)

    def store(k):
        at = pl.ds(k * blk, blk)
        return pltpu.make_async_copy(y_ref.at[:, at], y_hbm.at[:, at], y_store.at[0])

    for i in (1, 0):
        for k in range(n_blk):
            near_part(i, k).start()
    for k in range(n_blk):
        at = pl.ds(k * blk, blk)
        near_part(1, k).wait_recv()
        pair_sum[:, at] = acc[pl.ds(pl.multiple_of(far * rows, rows), rows), at] + near_sum[1, :, at]
        far_part(k).start()
    count = [sum(KINDS[i % len(KINDS)] == kind for i in range(n_chunks)) for kind in range(3)]
    done(stats.at[pl.ds(0, N_COL * N_ROW - 1)], s_send.at[0])

    @pl.when(is_root)
    def _():
        done(gain.at[pl.ds(0, N_COL - 1)], g_send.at[0])
        done(x_all.at[pl.ds(0, (N_ROW - 1) * rows)], x_send.at[0])
        done(part.at[pl.ds(0, count[1] + count[2])], p_send.at[0])
        done(part.at[pl.ds(0, count[0] + count[1])], h_send.at[0])

    @pl.when(jnp.logical_not(is_root))
    def _():
        done(x_all, x_send.at[0])

    @pl.when(role_last)
    def _():
        done(part.at[pl.ds(0, count[0])], p_send.at[0])
        done(part.at[pl.ds(0, (count[1] + N_COL * count[2]) // 2)], w_send.at[0])

    @pl.when(jnp.logical_or(role_near, role_far))
    def _():
        done(part, p_send.at[0])

    @pl.when(forwards)
    def _():
        done(hid.at[pl.ds(0, count[0] + count[1])], h_send.at[0])

    for k in range(n_blk):
        at = pl.ds(k * blk, blk)
        near_part(0, k).wait_recv()
        far_part(k).wait_recv()
        own = acc[pl.ds(pl.multiple_of(r * rows, rows), rows), at] + near_sum[0, :, at] + far_sum[:, at]
        y_ref[:, at] = (x_own[:, at].astype(F32) + own).astype(BF16)
        store(k).start()

    done(near_sum, n_send.at[0])
    done(pair_sum, o_send.at[0])
    done(y_ref, y_store.at[0])


def solution(mesh):
    def local_block(x_blk, gain_blk, w_in_blk, w_out_blk):
        rows, depth = x_blk.shape
        blk = depth // 4
        n_chunks = w_in_blk.shape[1] // blk
        n_slots = n_chunks + n_chunks // 2
        tokens = rows * N_ROW
        dma = pltpu.SemaphoreType.DMA
        n_all = N_COL * N_ROW
        return pl.pallas_call(
            functools.partial(mlp_kernel, n_chunks, n_slots, blk),
            out_shape=jax.ShapeDtypeStruct((rows, depth), BF16),
            in_specs=[pl.BlockSpec(memory_space=pl.ANY)] * 4,
            out_specs=pl.BlockSpec(memory_space=pl.ANY),
            scratch_shapes=[
                pltpu.VMEM((rows, depth), BF16),
                pltpu.VMEM((N_COL, 1, depth), F32),
                pltpu.VMEM((n_all, 1, 128), F32),
                pltpu.VMEM((tokens, depth), BF16),
                pltpu.VMEM((tokens, depth), BF16),
                pltpu.VMEM((n_slots, depth, blk), BF16),
                pltpu.VMEM((n_chunks, tokens, blk), F32),
                pltpu.VMEM((n_chunks, tokens, blk), F32),
                pltpu.VMEM((n_chunks, tokens, blk), F32),
                pltpu.VMEM((n_chunks, tokens, blk), BF16),
                pltpu.VMEM((n_chunks, tokens, blk), BF16),
                pltpu.VMEM((tokens, depth), F32),
                pltpu.VMEM((2, rows, depth), F32),
                pltpu.VMEM((rows, depth), F32),
                pltpu.VMEM((rows, depth), F32),
                pltpu.VMEM((rows, depth), BF16),
                dma((2,)), dma((n_chunks // 4 + 2,)),
                dma((1,)), dma((1,)), dma((1,)), dma((1,)), dma((1,)), dma((1,)),
                dma((1,)), dma((n_chunks,)), dma((n_chunks,)),
                dma((1,)), dma((n_chunks,)), dma((1,)),
                dma((1,)), dma((2, depth // blk)), dma((1,)), dma((depth // blk,)), dma((1,)),
            ],
            compiler_params=pltpu.CompilerParams(
                collective_id=0, has_side_effects=True, vmem_limit_bytes=67_000_000
            ),
        )(x_blk, gain_blk.reshape(1, depth), w_in_blk, w_out_blk)

    return jax.shard_map(
        local_block,
        mesh=mesh,
        in_specs=(P(("dp", "row"), "col"), P("col"), P("row", "col"), P("row", "col")),
        out_specs=P(("dp", "row"), "col"),
        check_vma=False,
    )
```

```python
import functools

import jax
import jax.numpy as jnp
from jax import lax
from jax.experimental import pallas as pl
from jax.experimental.pallas import tpu as pltpu
from jax.sharding import PartitionSpec as P

NORM_EPS = 1e-5
MESH = pl.DeviceIdType.MESH
BF16, F32 = jnp.bfloat16, jnp.float32
N_COL = 4
N_ROW = 4
KINDS = (0, 1, 0, 1, 0, 1, 0, 1, 0, 1, 0, 1, 2, 2, 2, 2)


def gelu_tanh(x):
    return x * (0.5 * (1.0 + jnp.tanh(0.7978845608028654 * (x + 0.044715 * (x * x * x)))))


def mlp_kernel(
    n_chunks, n_slots, blk,
    x_hbm, g_hbm, w_in_hbm, w_out_hbm, y_hbm,
    x_own, gain, stats, x_all, z_ref, ring, part, from_near, from_far, hid, hid_sent, acc, near_sum, pair_sum, far_sum, y_ref,
    x_load, w_load, x_send, x_recv, g_send, g_recv, s_send, s_recv, p_send, p_recv, f_recv,
    h_send, h_recv, w_send, n_send, n_recv, o_send, o_recv, y_store,
):
    dp, c, r = lax.axis_index("dp"), lax.axis_index("col"), lax.axis_index("row")
    rows = x_own.shape[0]
    n_blk = x_own.shape[1] // blk
    d_model = x_own.shape[1] * N_COL
    near = r + 1 - 2 * (r % 2)
    far = (r + 2) % N_ROW
    me = c * N_ROW + r
    is_root = c == r

    def remote(src, dst, send, recv, to_col, to_row):
        return pltpu.make_async_remote_copy(
            src_ref=src, dst_ref=dst, send_sem=send, recv_sem=recv,
            device_id=(dp, to_col, to_row), device_id_type=MESH,
        )

    def peer(i):
        other = (me + i) % (N_COL * N_ROW)
        return other // N_ROW, other % N_ROW

    x_cp = pltpu.make_async_copy(x_hbm, x_own, x_load.at[0])
    x_cp.start()
    g_cp = pltpu.make_async_copy(g_hbm, gain.at[c], x_load.at[1])
    g_cp.start()
    barrier = pltpu.get_barrier_semaphore()
    for i in range(1, N_COL * N_ROW):
        pc, pr = peer(i)
        pl.semaphore_signal(barrier, inc=1, device_id=(dp, pc, pr), device_id_type=MESH)

    def load_in(j, slot):
        pltpu.make_async_copy(
            w_in_hbm.at[:, pl.ds(pl.multiple_of(j * blk, blk), blk)], ring.at[slot], w_load.at[j // 4]
        ).start()

    def load_out(j, slot):
        for k in range(n_blk):
            pltpu.make_async_copy(
                w_out_hbm.at[pl.ds(pl.multiple_of(j * blk, blk), blk), pl.ds(k * blk, blk)],
                ring.at[slot, pl.ds(k * blk, blk)], w_load.at[n_chunks // 4 + j // n_half],
            ).start()

    n_half = n_chunks // 2

    def done(ref, sem):
        pltpu.make_async_copy(ref, ref, sem).wait()

    def fill_in(j, _):
        load_in(j, j)
        return 0

    def fill_out(j, _):
        load_out(j, n_chunks + j)
        return 0

    lax.fori_loop(0, n_chunks, fill_in, 0)

    x_cp.wait()
    g_cp.wait()
    x_f32 = x_own[...].astype(F32)
    lane = lax.broadcasted_iota(jnp.int32, (rows, 128), 1)
    sub = lax.broadcasted_iota(jnp.int32, (rows, 128), 0)
    total = jnp.sum(x_f32, axis=1, keepdims=True)
    square = jnp.sum(x_f32 * x_f32, axis=1, keepdims=True)
    packed = jnp.where(lane == sub, total, 0.0) + jnp.where(lane == sub + rows, square, 0.0)
    stats[me] = jnp.sum(packed, axis=0, keepdims=True)

    pl.semaphore_wait(barrier, N_COL * N_ROW - 1)

    def stat_copy(i):
        pc, pr = peer(i)
        return remote(stats.at[me], stats.at[me], s_send.at[0], s_recv.at[0], pc, pr)

    def far_first(i):
        if i == 0:
            return c
        if i == 3:
            return jnp.where(c < 2, 3, 0)
        if i == 2:
            return jnp.where(c < 2, 2, 1)
        return jnp.where(c < 2, 1 - c, 5 - c)

    def x_copy(i):
        return remote(x_own, x_all.at[pl.ds(r * rows, rows)], x_send.at[0], x_recv.at[0], far_first(i), c)

    def g_copy(i):
        return remote(gain.at[c], gain.at[c], g_send.at[0], g_recv.at[0], far_first(i), c)

    @pl.when(is_root)
    def _():
        for i in (3, 2, 1):
            g_copy(i).start()

    for i in range(1, N_COL * N_ROW):
        stat_copy(i).start()
    for i in (3, 2, 1):
        x_copy(i).start()

    @pl.when(is_root)
    def _():
        x_all[pl.ds(pl.multiple_of(r * rows, rows), rows), :] = x_own[...]

    @pl.when(jnp.logical_not(is_root))
    def _():
        x_copy(0).start()

    lax.fori_loop(0, n_slots - n_chunks, fill_out, 0)

    done(stats.at[pl.ds(0, N_COL * N_ROW - 1)], s_recv.at[0])

    @pl.when(is_root)
    def _():
        done(x_all.at[pl.ds(0, (N_ROW - 1) * rows)], x_recv.at[0])

    @pl.when(jnp.logical_not(is_root))
    def _():
        done(gain.at[0], g_recv.at[0])
        done(x_all, x_recv.at[0])

    for q in range(N_ROW):
        at = pl.ds(q * rows, rows)
        whole = stats[q] + stats[N_ROW + q] + stats[2 * N_ROW + q] + stats[3 * N_ROW + q]
        whole = jnp.broadcast_to(whole, (rows, 128))
        mean = jnp.sum(jnp.where(lane == sub, whole, 0.0), axis=1, keepdims=True) / d_model
        mean_sq = jnp.sum(jnp.where(lane == sub + rows, whole, 0.0), axis=1, keepdims=True) / d_model
        inv = lax.rsqrt(mean_sq - mean * mean + NORM_EPS)
        z_ref[at, :] = ((x_all[at, :].astype(F32) - mean) * inv * gain[r]).astype(BF16)

    role_near = near == c
    role_far = far == c
    role_last = r == N_ROW - 1 - c

    def one_of(j, kind):
        found = [j == i for i in range(n_chunks) if KINDS[i % len(KINDS)] == kind]
        return functools.reduce(jnp.logical_or, found)

    def at_root(j):
        return one_of(j, 0)

    def by_root(j):
        return one_of(j, 1)

    def direct(j):
        return one_of(j, 2)

    def near_copy(j):
        return remote(part.at[j], from_near.at[j], p_send.at[0], p_recv.at[j], c, near)

    def far_copy(j):
        return remote(part.at[j], from_far.at[j], p_send.at[0], f_recv.at[j], c, far)

    def passes(j):
        return jnp.logical_or(
            jnp.logical_and(at_root(j), role_far), jnp.logical_and(jnp.logical_not(at_root(j)), role_near)
        )

    def ends(j):
        return jnp.logical_or(
            jnp.logical_and(at_root(j), is_root), jnp.logical_and(jnp.logical_not(at_root(j)), role_last)
        )

    def gives(j):
        return jnp.logical_not(jnp.logical_or(passes(j), ends(j)))

    def pass_on(j):
        @pl.when(passes(j))
        def _():
            near_copy(j).wait_recv()
            part[j] = part[j] + from_near[j]
            far_copy(j).start()

    def product(j):
        total = jnp.dot(z_ref[:, pl.ds(0, blk)], ring[j, pl.ds(0, blk)], preferred_element_type=F32)
        for k in range(1, n_blk):
            at = pl.ds(k * blk, blk)
            total += jnp.dot(z_ref[:, at], ring[j, at], preferred_element_type=F32)
        return total

    def up(i, _):
        pair = (2 * i, 2 * i + 1)

        @pl.when(i % 2 == 0)
        def _():
            done(ring.at[pl.ds(0, 4)], w_load.at[i // 2])

        totals = [product(j) for j in pair]
        for j, total in zip(pair, totals):
            part[j] = total
        for j in pair:
            @pl.when(gives(j))
            def _():
                near_copy(j).start()

        @pl.when(i < (2 * n_chunks - n_slots) // 2)
        def _():
            for j in pair:
                load_out(j + n_slots - n_chunks, j)

        @pl.when(i >= 1)
        def _():
            for j in pair:
                pass_on(j - 2)

        return 0

    lax.fori_loop(0, n_chunks // 2, up, 0)
    for j in (n_chunks - 2, n_chunks - 1):
        pass_on(j)

    inner = 1 + c % 2
    outer = (3 * c + 2) % 5
    inside = jnp.logical_or(c == 1, c == 2)
    forwards = jnp.logical_or(jnp.logical_and(c == 2, r < 2), jnp.logical_and(c == 1, r >= 2))

    def inner_copy(j):
        return remote(hid.at[j], hid.at[j], h_send.at[0], h_recv.at[j], inner, r)

    def outer_copy(j):
        return remote(hid.at[j], hid.at[j], h_send.at[0], h_recv.at[j], outer, r)

    def forward_copy(j):
        return remote(hid.at[j], hid.at[j], h_send.at[0], h_recv.at[j], 3 * (c - 1), r)

    def last_copy(j, to):
        return remote(hid_sent.at[j], hid.at[j], w_send.at[0], h_recv.at[j], to, c)

    acc[...] = jnp.zeros_like(acc)
    behind = 3
    lag = jnp.where(is_root, 1, jnp.where(role_last, jnp.where(inside, n_chunks // 2, n_chunks), 0))
    root_lag = jnp.where(is_root, behind, lag + behind)
    direct_lag = jnp.where(is_root, 4, lag - jnp.where(inside, 0, 8))
    second_half = jnp.where(is_root | inside, lag, direct_lag + 2) + n_half
    done(ring.at[pl.ds(n_chunks, n_half)], w_load.at[n_chunks // 4])

    def finish_sum(j):
        @pl.when(ends(j))
        def _():
            near_copy(j).wait_recv()
            far_copy(j).wait_recv()
            chunk = gelu_tanh(part[j] + from_near[j] + from_far[j]).astype(BF16)

            @pl.when(is_root)
            def _():
                hid[j] = chunk
                inner_copy(j).start()
                outer_copy(j).start()

            @pl.when(jnp.logical_not(is_root))
            def _():
                hid_sent[j] = chunk

                @pl.when(by_root(j))
                def _():
                    last_copy(j, c).start()

                @pl.when(direct(j))
                def _():
                    for to in range(N_COL):
                        last_copy(j, to).start()

    def use(j):
        @pl.when(jnp.logical_not(jnp.logical_and(is_root, at_root(j))))
        def _():
            inner_copy(j).wait_recv()

        @pl.when(jnp.logical_and(is_root, by_root(j)))
        def _():
            inner_copy(j).start()
            outer_copy(j).start()

        @pl.when(jnp.logical_and(forwards, jnp.logical_not(direct(j))))
        def _():
            forward_copy(j).start()

        slot = (n_chunks + j) % n_slots
        for k in range(n_blk):
            at = pl.ds(k * blk, blk)
            acc[:, at] += jnp.dot(hid[j], ring[slot, at], preferred_element_type=F32)

    def take(j, wanted):
        @pl.when(jnp.logical_and(j >= 0, j < n_chunks))
        def _():
            @pl.when(wanted(j))
            def _():
                use(j)

    def step(t, _):
        @pl.when(t < n_chunks)
        def _():
            finish_sum(t)

        @pl.when(t == second_half)
        def _():
            done(ring.at[pl.ds(0, n_half)], w_load.at[n_chunks // 4 + 1])

        take(t - lag, at_root)
        take(t - direct_lag, direct)
        take(t - root_lag, by_root)
        return 0

    lax.fori_loop(0, 2 * n_chunks + behind, step, 0)

    def near_part(i, k):
        other = near if i == 0 else (near + 2) % N_ROW
        at = pl.ds(k * blk, blk)
        return remote(
            acc.at[pl.ds(pl.multiple_of(other * rows, rows), rows), at], near_sum.at[i, :, at],
            n_send.at[0], n_recv.at[i, k], c, near,
        )

    def far_part(k):
        at = pl.ds(k * blk, blk)
        return remote(pair_sum.at[:, at], far_sum.at[:, at], o_send.at[0], o_recv.at[k], c, far)

    def store(k):
        at = pl.ds(k * blk, blk)
        return pltpu.make_async_copy(y_ref.at[:, at], y_hbm.at[:, at], y_store.at[0])

    for i in (1, 0):
        for k in range(n_blk):
            near_part(i, k).start()
    for k in range(n_blk):
        at = pl.ds(k * blk, blk)
        near_part(1, k).wait_recv()
        pair_sum[:, at] = acc[pl.ds(pl.multiple_of(far * rows, rows), rows), at] + near_sum[1, :, at]
        far_part(k).start()
    count = [sum(KINDS[i % len(KINDS)] == kind for i in range(n_chunks)) for kind in range(3)]
    done(stats.at[pl.ds(0, N_COL * N_ROW - 1)], s_send.at[0])

    @pl.when(is_root)
    def _():
        done(gain.at[pl.ds(0, N_COL - 1)], g_send.at[0])
        done(x_all.at[pl.ds(0, (N_ROW - 1) * rows)], x_send.at[0])
        done(part.at[pl.ds(0, count[1] + count[2])], p_send.at[0])
        done(part.at[pl.ds(0, count[0] + count[1])], h_send.at[0])

    @pl.when(jnp.logical_not(is_root))
    def _():
        done(x_all, x_send.at[0])

    @pl.when(role_last)
    def _():
        done(part.at[pl.ds(0, count[0])], p_send.at[0])
        done(part.at[pl.ds(0, (count[1] + N_COL * count[2]) // 2)], w_send.at[0])

    @pl.when(jnp.logical_or(role_near, role_far))
    def _():
        done(part, p_send.at[0])

    @pl.when(forwards)
    def _():
        done(hid.at[pl.ds(0, count[0] + count[1])], h_send.at[0])

    for k in range(n_blk):
        at = pl.ds(k * blk, blk)
        near_part(0, k).wait_recv()
        far_part(k).wait_recv()
        own = acc[pl.ds(pl.multiple_of(r * rows, rows), rows), at] + near_sum[0, :, at] + far_sum[:, at]
        y_ref[:, at] = (x_own[:, at].astype(F32) + own).astype(BF16)
        store(k).start()

    done(near_sum, n_send.at[0])
    done(pair_sum, o_send.at[0])
    done(y_ref, y_store.at[0])


def solution(mesh):
    def local_block(x_blk, gain_blk, w_in_blk, w_out_blk):
        rows, depth = x_blk.shape
        blk = depth // 4
        n_chunks = w_in_blk.shape[1] // blk
        n_slots = n_chunks + n_chunks // 2
        tokens = rows * N_ROW
        dma = pltpu.SemaphoreType.DMA
        n_all = N_COL * N_ROW
        return pl.pallas_call(
            functools.partial(mlp_kernel, n_chunks, n_slots, blk),
            out_shape=jax.ShapeDtypeStruct((rows, depth), BF16),
            in_specs=[pl.BlockSpec(memory_space=pl.ANY)] * 4,
            out_specs=pl.BlockSpec(memory_space=pl.ANY),
            scratch_shapes=[
                pltpu.VMEM((rows, depth), BF16),
                pltpu.VMEM((N_COL, 1, depth), F32),
                pltpu.VMEM((n_all, 1, 128), F32),
                pltpu.VMEM((tokens, depth), BF16),
                pltpu.VMEM((tokens, depth), BF16),
                pltpu.VMEM((n_slots, depth, blk), BF16),
                pltpu.VMEM((n_chunks, tokens, blk), F32),
                pltpu.VMEM((n_chunks, tokens, blk), F32),
                pltpu.VMEM((n_chunks, tokens, blk), F32),
                pltpu.VMEM((n_chunks, tokens, blk), BF16),
                pltpu.VMEM((n_chunks, tokens, blk), BF16),
                pltpu.VMEM((tokens, depth), F32),
                pltpu.VMEM((2, rows, depth), F32),
                pltpu.VMEM((rows, depth), F32),
                pltpu.VMEM((rows, depth), F32),
                pltpu.VMEM((rows, depth), BF16),
                dma((2,)), dma((n_chunks // 4 + 2,)),
                dma((1,)), dma((1,)), dma((1,)), dma((1,)), dma((1,)), dma((1,)),
                dma((1,)), dma((n_chunks,)), dma((n_chunks,)),
                dma((1,)), dma((n_chunks,)), dma((1,)),
                dma((1,)), dma((2, depth // blk)), dma((1,)), dma((depth // blk,)), dma((1,)),
            ],
            compiler_params=pltpu.CompilerParams(
                collective_id=0, has_side_effects=True, vmem_limit_bytes=67_000_000
            ),
        )(x_blk, gain_blk.reshape(1, depth), w_in_blk, w_out_blk)

    return jax.shard_map(
        local_block,
        mesh=mesh,
        in_specs=(P(("dp", "row"), "col"), P("col"), P("row", "col"), P("row", "col")),
        out_specs=P(("dp", "row"), "col"),
        check_vma=False,
    )
```

```python
import functools

import jax
import jax.numpy as jnp
from jax import lax
from jax.experimental import pallas as pl
from jax.experimental.pallas import tpu as pltpu
from jax.sharding import PartitionSpec as P

NORM_EPS = 1e-5
MESH = pl.DeviceIdType.MESH
BF16, F32 = jnp.bfloat16, jnp.float32
N_COL = 4
N_ROW = 4
KINDS = (0, 1, 0, 1, 0, 1, 0, 1, 0, 0, 0, 2, 2, 2, 2, 2)


def gelu_tanh(x):
    return x * (0.5 * (1.0 + jnp.tanh(0.7978845608028654 * (x + 0.044715 * (x * x * x)))))


def mlp_kernel(
    n_chunks, n_slots, blk,
    x_hbm, g_hbm, w_in_hbm, w_out_hbm, y_hbm,
    x_own, gain, stats, x_all, z_ref, ring, part, from_near, from_far, hid, hid_sent, acc, near_sum, pair_sum, far_sum, y_ref,
    x_load, w_load, x_send, x_recv, g_send, g_recv, s_send, s_recv, p_send, p_recv, f_recv,
    h_send, h_recv, w_send, n_send, n_recv, o_send, o_recv, y_store,
):
    dp, c, r = lax.axis_index("dp"), lax.axis_index("col"), lax.axis_index("row")
    rows = x_own.shape[0]
    n_blk = x_own.shape[1] // blk
    d_model = x_own.shape[1] * N_COL
    near = r + 1 - 2 * (r % 2)
    far = (r + 2) % N_ROW
    me = c * N_ROW + r
    is_root = c == r

    def remote(src, dst, send, recv, to_col, to_row):
        return pltpu.make_async_remote_copy(
            src_ref=src, dst_ref=dst, send_sem=send, recv_sem=recv,
            device_id=(dp, to_col, to_row), device_id_type=MESH,
        )

    def peer(i):
        other = (me + i) % (N_COL * N_ROW)
        return other // N_ROW, other % N_ROW

    x_cp = pltpu.make_async_copy(x_hbm, x_own, x_load.at[0])
    x_cp.start()
    g_cp = pltpu.make_async_copy(g_hbm, gain.at[c], x_load.at[1])
    g_cp.start()
    barrier = pltpu.get_barrier_semaphore()
    for i in range(1, N_COL * N_ROW):
        pc, pr = peer(i)
        pl.semaphore_signal(barrier, inc=1, device_id=(dp, pc, pr), device_id_type=MESH)

    def load_in(j, slot):
        pltpu.make_async_copy(
            w_in_hbm.at[:, pl.ds(pl.multiple_of(j * blk, blk), blk)], ring.at[slot], w_load.at[j // 4]
        ).start()

    def load_out(j, slot):
        for k in range(n_blk):
            pltpu.make_async_copy(
                w_out_hbm.at[pl.ds(pl.multiple_of(j * blk, blk), blk), pl.ds(k * blk, blk)],
                ring.at[slot, pl.ds(k * blk, blk)], w_load.at[n_chunks // 4 + j // n_half],
            ).start()

    n_half = n_chunks // 2

    def done(ref, sem):
        pltpu.make_async_copy(ref, ref, sem).wait()

    def fill_in(j, _):
        load_in(j, j)
        return 0

    def fill_out(j, _):
        load_out(j, n_chunks + j)
        return 0

    lax.fori_loop(0, n_chunks, fill_in, 0)

    x_cp.wait()
    g_cp.wait()
    x_f32 = x_own[...].astype(F32)
    lane = lax.broadcasted_iota(jnp.int32, (rows, 128), 1)
    sub = lax.broadcasted_iota(jnp.int32, (rows, 128), 0)
    total = jnp.sum(x_f32, axis=1, keepdims=True)
    square = jnp.sum(x_f32 * x_f32, axis=1, keepdims=True)
    packed = jnp.where(lane == sub, total, 0.0) + jnp.where(lane == sub + rows, square, 0.0)
    stats[me] = jnp.sum(packed, axis=0, keepdims=True)

    pl.semaphore_wait(barrier, N_COL * N_ROW - 1)

    def stat_copy(i):
        pc, pr = peer(i)
        return remote(stats.at[me], stats.at[me], s_send.at[0], s_recv.at[0], pc, pr)

    def far_first(i):
        if i == 0:
            return c
        if i == 3:
            return jnp.where(c < 2, 3, 0)
        if i == 2:
            return jnp.where(c < 2, 2, 1)
        return jnp.where(c < 2, 1 - c, 5 - c)

    def x_copy(i):
        return remote(x_own, x_all.at[pl.ds(r * rows, rows)], x_send.at[0], x_recv.at[0], far_first(i), c)

    def g_copy(i):
        return remote(gain.at[c], gain.at[c], g_send.at[0], g_recv.at[0], far_first(i), c)

    @pl.when(is_root)
    def _():
        for i in (3, 2, 1):
            g_copy(i).start()

    for i in range(1, N_COL * N_ROW):
        stat_copy(i).start()
    for i in (3, 2, 1):
        x_copy(i).start()

    @pl.when(is_root)
    def _():
        x_all[pl.ds(pl.multiple_of(r * rows, rows), rows), :] = x_own[...]

    @pl.when(jnp.logical_not(is_root))
    def _():
        x_copy(0).start()

    lax.fori_loop(0, n_slots - n_chunks, fill_out, 0)

    done(stats.at[pl.ds(0, N_COL * N_ROW - 1)], s_recv.at[0])

    @pl.when(is_root)
    def _():
        done(x_all.at[pl.ds(0, (N_ROW - 1) * rows)], x_recv.at[0])

    @pl.when(jnp.logical_not(is_root))
    def _():
        done(gain.at[0], g_recv.at[0])
        done(x_all, x_recv.at[0])

    for q in range(N_ROW):
        at = pl.ds(q * rows, rows)
        whole = stats[q] + stats[N_ROW + q] + stats[2 * N_ROW + q] + stats[3 * N_ROW + q]
        whole = jnp.broadcast_to(whole, (rows, 128))
        mean = jnp.sum(jnp.where(lane == sub, whole, 0.0), axis=1, keepdims=True) / d_model
        mean_sq = jnp.sum(jnp.where(lane == sub + rows, whole, 0.0), axis=1, keepdims=True) / d_model
        inv = lax.rsqrt(mean_sq - mean * mean + NORM_EPS)
        z_ref[at, :] = ((x_all[at, :].astype(F32) - mean) * inv * gain[r]).astype(BF16)

    role_near = near == c
    role_far = far == c
    role_last = r == N_ROW - 1 - c

    def one_of(j, kind):
        found = [j == i for i in range(n_chunks) if KINDS[i % len(KINDS)] == kind]
        return functools.reduce(jnp.logical_or, found)

    def at_root(j):
        return one_of(j, 0)

    def by_root(j):
        return one_of(j, 1)

    def direct(j):
        return one_of(j, 2)

    def near_copy(j):
        return remote(part.at[j], from_near.at[j], p_send.at[0], p_recv.at[j], c, near)

    def far_copy(j):
        return remote(part.at[j], from_far.at[j], p_send.at[0], f_recv.at[j], c, far)

    def passes(j):
        return jnp.logical_or(
            jnp.logical_and(at_root(j), role_far), jnp.logical_and(jnp.logical_not(at_root(j)), role_near)
        )

    def ends(j):
        return jnp.logical_or(
            jnp.logical_and(at_root(j), is_root), jnp.logical_and(jnp.logical_not(at_root(j)), role_last)
        )

    def gives(j):
        return jnp.logical_not(jnp.logical_or(passes(j), ends(j)))

    def pass_on(j):
        @pl.when(passes(j))
        def _():
            near_copy(j).wait_recv()
            part[j] = part[j] + from_near[j]
            far_copy(j).start()

    def product(j):
        total = jnp.dot(z_ref[:, pl.ds(0, blk)], ring[j, pl.ds(0, blk)], preferred_element_type=F32)
        for k in range(1, n_blk):
            at = pl.ds(k * blk, blk)
            total += jnp.dot(z_ref[:, at], ring[j, at], preferred_element_type=F32)
        return total

    def up(i, _):
        pair = (2 * i, 2 * i + 1)

        @pl.when(i % 2 == 0)
        def _():
            done(ring.at[pl.ds(0, 4)], w_load.at[i // 2])

        totals = [product(j) for j in pair]
        for j, total in zip(pair, totals):
            part[j] = total
        for j in pair:
            @pl.when(gives(j))
            def _():
                near_copy(j).start()

        @pl.when(i < (2 * n_chunks - n_slots) // 2)
        def _():
            for j in pair:
                load_out(j + n_slots - n_chunks, j)

        @pl.when(i >= 1)
        def _():
            for j in pair:
                pass_on(j - 2)

        return 0

    lax.fori_loop(0, n_chunks // 2, up, 0)
    for j in (n_chunks - 2, n_chunks - 1):
        pass_on(j)

    inner = 1 + c % 2
    outer = (3 * c + 2) % 5
    inside = jnp.logical_or(c == 1, c == 2)
    forwards = jnp.logical_or(jnp.logical_and(c == 2, r < 2), jnp.logical_and(c == 1, r >= 2))

    def inner_copy(j):
        return remote(hid.at[j], hid.at[j], h_send.at[0], h_recv.at[j], inner, r)

    def outer_copy(j):
        return remote(hid.at[j], hid.at[j], h_send.at[0], h_recv.at[j], outer, r)

    def forward_copy(j):
        return remote(hid.at[j], hid.at[j], h_send.at[0], h_recv.at[j], 3 * (c - 1), r)

    def last_copy(j, to):
        return remote(hid_sent.at[j], hid.at[j], w_send.at[0], h_recv.at[j], to, c)

    acc[...] = jnp.zeros_like(acc)
    behind = 2
    lag = jnp.where(is_root, 1, jnp.where(role_last, jnp.where(inside, n_chunks // 2, n_chunks), 0))
    root_lag = jnp.where(is_root, behind, lag + behind)
    direct_lag = jnp.where(is_root, 4, lag - jnp.where(inside, 0, 8))
    second_half = jnp.where(is_root | inside, lag, direct_lag + 2) + n_half
    done(ring.at[pl.ds(n_chunks, n_half)], w_load.at[n_chunks // 4])

    def finish_sum(j):
        @pl.when(ends(j))
        def _():
            near_copy(j).wait_recv()
            far_copy(j).wait_recv()
            chunk = gelu_tanh(part[j] + from_near[j] + from_far[j]).astype(BF16)

            @pl.when(is_root)
            def _():
                hid[j] = chunk
                inner_copy(j).start()
                outer_copy(j).start()

            @pl.when(jnp.logical_not(is_root))
            def _():
                hid_sent[j] = chunk

                @pl.when(by_root(j))
                def _():
                    last_copy(j, c).start()

                @pl.when(direct(j))
                def _():
                    for to in range(N_COL):
                        last_copy(j, to).start()

    def use(j):
        @pl.when(jnp.logical_not(jnp.logical_and(is_root, at_root(j))))
        def _():
            inner_copy(j).wait_recv()

        @pl.when(jnp.logical_and(is_root, by_root(j)))
        def _():
            inner_copy(j).start()
            outer_copy(j).start()

        @pl.when(jnp.logical_and(forwards, jnp.logical_not(direct(j))))
        def _():
            forward_copy(j).start()

        slot = (n_chunks + j) % n_slots
        for k in range(n_blk):
            at = pl.ds(k * blk, blk)
            acc[:, at] += jnp.dot(hid[j], ring[slot, at], preferred_element_type=F32)

    def take(j, wanted):
        @pl.when(jnp.logical_and(j >= 0, j < n_chunks))
        def _():
            @pl.when(wanted(j))
            def _():
                use(j)

    def step(t, _):
        @pl.when(t < n_chunks)
        def _():
            finish_sum(t)

        @pl.when(t == second_half)
        def _():
            done(ring.at[pl.ds(0, n_half)], w_load.at[n_chunks // 4 + 1])

        take(t - lag, at_root)
        take(t - direct_lag, direct)
        take(t - root_lag, by_root)
        return 0

    lax.fori_loop(0, 2 * n_chunks + behind, step, 0)

    def near_part(i, k):
        other = near if i == 0 else (near + 2) % N_ROW
        at = pl.ds(k * blk, blk)
        return remote(
            acc.at[pl.ds(pl.multiple_of(other * rows, rows), rows), at], near_sum.at[i, :, at],
            n_send.at[0], n_recv.at[i, k], c, near,
        )

    def far_part(k):
        at = pl.ds(k * blk, blk)
        return remote(pair_sum.at[:, at], far_sum.at[:, at], o_send.at[0], o_recv.at[k], c, far)

    def store(k):
        at = pl.ds(k * blk, blk)
        return pltpu.make_async_copy(y_ref.at[:, at], y_hbm.at[:, at], y_store.at[0])

    for i in (1, 0):
        for k in range(n_blk):
            near_part(i, k).start()
    for k in range(n_blk):
        at = pl.ds(k * blk, blk)
        near_part(1, k).wait_recv()
        pair_sum[:, at] = acc[pl.ds(pl.multiple_of(far * rows, rows), rows), at] + near_sum[1, :, at]
        far_part(k).start()
    count = [sum(KINDS[i % len(KINDS)] == kind for i in range(n_chunks)) for kind in range(3)]
    done(stats.at[pl.ds(0, N_COL * N_ROW - 1)], s_send.at[0])

    @pl.when(is_root)
    def _():
        done(gain.at[pl.ds(0, N_COL - 1)], g_send.at[0])
        done(x_all.at[pl.ds(0, (N_ROW - 1) * rows)], x_send.at[0])
        done(part.at[pl.ds(0, count[1] + count[2])], p_send.at[0])
        done(part.at[pl.ds(0, count[0] + count[1])], h_send.at[0])

    @pl.when(jnp.logical_not(is_root))
    def _():
        done(x_all, x_send.at[0])

    @pl.when(role_last)
    def _():
        done(part.at[pl.ds(0, count[0])], p_send.at[0])
        done(part.at[pl.ds(0, (count[1] + N_COL * count[2]) // 2)], w_send.at[0])

    @pl.when(jnp.logical_or(role_near, role_far))
    def _():
        done(part, p_send.at[0])

    @pl.when(forwards)
    def _():
        done(hid.at[pl.ds(0, count[0] + count[1])], h_send.at[0])

    for k in range(n_blk):
        at = pl.ds(k * blk, blk)
        near_part(0, k).wait_recv()
        far_part(k).wait_recv()
        own = acc[pl.ds(pl.multiple_of(r * rows, rows), rows), at] + near_sum[0, :, at] + far_sum[:, at]
        y_ref[:, at] = (x_own[:, at].astype(F32) + own).astype(BF16)
        store(k).start()

    done(near_sum, n_send.at[0])
    done(pair_sum, o_send.at[0])
    done(y_ref, y_store.at[0])


def solution(mesh):
    def local_block(x_blk, gain_blk, w_in_blk, w_out_blk):
        rows, depth = x_blk.shape
        blk = depth // 4
        n_chunks = w_in_blk.shape[1] // blk
        n_slots = n_chunks + n_chunks // 2
        tokens = rows * N_ROW
        dma = pltpu.SemaphoreType.DMA
        n_all = N_COL * N_ROW
        return pl.pallas_call(
            functools.partial(mlp_kernel, n_chunks, n_slots, blk),
            out_shape=jax.ShapeDtypeStruct((rows, depth), BF16),
            in_specs=[pl.BlockSpec(memory_space=pl.ANY)] * 4,
            out_specs=pl.BlockSpec(memory_space=pl.ANY),
            scratch_shapes=[
                pltpu.VMEM((rows, depth), BF16),
                pltpu.VMEM((N_COL, 1, depth), F32),
                pltpu.VMEM((n_all, 1, 128), F32),
                pltpu.VMEM((tokens, depth), BF16),
                pltpu.VMEM((tokens, depth), BF16),
                pltpu.VMEM((n_slots, depth, blk), BF16),
                pltpu.VMEM((n_chunks, tokens, blk), F32),
                pltpu.VMEM((n_chunks, tokens, blk), F32),
                pltpu.VMEM((n_chunks, tokens, blk), F32),
                pltpu.VMEM((n_chunks, tokens, blk), BF16),
                pltpu.VMEM((n_chunks, tokens, blk), BF16),
                pltpu.VMEM((tokens, depth), F32),
                pltpu.VMEM((2, rows, depth), F32),
                pltpu.VMEM((rows, depth), F32),
                pltpu.VMEM((rows, depth), F32),
                pltpu.VMEM((rows, depth), BF16),
                dma((2,)), dma((n_chunks // 4 + 2,)),
                dma((1,)), dma((1,)), dma((1,)), dma((1,)), dma((1,)), dma((1,)),
                dma((1,)), dma((n_chunks,)), dma((n_chunks,)),
                dma((1,)), dma((n_chunks,)), dma((1,)),
                dma((1,)), dma((2, depth // blk)), dma((1,)), dma((depth // blk,)), dma((1,)),
            ],
            compiler_params=pltpu.CompilerParams(
                collective_id=0, has_side_effects=True, vmem_limit_bytes=67_000_000
            ),
        )(x_blk, gain_blk.reshape(1, depth), w_in_blk, w_out_blk)

    return jax.shard_map(
        local_block,
        mesh=mesh,
        in_specs=(P(("dp", "row"), "col"), P("col"), P("row", "col"), P("row", "col")),
        out_specs=P(("dp", "row"), "col"),
        check_vma=False,
    )
```
